128 devices in a mesh: seq: 32 (over z, y_hi, x), head: 4 (over y_lo, core).
Axes of the slice: x: 4, y: 4 (y_hi: 2, y_lo: 2; y = y_hi * 2 + y_lo), z: 4, core: 2. Of those that a mesh axis runs over, the one named last changes fastest.
Arguments:
- queries: bfloat16 [8192, 3584], P('seq', 'head'), may hold values from -5 to 5
- keys: bfloat16 [8192, 3584], P('seq', 'head'), may hold values from -5 to 5
- values: bfloat16 [8192, 3584], P('seq', 'head'), may hold values from -6 to 6
- attn_grad: bfloat16 [8192, 3584], P('seq', 'head'), may hold values from -6 to 6
- doc_ids: int32 [8192], replicated, may hold values from 0 to 7, never falling along the last dimension, each value on 1 to 4096 neighbouring positions
- conv_input: bfloat16 [8192, 7168], P('seq', 'head'), may hold values from -6 to 6
- conv_weight: float32 [4, 7168], P(None, 'head'), may hold values from -3 to 3
- step_raw: float32 [8192, 112], P('seq', 'head'), may hold values from -4 to 4
- step_bias: float32 [112], P('head'), may hold values from -1.5 to 0
- rate_log: float32 [112], P('head'), may hold values from -13 to -1
- skip_gain: float32 [112], P('head'), may hold values from 0.5 to 1.5
- input_coeff: bfloat16 [8192, 128], P('seq'), may hold values from -0.625 to 0.625
- output_coeff: bfloat16 [8192, 128], P('seq'), may hold values from -0.625 to 0.625
- gate_input: bfloat16 [8192, 7168], P('seq', 'head'), may hold values from -6 to 6
- mix_grad: bfloat16 [8192, 7168], P('seq', 'head'), may hold values from -1.5 to 1.5
Outputs:
- grad_queries: bfloat16 [8192, 3584], P('seq', 'head')
- grad_keys: bfloat16 [8192, 3584], P('seq', 'head')
- grad_values: bfloat16 [8192, 3584], P('seq', 'head')
- grad_conv_input: bfloat16 [8192, 7168], P('seq', 'head')
- grad_gate: bfloat16 [8192, 7168], P('seq', 'head')
- grad_step: float32 [8192, 112], P('seq', 'head')
- grad_input_coeff: float32 [8192, 128], P('seq')
- grad_output_coeff: float32 [8192, 128], P('seq')
- grad_conv_weight: float32 [4, 7168], P(None, 'head')
- grad_step_bias: float32 [112], P('head')
- grad_rate_log: float32 [112], P('head')
- grad_skip: float32 [112], P('head')
The draws below stay inside these ranges and needn't reach their ends.
Inputs may be any that keep to these rules, and one draw needn't show every extreme that they name: doc_ids never fall along the sequence.
All inputs are finite; a program needn't handle non-finite values.
Results may differ from the reference program's by a relative error of at most 0.012.
Values may be sent and summed in bfloat16 or wider, within the bound.
A program may use at most 128 MiB of HBM per device.

```python
import math
import jax
import jax.numpy as jnp
import numpy as np
from jax import lax

T_DEV = 256
HEADS = 16
HEAD_DIM = 224
WINDOW = 1024
SSM_HEADS = 112
SSM_DIM = 64
STATE = 64
GROUPS = 2
KERNEL = 4
STRETCH = 128
SEQLEN = 8192
INNER = 7168
DOCS = 8


def aligned_pair(key):
    shape = (SEQLEN, HEADS * HEAD_DIM)
    normal_query = jax.random.truncated_normal(jax.random.fold_in(key, 11), -4.5, 4.5, shape, jnp.float32)
    normal_key = jax.random.truncated_normal(jax.random.fold_in(key, 12), -4.5, 4.5, shape, jnp.float32)
    return (normal_query, normal_key)


def draw_queries(key, part):
    return aligned_pair(key)[0].astype(jnp.bfloat16)


def draw_keys(key, part):
    return aligned_pair(key)[1].astype(jnp.bfloat16)


def draw_step_raw(key, part):
    blocks = SEQLEN // STRETCH
    offsets = jax.random.uniform(jax.random.fold_in(key, 21), (blocks, 1, SSM_HEADS), jnp.float32, -1.0, 1.0)
    noise = 0.5 * jax.random.truncated_normal(jax.random.fold_in(key, 23), -5.0, 5.0, (blocks, STRETCH, SSM_HEADS), jnp.float32)
    return (noise + offsets).reshape(SEQLEN, SSM_HEADS)


def draw_rate_log(key, part):
    chance = 0.5
    picked = jax.random.uniform(jax.random.fold_in(key, 31), (SSM_HEADS,), jnp.float32) < chance
    quick = jnp.log(jax.random.uniform(jax.random.fold_in(key, 32), (SSM_HEADS,), jnp.float32, 0.05, 0.3))
    slowly = jnp.log(jax.random.uniform(jax.random.fold_in(key, 33), (SSM_HEADS,), jnp.float32, 0.3, 2.0) / SEQLEN)
    return jnp.where(picked, quick, slowly)


def level_of(rng, shape, cuts, least, top_value):
    factor_of = 1.0
    for dim, shards_of in cuts:
        steps = jax.random.uniform(jax.random.fold_in(jax.random.fold_in(rng, 6), dim), (shards_of,), jnp.float32, least / len(cuts), top_value / len(cuts))
        factor_of = factor_of * jnp.repeat(jnp.exp(steps), shape[dim] // shards_of).reshape((-1,) + (1,) * (len(shape) - 1 - dim))
    return factor_of


def length_profile(count, total, bound, skew):
    loads = [(1 << 20) // math.isqrt(standing ** skew) + 1 for standing in range(2, count + 1)]
    rest, holding = total - bound - (count - 1), [1] * (count - 1)
    while rest > 0:
        free = [i for i in range(count - 1) if holding[i] < bound]
        whole, left = sum([loads[i] for i in free]), rest
        for i in free:
            addition = min(bound - holding[i], max(1, left * loads[i] // whole), rest)
            holding[i] = holding[i] + addition
            rest = rest - addition
    return np.array([bound] + holding)


def ragged_sizes(rng, number_of, total, reach, slope):
    if number_of == 2:
        one = jax.random.randint(rng, (), max(1, total - reach), min(reach, total - 1) + 1)
        return jnp.stack([one, total - one])
    sizes = jnp.asarray(length_profile(number_of, total, reach, slope), jnp.int32)
    twos = (number_of - 1) // 2
    giver, sink = sizes[1:1 + 2 * twos:2], sizes[2:2 + 2 * twos:2]
    margin = jnp.minimum(giver - 1, reach - sink)
    moved = jax.random.randint(jax.random.fold_in(rng, 1), (twos,), 0, 1 << 20) % (margin + 1)
    sizes = sizes.at[1:1 + 2 * twos:2].set(giver - moved).at[2:2 + 2 * twos:2].set(sink + moved)
    return sizes[jax.random.permutation(jax.random.fold_in(rng, 2), number_of)]


def bell_draw(key, shape, scale, most, split=(), kind=jnp.bfloat16):
    entries = jax.random.normal(key, shape, jnp.float32) * scale
    if len(split) > 0:
        entries = level_of(key, shape, split, -0.22, 0.18) * entries
    return jnp.clip(entries, min=-most, max=most).astype(kind)


def setup_inputs(seed: int = 0) -> dict:
    arg_keys = jax.random.split(jax.random.key(seed), 16)
    queries = draw_queries(jax.random.fold_in(arg_keys[15], 71), 0)
    keys = draw_keys(jax.random.fold_in(arg_keys[15], 71), 0)
    values = bell_draw(arg_keys[2], (SEQLEN, HEADS * HEAD_DIM), 1.0, 6.0, ((0, 32), (1, 4)))
    attn_grad = bell_draw(arg_keys[3], (SEQLEN, HEADS * HEAD_DIM), 1.0, 6.0, ((0, 32), (1, 4)))
    doc_ids = jnp.searchsorted(jnp.cumsum(ragged_sizes(arg_keys[4], DOCS, SEQLEN, SEQLEN // 2, 2)), jnp.arange(SEQLEN), side="right").astype(jnp.int32)
    conv_input = bell_draw(arg_keys[5], (SEQLEN, INNER), 1.0, 6.0, ((0, 32), (1, 4)))
    conv_weight = bell_draw(arg_keys[6], (KERNEL, INNER), KERNEL ** -0.5, 3.0, ((1, 4),), jnp.float32)
    step_raw = draw_step_raw(jax.random.fold_in(arg_keys[15], 71), 0)
    step_bias = jnp.clip(-1.5 + 1.5 * jax.random.uniform(arg_keys[8], (SSM_HEADS,), jnp.float32) ** level_of(arg_keys[8], (SSM_HEADS,), ((0, 4),), -0.2, 0.2), -1.5, 0.0)
    rate_log = draw_rate_log(jax.random.fold_in(arg_keys[15], 71), 0)
    skip_gain = jnp.clip(0.5 + 1.0 * jax.random.uniform(arg_keys[10], (SSM_HEADS,), jnp.float32) ** level_of(arg_keys[10], (SSM_HEADS,), ((0, 4),), -0.2, 0.2), 0.5, 1.5)
    input_coeff = bell_draw(arg_keys[11], (SEQLEN, GROUPS * STATE), 0.1, 0.625, ((0, 32),))
    output_coeff = bell_draw(arg_keys[12], (SEQLEN, GROUPS * STATE), 0.1, 0.625, ((0, 32),))
    gate_input = bell_draw(arg_keys[13], (SEQLEN, INNER), 1.0, 6.0, ((0, 32), (1, 4)))
    mix_grad = bell_draw(arg_keys[14], (SEQLEN, INNER), 0.25, 1.5, ((0, 32), (1, 4)))
    return dict(queries=queries, keys=keys, values=values, attn_grad=attn_grad, doc_ids=doc_ids, conv_input=conv_input, conv_weight=conv_weight, step_raw=step_raw, step_bias=step_bias, rate_log=rate_log, skip_gain=skip_gain, input_coeff=input_coeff, output_coeff=output_coeff, gate_input=gate_input, mix_grad=mix_grad)


NEG_FILL = -1e+30
EXACT = lax.Precision.HIGHEST

def conv_act(padded, doc_ext, weight):
    kernel_taps = weight.shape[0]
    length = padded.shape[0] - kernel_taps + 1
    doc_now = doc_ext[kernel_taps - 1:]
    summed = jnp.zeros((length, padded.shape[1]), jnp.float32)
    for lagged in range(kernel_taps):
        first_row = kernel_taps - 1 - lagged
        shifted = padded[first_row:first_row + length]
        same_doc = doc_ext[first_row:first_row + length] == doc_now
        summed = summed + weight[lagged] * jnp.where(same_doc[:, None], shifted, 0.0)
    return jax.nn.silu(summed)

def stretch_layout(log_decay, doc_row, doc_before):
    blocks = doc_row.shape[0] // STRETCH
    cumulative = jnp.cumsum(log_decay.reshape(blocks, STRETCH), axis=1)
    doc_grid = doc_row.reshape(blocks, STRETCH)
    previous = jnp.concatenate([jnp.reshape(doc_before, (1,)), doc_grid[:-1, -1]])
    return (cumulative, doc_grid, previous)

def head_final(head_act, step_size, log_decay, in_grid, start_state, doc_row, doc_before):
    cumulative, doc_grid, previous = stretch_layout(log_decay, doc_row, doc_before)
    blocks = cumulative.shape[0]
    scaled = (head_act * step_size[:, None]).reshape(blocks, STRETCH, head_act.shape[1])
    same_end = doc_grid == doc_grid[:, -1:]
    to_end = jnp.where(same_end, jnp.exp(jnp.where(same_end, cumulative[:, -1:] - cumulative, 0.0)), 0.0)
    local_state = jnp.einsum('cjp,cjn->cpn', scaled * to_end[:, :, None], in_grid, precision=EXACT)
    through = jnp.where(doc_grid[:, -1] == previous, jnp.exp(cumulative[:, -1]), 0.0)

    def advance(carry_state, pair_item):
        return (pair_item[0] * carry_state + pair_item[1], carry_state)
    final_state, starts = lax.scan(advance, start_state, (through, local_state))
    return (final_state, starts, cumulative, doc_grid, previous, scaled)

def head_output(head_act, step_size, log_decay, pair_grid, in_grid, out_grid, gate_part, skip_gain, start_state, doc_row, doc_before):
    final_state, starts, cumulative, doc_grid, previous, scaled = head_final(head_act, step_size, log_decay, in_grid, start_state, doc_row, doc_before)
    causal = jnp.arange(STRETCH)[:, None] >= jnp.arange(STRETCH)[None, :]
    same_doc = (doc_grid[:, :, None] == doc_grid[:, None, :]) & causal[None]
    weights = jnp.where(same_doc, jnp.exp(jnp.where(same_doc, cumulative[:, :, None] - cumulative[:, None, :], 0.0)), 0.0)
    inner_part = jnp.einsum('cij,cjp->cip', pair_grid * weights, scaled, precision=EXACT)
    enter_gain = jnp.where(doc_grid == previous[:, None], jnp.exp(cumulative), 0.0)
    carried = jnp.einsum('cin,cpn->cip', out_grid, starts, precision=EXACT) * enter_gain[:, :, None]
    mixed_out = (inner_part + carried).reshape(head_act.shape) + skip_gain * head_act
    return (mixed_out * jax.nn.silu(gate_part), final_state)

def round_edge(term):
    edge = lax.optimization_barrier(term[:WINDOW].astype(jnp.bfloat16)).astype(jnp.float32)
    return jnp.concatenate([edge, term[WINDOW:]], axis=0)

def attention_grads(queries, keys, values, attn_grad, doc_ids):
    width = HEADS * HEAD_DIM
    span = WINDOW + T_DEV
    scale = HEAD_DIM ** (-0.5)
    key_pad = jnp.concatenate([jnp.zeros((WINDOW, width), keys.dtype), keys])
    value_pad = jnp.concatenate([jnp.zeros((WINDOW, width), values.dtype), values])
    doc_pad = jnp.concatenate([jnp.full((WINDOW,), -1, jnp.int32), doc_ids])
    distance = jnp.arange(T_DEV)[:, None] + WINDOW - jnp.arange(span)[None, :]
    in_window = (distance >= 0) & (distance < WINDOW)

    def one_block(carry, index):
        key_acc, value_acc = carry
        first_row = index * T_DEV
        query_part = lax.dynamic_slice_in_dim(queries, first_row, T_DEV).astype(jnp.float32).reshape(T_DEV, HEADS, HEAD_DIM)
        grad_part = lax.dynamic_slice_in_dim(attn_grad, first_row, T_DEV).astype(jnp.float32).reshape(T_DEV, HEADS, HEAD_DIM)
        key_part = lax.dynamic_slice_in_dim(key_pad, first_row, span).astype(jnp.float32).reshape(span, HEADS, HEAD_DIM)
        value_part = lax.dynamic_slice_in_dim(value_pad, first_row, span).astype(jnp.float32).reshape(span, HEADS, HEAD_DIM)
        doc_query = lax.dynamic_slice_in_dim(doc_ids, first_row, T_DEV)
        doc_key = lax.dynamic_slice_in_dim(doc_pad, first_row, span)
        allowed = in_window & (doc_query[:, None] == doc_key[None, :])
        scores = jnp.where(allowed[None], jnp.einsum('ihd,jhd->hij', query_part, key_part) * scale, NEG_FILL)
        row_max = lax.optimization_barrier(jnp.max(scores, axis=-1))
        expo = jnp.where(allowed[None], jnp.exp(scores - row_max[:, :, None]), 0.0)
        row_sum = lax.optimization_barrier(jnp.sum(expo, axis=-1))
        probs = expo / jnp.maximum(row_sum, 1.0)[:, :, None]
        probs_half = lax.optimization_barrier(probs.astype(jnp.bfloat16)).astype(jnp.float32)
        attn_out = jnp.einsum('hij,jhd->ihd', probs_half, value_part)
        delta = lax.optimization_barrier(jnp.sum(grad_part * attn_out, axis=-1)).T
        dprob = jnp.einsum('ihd,jhd->hij', grad_part, value_part)
        dscore = lax.optimization_barrier((probs * (dprob - delta[:, :, None])).astype(jnp.bfloat16)).astype(jnp.float32)
        grad_query = (jnp.einsum('hij,jhd->ihd', dscore, key_part) * scale).reshape(T_DEV, width).astype(jnp.bfloat16)
        key_term = round_edge(jnp.einsum('hij,ihd->jhd', dscore, query_part).reshape(span, width))
        value_term = round_edge(jnp.einsum('hij,ihd->jhd', probs_half, grad_part).reshape(span, width))
        key_acc = lax.dynamic_update_slice_in_dim(key_acc, lax.dynamic_slice_in_dim(key_acc, first_row, span) + key_term, first_row, 0)
        value_acc = lax.dynamic_update_slice_in_dim(value_acc, lax.dynamic_slice_in_dim(value_acc, first_row, span) + value_term, first_row, 0)
        return ((key_acc, value_acc), grad_query)
    zero_acc = jnp.zeros((WINDOW + SEQLEN, width), jnp.float32)
    (key_acc, value_acc), grad_blocks = lax.scan(one_block, (zero_acc, zero_acc), jnp.arange(SEQLEN // T_DEV, dtype=jnp.int32))
    grad_queries = grad_blocks.reshape(SEQLEN, width)
    grad_keys = (key_acc[WINDOW:] * scale).astype(jnp.bfloat16)
    grad_values = value_acc[WINDOW:].astype(jnp.bfloat16)
    return (grad_queries, grad_keys, grad_values)

def mixer_grads(doc_ids, conv_input, conv_weight, step_raw, step_bias, rate_log, skip_gain, input_coeff, output_coeff, gate_input, mix_grad):
    doc_ext = jnp.concatenate([jnp.full((KERNEL - 1,), -1, jnp.int32), doc_ids])
    padded_all = jnp.concatenate([jnp.zeros((KERNEL - 1, INNER), jnp.float32), conv_input.astype(jnp.float32)])
    group_heads = SSM_HEADS // GROUPS
    blocks = SEQLEN // STRETCH
    zero_state = jnp.zeros((SSM_DIM, STATE), jnp.float32)
    start_doc = jnp.int32(-1)

    def forward(padded, weight, raw_step, bias_one, rate_one, skip_one, group_in, group_out, gate_part):
        head_act = conv_act(padded, doc_ext, weight)
        step_size = jax.nn.softplus(raw_step + bias_one)
        log_decay = -step_size * jnp.exp(rate_one)
        in_grid = group_in.reshape(blocks, STRETCH, STATE)
        out_grid = group_out.reshape(blocks, STRETCH, STATE)
        pair_grid = jnp.einsum('cin,cjn->cij', out_grid, in_grid, precision=EXACT)
        return head_output(head_act, step_size, log_decay, pair_grid, in_grid, out_grid, gate_part, skip_one, zero_state, doc_ids, start_doc)[0]

    def one_head(carry, head_index):
        sum_in, sum_out = carry
        column = head_index * SSM_DIM
        group_col = head_index // group_heads * STATE
        primals = (lax.dynamic_slice_in_dim(padded_all, column, SSM_DIM, 1), lax.dynamic_slice_in_dim(conv_weight, column, SSM_DIM, 1), lax.dynamic_index_in_dim(step_raw, head_index, 1, keepdims=False), step_bias[head_index], rate_log[head_index], skip_gain[head_index], lax.dynamic_slice_in_dim(input_coeff, group_col, STATE, 1).astype(jnp.float32), lax.dynamic_slice_in_dim(output_coeff, group_col, STATE, 1).astype(jnp.float32), lax.dynamic_slice_in_dim(gate_input, column, SSM_DIM, 1).astype(jnp.float32))
        cotangent = lax.dynamic_slice_in_dim(mix_grad, column, SSM_DIM, 1).astype(jnp.float32)
        gradients = jax.vjp(forward, *primals)[1](cotangent)
        sum_in = lax.dynamic_update_slice_in_dim(sum_in, lax.dynamic_slice_in_dim(sum_in, group_col, STATE, 1) + gradients[6], group_col, 1)
        sum_out = lax.dynamic_update_slice_in_dim(sum_out, lax.dynamic_slice_in_dim(sum_out, group_col, STATE, 1) + gradients[7], group_col, 1)
        return ((sum_in, sum_out), (gradients[0][KERNEL - 1:].astype(jnp.bfloat16), gradients[8].astype(jnp.bfloat16), gradients[2], gradients[1], gradients[3], gradients[4], gradients[5]))
    zero_cols = jnp.zeros((SEQLEN, GROUPS * STATE), jnp.float32)
    (sum_in, sum_out), stacked = lax.scan(one_head, (zero_cols, zero_cols), jnp.arange(SSM_HEADS, dtype=jnp.int32))
    conv_grad, gate_grad, step_grad, weight_grad, bias_grad, rate_grad, skip_grad = stacked
    grad_conv_input = jnp.transpose(conv_grad, (1, 0, 2)).reshape(SEQLEN, INNER)
    grad_gate = jnp.transpose(gate_grad, (1, 0, 2)).reshape(SEQLEN, INNER)
    grad_conv_weight = jnp.transpose(weight_grad, (1, 0, 2)).reshape(KERNEL, INNER)
    return (grad_conv_input, grad_gate, step_grad.T, sum_in, sum_out, grad_conv_weight, bias_grad, rate_grad, skip_grad)

def reference(queries, keys, values, attn_grad, doc_ids, conv_input, conv_weight, step_raw, step_bias, rate_log, skip_gain, input_coeff, output_coeff, gate_input, mix_grad):
    grad_queries, grad_keys, grad_values = attention_grads(queries, keys, values, attn_grad, doc_ids)
    grad_conv_input, grad_gate, grad_step, grad_input_coeff, grad_output_coeff, grad_conv_weight, grad_step_bias, grad_rate_log, grad_skip = mixer_grads(doc_ids, conv_input, conv_weight, step_raw, step_bias, rate_log, skip_gain, input_coeff, output_coeff, gate_input, mix_grad)
    return (grad_queries, grad_keys, grad_values, grad_conv_input, grad_gate, grad_step, grad_input_coeff, grad_output_coeff, grad_conv_weight, grad_step_bias, grad_rate_log, grad_skip)
```

```python
import jax
import jax.numpy as jnp
from jax import lax
from jax.experimental import pallas as pl
from jax.experimental.pallas import tpu as pltpu
from jax.sharding import PartitionSpec as P

HEAD_DIM = 224
WINDOW = 1024
KERNEL = 4
PAD = 8
LANES = 128
PLACES = 4
DOCS = 8
REACH = 4

EXACT = lax.Precision.HIGHEST
F32 = jnp.float32
BF16 = jnp.bfloat16
NEG_FILL = -1e30
SCALE = HEAD_DIM ** (-0.5)


def dot(a, b, ca, cb, precision=None):
    return lax.dot_general(
        a, b, (((ca,), (cb,)), ((), ())), preferred_element_type=F32, precision=precision
    )


def where_am_i():
    index = lax.axis_index("seq")
    groups = lax.axis_size("seq") // PLACES
    return lax.div(index, PLACES), lax.rem(index, PLACES), groups


def shard(group, place, groups):
    return {"seq": lax.rem(group + 2 * groups, groups) * PLACES + place}


def greet(partners):
    barrier = pltpu.get_barrier_semaphore()
    for partner in partners:
        pl.semaphore_signal(barrier, inc=1, device_id=partner, device_id_type=pl.DeviceIdType.MESH)
    return lambda: pl.semaphore_wait(barrier, len(partners))


class Post:
    def __init__(self, sends, receives):
        self.sends, self.receives, self.used = sends, receives, 0

    def send(self, source, target, device):
        copy = pltpu.make_async_remote_copy(
            src_ref=source, dst_ref=target, send_sem=self.sends.at[self.used],
            recv_sem=self.receives.at[self.used], device_id=device,
            device_id_type=pl.DeviceIdType.MESH,
        )
        self.used += 1
        copy.start()
        return copy


def spreader(heads, channels):
    width = channels // heads
    row = lax.broadcasted_iota(jnp.int32, (LANES, channels), 0)
    col = lax.broadcasted_iota(jnp.int32, (LANES, channels), 1)
    return ((col >= row * width) & (col < row * width + width)).astype(F32)


def causal(rows):
    i = lax.broadcasted_iota(jnp.int32, (rows, rows), 0)
    j = lax.broadcasted_iota(jnp.int32, (rows, rows), 1)
    return i, j


def pair_columns(cols, index, lower):
    return jnp.where(lower, cols[:, 2 * index : 2 * index + 1], cols[:, 2 * index + 1 : 2 * index + 2])


def fill_masks(since_ref, mask_ref):
    for lag in range(1, KERNEL):
        mask_ref[lag - 1] = jnp.broadcast_to((since_ref[...] >= lag).astype(F32), mask_ref.shape[1:])


def conv_pre(conv, tail, wt, mask_ref, xp_ref):
    rows = conv.shape[0]
    xp_ref[:PAD, :] = tail.astype(F32)[PAD:]
    xp_ref[PAD:, :] = conv.astype(F32)
    pre = wt[0:1, :] * xp_ref[PAD:, :]
    for lag in range(1, KERNEL):
        pre = pre + wt[lag : lag + 1, :] * (xp_ref[PAD - lag : PAD - lag + rows, :] * mask_ref[lag - 1])
    return pre


def group_part(ref):
    half = ref.shape[1] // 2
    whole = ref[...].astype(F32)
    first = lax.axis_index("head") < lax.axis_size("head") // 2
    return jnp.where(first, whole[:, :half], whole[:, half:]).astype(BF16)


def pre_kernel(
    q_ref, k_ref, v_ref, do_ref, since_ref, step_ref, bias_ref, rate_ref, b_ref, c_ref, wt_ref,
    conv_hbm, gate_hbm, mix_hbm,
    recv_ref, prev_ref, cols_ref, rowc_ref, through_ref, state_ref, tail_ref,
    pack_ref, conv_ref, gate_ref, mix_ref, tail_buf, spread_ref, mask_ref, xp_ref,
    ends_ref, a_ref, end_out, cot_out, g_out, e_in, c_in, ge_in, gc_in, back_ref, state_buf, t_out, t_all,
    sends, receives, loads, locals_,
):
    group, place, groups = where_am_i()
    rows, heads = step_ref.shape
    channels = conv_ref.shape[1]
    pairs = channels // LANES
    peers = [lax.rem(place + d, PLACES) for d in range(1, PLACES)]
    post = Post(sends, receives)
    partners = [shard(group, peer, groups) for peer in peers]
    partners += [shard(group + side, other, groups) for side in (1, -1) for other in range(PLACES)]
    partners += [shard(group + far, place, groups) for far in range(2, groups - 1)]
    wait_partners = greet(partners)

    fetches = [
        pltpu.make_async_copy(source, target, loads.at[n])
        for n, (source, target) in enumerate(
            ((conv_hbm, conv_ref), (gate_hbm, gate_ref), (mix_hbm, mix_ref))
        )
    ]
    for fetch in fetches:
        fetch.start()
    for n, ref in enumerate((q_ref, do_ref, k_ref, v_ref)):
        for r in range(PLACES):
            pack_ref[r, :, n * HEAD_DIM : (n + 1) * HEAD_DIM] = ref[:, r * HEAD_DIM : (r + 1) * HEAD_DIM]
    fetches[0].wait()
    wait_partners()

    last = place == PLACES - 1
    follower = shard(jnp.where(last, group + 1, group), lax.rem(place + 1, PLACES), groups)
    tail_copy = post.send(conv_ref.at[rows - 2 * PAD :, :], tail_buf, follower)
    bulk = []
    for r in [place] + peers:
        bulk.append(post.send(pack_ref.at[r, :, 3 * LANES :], prev_ref.at[place], shard(group + 1, r, groups)))
    for peer in peers:
        bulk.append(post.send(pack_ref.at[peer], recv_ref.at[place], shard(group, peer, groups)))
    keep = pltpu.make_async_copy(pack_ref.at[place], recv_ref.at[place], locals_.at[0])
    keep.start()

    since = since_ref[...]
    raw = step_ref[...] + bias_ref[...]
    step = jnp.maximum(raw, 0.0) + jnp.log1p(jnp.exp(-jnp.abs(raw)))
    log_decay = -step * jnp.exp(rate_ref[...])
    i, j = causal(rows)
    tri = (i >= j).astype(F32)
    cum = dot(tri, log_decay, 1, 0, EXACT)
    row_cum = dot(log_decay, tri, 0, 1, EXACT)
    t = lax.broadcasted_iota(jnp.int32, (rows, 1), 0).astype(F32)
    enter = jnp.where(since > t, jnp.exp(cum), 0.0)
    final = cum[rows - 1 : rows]
    to_end = jnp.where((rows - 1) - t <= since[rows - 1 : rows], jnp.exp(final - cum), 0.0)
    through = enter[rows - 1 : rows]
    t_out[...] = jnp.zeros_like(t_out)
    t_out[0:1, 0:heads] = through
    through_ref[...] = through
    t_all[place] = t_out[...]
    t_copies = [post.send(t_out, t_all.at[place], shard(group, peer, groups)) for peer in peers]
    for n in range(pairs):
        two = slice(2 * n, 2 * n + 2)
        cols_ref[n] = jnp.concatenate([cum[:, two], step[:, two], enter[:, two], to_end[:, two]], axis=1)
        rowc_ref[n] = row_cum[two]
    spread_ref[...] = spreader(heads, channels)
    fill_masks(since_ref, mask_ref)
    lower = lax.broadcasted_iota(jnp.int32, (rows, LANES), 1) < LANES // 2
    b_part, c_part = group_part(b_ref), group_part(c_ref)
    fetches[1].wait()
    fetches[2].wait()
    tail_copy.wait()
    tail_ref[...] = tail_buf[...]

    def ends(n, carry):
        lanes = pl.ds(pl.multiple_of(n * LANES, LANES), LANES)
        cols = cols_ref[n]
        pre = conv_pre(conv_ref[:, lanes], tail_buf[:, lanes], wt_ref[:, lanes], mask_ref, xp_ref)
        act = pre * jax.nn.sigmoid(pre)
        weighted = act * pair_columns(cols, 1, lower) * pair_columns(cols, 3, lower)
        end = dot(b_part, weighted.astype(BF16), 0, 0).astype(BF16)
        gate = gate_ref[:, lanes].astype(F32)
        dy = mix_ref[:, lanes].astype(F32) * (gate * jax.nn.sigmoid(gate))
        start = dot(c_part, (dy * pair_columns(cols, 2, lower)).astype(BF16), 0, 0).astype(BF16)
        for r in range(PLACES):
            part = slice(2 * PAD * r, 2 * PAD * (r + 1))
            ends_ref[r, 0, :, lanes] = end[part]
            ends_ref[r, 1, :, lanes] = start[part]
        return carry

    lax.fori_loop(0, pairs, ends, 0)

    a_copies = [post.send(ends_ref.at[peer], a_ref.at[place], shard(group, peer, groups)) for peer in peers]
    a_ref[place] = ends_ref[place]
    for copy in t_copies + a_copies:
        copy.wait()
    decays = dot(t_all[...].reshape(PLACES * PAD, LANES), spread_ref[...], 1, 0, EXACT)
    decay = [decays[PAD * n : PAD * n + 1] for n in range(PLACES)]
    end_of = lambda n: a_ref[n, 0].astype(F32)
    cot_of = lambda n: a_ref[n, 1].astype(F32)
    end, cot = end_of(0), cot_of(PLACES - 1)
    for n in range(1, PLACES):
        end = end_of(n) + decay[n] * end
        cot = cot_of(PLACES - 1 - n) + decay[PLACES - 1 - n] * cot
    end_out[...] = end.astype(BF16)
    cot_out[...] = cot.astype(BF16)
    g_out[...] = t_all[0] * t_all[1] * t_all[2] * t_all[3]
    b_copies = []
    for far in range(1, REACH + 1):
        later, earlier = shard(group + far, place, groups), shard(group - far, place, groups)
        b_copies.append(post.send(end_out, e_in.at[far - 1], later))
        b_copies.append(post.send(g_out, ge_in.at[far - 1], later))
        b_copies.append(post.send(cot_out, c_in.at[far - 1], earlier))
        b_copies.append(post.send(g_out, gc_in.at[far - 1], earlier))
    for copy in b_copies:
        copy.wait()
    before = dot(ge_in[...].reshape(REACH * PAD, LANES), spread_ref[...], 1, 0, EXACT)
    after = dot(gc_in[...].reshape(REACH * PAD, LANES), spread_ref[...], 1, 0, EXACT)
    state = e_in[REACH - 1].astype(F32)
    cot = c_in[REACH - 1].astype(F32) * (group + REACH < groups).astype(F32)
    for far in range(REACH - 2, -1, -1):
        state = e_in[far].astype(F32) + before[PAD * far : PAD * far + 1] * state
        cot = (c_in[far].astype(F32) + after[PAD * far : PAD * far + 1] * cot) * (
            group + far + 1 < groups
        ).astype(F32)
    for n in range(PLACES):
        back_ref[n, 0] = state.astype(BF16)
        state = end_of(n) + decay[n] * state
        m = PLACES - 1 - n
        back_ref[m, 1] = cot.astype(BF16)
        cot = cot_of(m) + decay[m] * cot
    final_copies = [
        post.send(back_ref.at[peer], state_buf.at[place], shard(group, peer, groups)) for peer in peers
    ]
    state_buf[place] = back_ref[place]
    for copy in final_copies:
        copy.wait()
    state_ref[...] = state_buf[...]
    for copy in bulk:
        copy.wait()
    keep.wait()


def attn_kernel(low_ref, recv_ref, prev_ref, own_ref, back_ref, q_all, do_all, k_all, v_all, dk_all, dv_all):
    places, rows, _ = recv_ref.shape
    span = places * rows
    for r in range(places):
        here, later = slice(r * rows, (r + 1) * rows), slice(span + r * rows, span + (r + 1) * rows)
        q_all[here, :] = recv_ref[r, :, 0:HEAD_DIM]
        do_all[here, :] = recv_ref[r, :, HEAD_DIM : 2 * HEAD_DIM]
        k_all[later, :] = recv_ref[r, :, 2 * HEAD_DIM : 3 * HEAD_DIM]
        v_all[later, :] = recv_ref[r, :, 3 * HEAD_DIM : 4 * HEAD_DIM]
        skip = 2 * HEAD_DIM - 3 * LANES
        k_all[here, :] = prev_ref[r, :, skip : skip + HEAD_DIM]
        v_all[here, :] = prev_ref[r, :, skip + HEAD_DIM : skip + 2 * HEAD_DIM]
    dk_all[...] = jnp.zeros_like(dk_all)
    dv_all[...] = jnp.zeros_like(dv_all)
    j = lax.broadcasted_iota(jnp.int32, (rows, rows), 0)
    i = lax.broadcasted_iota(jnp.int32, (rows, rows), 1)

    def block(b, carry):
        mine = pl.ds(pl.multiple_of(b * rows, rows), rows)
        q = q_all[mine, :]
        grad = do_all[mine, :]
        low = low_ref[pl.ds(b, 1), :]
        at = [pl.ds(pl.multiple_of((b + places - gap) * rows, rows), rows) for gap in range(places + 1)]
        scores = []
        top = None
        for gap in range(places + 1):
            allowed = j + (b + places - gap) * rows >= low
            if gap == 0:
                allowed = allowed & (i >= j)
            s = jnp.where(allowed, dot(k_all[at[gap], :], q, 1, 1) * SCALE, NEG_FILL)
            scores.append(s)
            m = jnp.max(s, axis=0, keepdims=True)
            top = m if top is None else jnp.maximum(top, m)
        total = None
        expo = []
        for gap in range(places + 1):
            e = jnp.exp(scores[gap] - top)
            expo.append(e)
            t = jnp.sum(e, axis=0, keepdims=True)
            total = t if total is None else total + t
        inverse = 1.0 / jnp.maximum(total, 1.0)
        delta = None
        dprobs = []
        for gap in range(places + 1):
            half = (expo[gap] * inverse).astype(BF16)
            dp = dot(v_all[at[gap], :], grad, 1, 1)
            d = jnp.sum(half.astype(F32) * dp, axis=0, keepdims=True)
            delta = d if delta is None else delta + d
            dv_all[at[gap], :] += dot(half, grad, 1, 0)
            dprobs.append(dp)
        dq = None
        for gap in range(places + 1):
            ds = (expo[gap] * inverse * (dprobs[gap] - delta)).astype(BF16)
            dk_all[at[gap], :] += dot(ds, q, 1, 0)
            part = dot(ds, k_all[at[gap], :], 0, 0)
            dq = part if dq is None else dq + part
        own_ref[b, :, 0:HEAD_DIM] = (dq * SCALE).astype(BF16)
        return carry

    lax.fori_loop(0, places, block, 0)
    for r in range(places):
        here, later = slice(r * rows, (r + 1) * rows), slice(span + r * rows, span + (r + 1) * rows)
        own_ref[r, :, HEAD_DIM : 2 * HEAD_DIM] = dk_all[later, :].astype(BF16)
        own_ref[r, :, 2 * HEAD_DIM : 3 * HEAD_DIM] = dv_all[later, :].astype(BF16)
        own_ref[r, :, 3 * HEAD_DIM :] = jnp.zeros((rows, own_ref.shape[2] - 3 * HEAD_DIM), BF16)
        back_ref[r, :, 0:HEAD_DIM] = dk_all[here, :].astype(BF16)
        back_ref[r, :, HEAD_DIM : 2 * HEAD_DIM] = dv_all[here, :].astype(BF16)
        back_ref[r, :, 2 * HEAD_DIM :] = jnp.zeros((rows, back_ref.shape[2] - 2 * HEAD_DIM), BF16)


def post_kernel(
    since_ref, step_ref, bias_ref, rate_ref, b_ref, c_ref, wt_ref, conv_ref, gate_ref, mix_ref, tail_ref,
    cols_ref, rowc_ref, through_ref, state_ref, own_ref, back_ref,
    ret_own, ret_back, gconv_ref, ggate_ref, gstep_ref, gin_ref, gout_ref, total_ref,
    mask_ref, xp_ref, mix_bias, pair_ref, dpair_ref, dpad_ref, z_ref, u_ref, db_ref, dc_ref, spread_ref,
    sums_ref, edge_ref, end_ref, spill_ref, coef_out, coef_all, red_out, red_a, red_mid, red_b, own_buf,
    sends, receives, locals_,
):
    group, place, groups = where_am_i()
    head, head_count = lax.axis_index("head"), lax.axis_size("head")
    rows, heads = step_ref.shape
    channels = conv_ref.shape[1]
    pairs = channels // LANES
    peers = [lax.rem(place + d, PLACES) for d in range(1, PLACES)]
    post = Post(sends, receives)
    partners = [shard(group, peer, groups) for peer in peers]
    partners += [shard(group + side, other, groups) for side in (1, -1) for other in range(PLACES)]
    partners += [shard(group + far, place, groups) for far in range(2, groups - 1)]
    head_peers = [{"head": lax.rem(head + d, head_count)} for d in range(1, head_count)]
    wait_partners = greet(partners + head_peers)
    keep_in = pltpu.make_async_copy(own_ref.at[place], own_buf, locals_.at[0])
    keep_in.start()
    wait_partners()
    bulk = []
    for r in [place] + peers:
        bulk.append(post.send(back_ref.at[r], ret_back.at[place], shard(group - 1, r, groups)))
    for peer in peers:
        bulk.append(post.send(own_ref.at[peer], ret_own.at[place], shard(group, peer, groups)))
    keep_in.wait()
    keep_out = pltpu.make_async_copy(own_buf, ret_own.at[place], locals_.at[1])
    keep_out.start()

    fill_masks(since_ref, mask_ref)
    i, j = causal(rows)
    since = since_ref[...]
    mix_bias[...] = jnp.where((i >= j) & ((i - j).astype(F32) <= since), 0.0, NEG_FILL)
    b_part, c_part = group_part(b_ref), group_part(c_ref)
    pair_ref[...] = dot(c_part, b_part, 1, 1)
    spread_ref[...] = spreader(heads, channels)
    for ref in (dpair_ref, z_ref, u_ref, db_ref, dc_ref, dpad_ref):
        ref[...] = jnp.zeros_like(ref)
    lower = lax.broadcasted_iota(jnp.int32, (rows, LANES), 1) < LANES // 2
    lane = lax.broadcasted_iota(jnp.int32, (rows, heads), 1)

    def mixer(n, carry):
        lanes = pl.ds(pl.multiple_of(n * LANES, LANES), LANES)
        cols = cols_ref[n]
        wt = wt_ref[:, lanes]
        size = pair_columns(cols, 1, lower)
        enter = pair_columns(cols, 2, lower)
        to_end = pair_columns(cols, 3, lower)
        pre = conv_pre(conv_ref[:, lanes], tail_ref[:, lanes], wt, mask_ref, xp_ref)
        sig_pre = jax.nn.sigmoid(pre)
        act = pre * sig_pre
        x_half = (act * size).astype(BF16)
        gate = gate_ref[:, lanes].astype(F32)
        sig_gate = jax.nn.sigmoid(gate)
        silu_gate = gate * sig_gate
        cot = mix_ref[:, lanes].astype(F32)
        dy = cot * silu_gate
        dy_half = dy.astype(BF16)
        state = jnp.concatenate([state_ref[r, 0, :, lanes] for r in range(PLACES)], axis=0)
        end_cot = jnp.concatenate([state_ref[r, 1, :, lanes] for r in range(PLACES)], axis=0)
        zero = jnp.zeros_like(dy_half)
        y_parts, dx_parts = [], []
        dpair = dpair_ref[...]
        rowc = rowc_ref[n]
        for k in range(2):
            weights = jnp.exp((cols[:, k : k + 1] - rowc[k : k + 1, :]) + mix_bias[...])
            mixing = (pair_ref[...] * weights).astype(BF16)
            y_parts.append(dot(mixing, x_half, 1, 0))
            dx_parts.append(dot(mixing, dy_half, 0, 0))
            dy_one = jnp.where(lower if k == 0 else ~lower, dy_half, zero)
            dpair = dpair + dot(dy_one, x_half, 1, 1) * weights
        dpair_ref[...] = dpair
        inner = jnp.where(lower, y_parts[0], y_parts[1]) + enter * dot(c_part, state, 1, 0)
        end_part = to_end * dot(b_part, end_cot, 1, 0)
        dx = jnp.where(lower, dx_parts[0], dx_parts[1]) + end_part
        skip = wt[KERNEL : KERNEL + 1, :]
        y = inner + skip * act
        ggate_ref[:, lanes] = (cot * y * (sig_gate + silu_gate * (1.0 - sig_gate))).astype(BF16)
        x_wide = x_half.astype(F32)
        zed = dy_half.astype(F32) * inner - x_wide * dx
        you = dx * act
        for k in range(2):
            side = lower if k == 0 else ~lower
            here = lane == 2 * n + k
            z_one = jnp.sum(jnp.where(side, zed, 0.0), axis=1, keepdims=True)
            u_one = jnp.sum(jnp.where(side, you, 0.0), axis=1, keepdims=True)
            z_ref[...] = jnp.where(here, z_one, z_ref[...])
            u_ref[...] = jnp.where(here, u_one, u_ref[...])
        dc_ref[...] += dot((enter * dy).astype(BF16), state, 1, 1)
        db_ref[...] += dot((to_end * x_wide).astype(BF16), end_cot, 1, 1)
        dact = dx * size + skip * dy
        dpre = dact * (sig_pre + act * (1.0 - sig_pre))
        sums_ref[0:1, lanes] = jnp.sum(dpre * xp_ref[PAD:, :], axis=0, keepdims=True)
        dpad_ref[0, PAD : PAD + rows, :] = dpre
        grown = wt[0:1, :] * dpad_ref[0, 0 : rows + PAD, :]
        for lag in range(1, KERNEL):
            masked = dpre * mask_ref[lag - 1]
            sums_ref[lag : lag + 1, lanes] = jnp.sum(
                masked * xp_ref[PAD - lag : PAD - lag + rows, :], axis=0, keepdims=True
            )
            dpad_ref[lag, PAD : PAD + rows, :] = masked
            grown = grown + wt[lag : lag + 1, :] * dpad_ref[lag, lag : lag + rows + PAD, :]
        gconv_ref[:, lanes] = grown[PAD:, :].astype(BF16)
        edge_ref[:, lanes] = grown[:PAD, :]
        end_ref[:, lanes] = grown[rows:, :]
        sums_ref[4:5, lanes] = jnp.sum(dy * act, axis=0, keepdims=True)
        sums_ref[5:6, lanes] = jnp.sum(state.astype(F32) * end_cot.astype(F32), axis=0, keepdims=True)
        sums_ref[6:7, lanes] = jnp.sum(x_wide * end_part, axis=0, keepdims=True)
        sums_ref[7:8, lanes] = jnp.zeros((1, LANES), F32)
        return carry

    lax.fori_loop(0, pairs, mixer, 0)

    first = place == 0
    former = shard(jnp.where(first, group - 1, group), lax.rem(place + PLACES - 1, PLACES), groups)
    spill_copy = post.send(edge_ref, spill_ref, former)
    raw = step_ref[...] + bias_ref[...]
    step = jnp.maximum(raw, 0.0) + jnp.log1p(jnp.exp(-jnp.abs(raw)))
    rate = jnp.exp(rate_ref[...])
    tri = (i >= j).astype(F32)
    per_head = dot(sums_ref[...], spread_ref[...], 1, 1, EXACT)[:, 0:heads]
    last_row = per_head[6:7] + through_ref[...] * per_head[5:6]
    t = lax.broadcasted_iota(jnp.int32, (rows, 1), 0)
    dcum = z_ref[...] + jnp.where(t == rows - 1, last_row, 0.0)
    dlog = dot(tri, dcum, 0, 0, EXACT)
    grad_step = (u_ref[...] - dlog * rate) * jax.nn.sigmoid(raw)
    gstep_ref[...] = grad_step
    red_out[...] = jnp.where(
        lax.broadcasted_iota(jnp.int32, red_out.shape, 0) < KERNEL, sums_ref[...], 0.0
    )
    red_out[4:5, 0:heads] = jnp.sum(grad_step, axis=0, keepdims=True)
    red_out[5:6, 0:heads] = jnp.sum(dlog * (-step * rate), axis=0, keepdims=True)
    red_out[6:7, 0:heads] = per_head[4:5]
    near = [post.send(red_out, red_a.at[place], shard(group, peer, groups)) for peer in peers]
    red_a[place] = red_out[...]
    dpair = dpair_ref[...]
    dc_ref[...] += dot(dpair, b_part.astype(F32), 1, 0, EXACT)
    db_ref[...] += dot(dpair, c_part.astype(F32), 0, 0, EXACT)
    coef_out[...] = jnp.concatenate([db_ref[...], dc_ref[...]], axis=1).astype(BF16)
    coefs = [post.send(coef_out, coef_all.at[head], peer) for peer in head_peers]
    coef_all[head] = coef_out[...]
    for copy in near:
        copy.wait()
    red_mid[...] = red_a[0] + red_a[1] + red_a[2] + red_a[3]
    wide = [
        post.send(red_mid, red_b.at[group], shard(group + far, place, groups)) for far in range(1, groups)
    ]
    red_b[group] = red_mid[...]
    spill_copy.wait()
    gconv_ref[rows - PAD :, :] = (end_ref[...] + spill_ref[...]).astype(BF16)
    for copy in coefs:
        copy.wait()
    halves = [coef_all[2 * n].astype(F32) + coef_all[2 * n + 1].astype(F32) for n in range(2)]
    half = coef_out.shape[1] // 2
    gin_ref[...] = jnp.concatenate([halves[0][:, :half], halves[1][:, :half]], axis=1)
    gout_ref[...] = jnp.concatenate([halves[0][:, half:], halves[1][:, half:]], axis=1)
    for copy in wide:
        copy.wait()
    total = red_b[0]
    for n in range(1, groups):
        total = total + red_b[n]
    total_ref[...] = total
    for copy in bulk:
        copy.wait()
    keep_out.wait()


def unpack_kernel(own_ref, back_ref, dq_ref, dk_ref, dv_ref):
    for r in range(own_ref.shape[0]):
        cols = slice(r * HEAD_DIM, (r + 1) * HEAD_DIM)
        dq_ref[:, cols] = own_ref[r, :, 0:HEAD_DIM]
        key = own_ref[r, :, HEAD_DIM : 2 * HEAD_DIM].astype(F32) + back_ref[r, :, 0:HEAD_DIM].astype(F32)
        dk_ref[:, cols] = (key * SCALE).astype(BF16)
        value = own_ref[r, :, 2 * HEAD_DIM : 3 * HEAD_DIM].astype(F32)
        dv_ref[:, cols] = (value + back_ref[r, :, HEAD_DIM : 2 * HEAD_DIM].astype(F32)).astype(BF16)


def local(
    queries, keys, values, attn_grad, doc_ids, conv_input, conv_weight, step_raw, step_bias,
    rate_log, skip_gain, input_coeff, output_coeff, gate_input, mix_grad,
):
    rows, width = queries.shape
    heads, channels = step_raw.shape[1], conv_input.shape[1]
    pairs = channels // LANES
    index = lax.axis_index("seq")
    groups = lax.axis_size("seq") // PLACES
    base = (index // PLACES) * PLACES * rows
    counts = jnp.sum(doc_ids[None, :] < jnp.arange(DOCS)[:, None], axis=1)
    docs = lax.dynamic_slice_in_dim(doc_ids, base, PLACES * rows)
    start = jnp.sum(jnp.where(docs[None, :] == jnp.arange(DOCS)[:, None], counts[:, None], 0), axis=0)
    where = base + jnp.arange(PLACES * rows, dtype=jnp.int32)
    low = (jnp.maximum(start, where - (WINDOW - 1)) - base + WINDOW).reshape(PLACES, rows)
    since = lax.dynamic_slice_in_dim(where - start, index % PLACES * rows, rows).astype(F32)[:, None]
    wt = jnp.concatenate(
        [conv_weight, jnp.repeat(skip_gain, channels // heads)[None], jnp.zeros((7 - KERNEL, channels), F32)]
    )
    bias, rate = step_bias[None], rate_log[None]

    struct = jax.ShapeDtypeStruct
    vmem = pl.BlockSpec(memory_space=pltpu.VMEM)
    loose = pl.BlockSpec(memory_space=pl.ANY)
    dma = lambda n: pltpu.SemaphoreType.DMA((n,))
    params = lambda n: pltpu.CompilerParams(
        collective_id=n, has_side_effects=True, vmem_limit_bytes=56 * 1024 * 1024
    )
    packed, key_cols = 4 * HEAD_DIM, 4 * LANES
    quarter = (2, 2 * PAD, channels)
    part = quarter[1:]
    recv, prev, cols, rowc, through, state, tail = pl.pallas_call(
        pre_kernel,
        in_specs=[vmem] * 11 + [loose] * 3,
        out_specs=[loose] * 2 + [vmem] * 5,
        out_shape=[
            struct((PLACES, rows, packed), BF16), struct((PLACES, rows, key_cols), BF16),
            struct((pairs, rows, 8), F32), struct((pairs, 2, rows), F32), struct((1, heads), F32),
            struct((PLACES, *quarter), BF16), struct((2 * PAD, channels), BF16),
        ],
        scratch_shapes=[
            pltpu.VMEM((PLACES, rows, packed), BF16),
            pltpu.VMEM((rows, channels), BF16), pltpu.VMEM((rows, channels), BF16),
            pltpu.VMEM((rows, channels), BF16), pltpu.VMEM((2 * PAD, channels), BF16),
            pltpu.VMEM((LANES, channels), F32), pltpu.VMEM((KERNEL - 1, rows, LANES), F32),
            pltpu.VMEM((rows + PAD, LANES), F32),
            pltpu.VMEM((PLACES, *quarter), BF16), pltpu.VMEM((PLACES, *quarter), BF16),
            pltpu.VMEM(part, BF16), pltpu.VMEM(part, BF16), pltpu.VMEM((PAD, LANES), F32),
            pltpu.VMEM((REACH, *part), BF16), pltpu.VMEM((REACH, *part), BF16),
            pltpu.VMEM((REACH, PAD, LANES), F32), pltpu.VMEM((REACH, PAD, LANES), F32),
            pltpu.VMEM((PLACES, *quarter), BF16), pltpu.VMEM((PLACES, *quarter), BF16),
            pltpu.VMEM((PAD, LANES), F32), pltpu.VMEM((PLACES, PAD, LANES), F32),
            dma(33), dma(33), dma(3), dma(1),
        ],
        name="pre",
        compiler_params=params(0),
    )(
        queries, keys, values, attn_grad, since, step_raw, bias, rate, input_coeff, output_coeff, wt,
        conv_input, gate_input, mix_grad,
    )
    span = PLACES * rows
    own, back = pl.pallas_call(
        attn_kernel,
        in_specs=[vmem] * 3,
        out_specs=[vmem] * 2,
        out_shape=[struct((PLACES, rows, 6 * LANES), BF16), struct((PLACES, rows, key_cols), BF16)],
        scratch_shapes=[
            pltpu.VMEM((span, HEAD_DIM), BF16), pltpu.VMEM((span, HEAD_DIM), BF16),
            pltpu.VMEM((2 * span, HEAD_DIM), BF16), pltpu.VMEM((2 * span, HEAD_DIM), BF16),
            pltpu.VMEM((2 * span, HEAD_DIM), F32), pltpu.VMEM((2 * span, HEAD_DIM), F32),
        ],
        name="attn",
        compiler_params=pltpu.CompilerParams(vmem_limit_bytes=56 * 1024 * 1024),
    )(low, recv, prev)
    wide_buf = lambda n: pltpu.VMEM((n, PAD, channels), F32)
    flat = pltpu.VMEM((PAD, channels), F32)
    ret_own, ret_back, gconv, ggate, gstep, gin, gout, total = pl.pallas_call(
        post_kernel,
        in_specs=[vmem] * 15 + [loose] * 2,
        out_specs=[loose] * 2 + [vmem] * 6,
        out_shape=[
            struct((PLACES, rows, 6 * LANES), BF16), struct((PLACES, rows, key_cols), BF16),
            struct((rows, channels), BF16), struct((rows, channels), BF16), struct((rows, heads), F32),
            struct((rows, LANES), F32), struct((rows, LANES), F32), struct((PAD, channels), F32),
        ],
        scratch_shapes=[
            pltpu.VMEM((KERNEL - 1, rows, LANES), F32), pltpu.VMEM((rows + PAD, LANES), F32),
            pltpu.VMEM((rows, rows), F32), pltpu.VMEM((rows, rows), F32), pltpu.VMEM((rows, rows), F32),
            pltpu.VMEM((KERNEL, rows + 2 * PAD, LANES), F32),
            pltpu.VMEM((rows, heads), F32), pltpu.VMEM((rows, heads), F32),
            pltpu.VMEM((rows, LANES // 2), F32), pltpu.VMEM((rows, LANES // 2), F32),
            pltpu.VMEM((LANES, channels), F32),
            flat, flat, flat, flat,
            pltpu.VMEM((rows, LANES), BF16), pltpu.VMEM((4, rows, LANES), BF16),
            flat, wide_buf(PLACES), flat, wide_buf(groups),
            pltpu.VMEM((rows, 6 * LANES), BF16),
            dma(21), dma(21), dma(2),
        ],
        name="post",
        compiler_params=params(1),
    )(
        since, step_raw, bias, rate, input_coeff, output_coeff, wt, conv_input, gate_input, mix_grad, tail,
        cols, rowc, through, state, own, back,
    )
    dq, dk, dv = pl.pallas_call(
        unpack_kernel,
        in_specs=[vmem] * 2,
        out_specs=[vmem] * 3,
        out_shape=[struct((rows, width), BF16)] * 3,
        name="unpack",
    )(ret_own, ret_back)
    return (
        dq, dk, dv, gconv, ggate, gstep, gin, gout, total[:KERNEL],
        total[4, :heads], total[5, :heads], total[6, :heads],
    )


def solution(mesh):
    sharded = P("seq", "head")
    return jax.shard_map(
        local,
        mesh=mesh,
        in_specs=(
            sharded, sharded, sharded, sharded, P(), sharded, P(None, "head"), sharded,
            P("head"), P("head"), P("head"), P("seq", None), P("seq", None), sharded, sharded,
        ),
        out_specs=(
            sharded, sharded, sharded, sharded, sharded, sharded,
            P("seq", None), P("seq", None), P(None, "head"), P("head"), P("head"), P("head"),
        ),
        check_vma=False,
    )
```

```python
import jax
import jax.numpy as jnp
from jax import lax
from jax.experimental import pallas as pl
from jax.experimental.pallas import tpu as pltpu
from jax.sharding import PartitionSpec as P

HEAD_DIM = 224
WINDOW = 1024
KERNEL = 4
PAD = 8
LANES = 128
PLACES = 4
DOCS = 8
REACH = 4

EXACT = lax.Precision.HIGHEST
F32 = jnp.float32
BF16 = jnp.bfloat16
NEG_FILL = -1e30
SENDS = 56
SCALE = HEAD_DIM ** (-0.5)


def dot(a, b, ca, cb, precision=None):
    return lax.dot_general(
        a, b, (((ca,), (cb,)), ((), ())), preferred_element_type=F32, precision=precision
    )


def where_am_i():
    index = lax.axis_index("seq")
    groups = lax.axis_size("seq") // PLACES
    return lax.div(index, PLACES), lax.rem(index, PLACES), groups


def shard(group, place, groups):
    return {"seq": lax.rem(group + 2 * groups, groups) * PLACES + place}


def greet(partners):
    barrier = pltpu.get_barrier_semaphore()
    for partner in partners:
        pl.semaphore_signal(barrier, inc=1, device_id=partner, device_id_type=pl.DeviceIdType.MESH)
    return lambda: pl.semaphore_wait(barrier, len(partners))


class Post:
    def __init__(self, sends, receives):
        self.sends, self.receives, self.used = sends, receives, 0

    def send(self, source, target, device):
        copy = pltpu.make_async_remote_copy(
            src_ref=source, dst_ref=target, send_sem=self.sends.at[self.used],
            recv_sem=self.receives.at[self.used], device_id=device,
            device_id_type=pl.DeviceIdType.MESH,
        )
        self.used += 1
        copy.start()
        return copy


def spreader(heads, channels):
    width = channels // heads
    row = lax.broadcasted_iota(jnp.int32, (LANES, channels), 0)
    col = lax.broadcasted_iota(jnp.int32, (LANES, channels), 1)
    return ((col >= row * width) & (col < row * width + width)).astype(F32)


def causal(rows):
    i = lax.broadcasted_iota(jnp.int32, (rows, rows), 0)
    j = lax.broadcasted_iota(jnp.int32, (rows, rows), 1)
    return i, j


def pair_columns(cols, index, lower):
    return jnp.where(lower, cols[:, 2 * index : 2 * index + 1], cols[:, 2 * index + 1 : 2 * index + 2])


def fill_masks(since_ref, mask_ref):
    for lag in range(1, KERNEL):
        mask_ref[lag - 1] = jnp.broadcast_to((since_ref[...] >= lag).astype(F32), mask_ref.shape[1:])


def conv_pre(conv, tail, wt, mask_ref, xp_ref):
    rows = conv.shape[0]
    xp_ref[:PAD, :] = tail.astype(F32)[PAD:]
    xp_ref[PAD:, :] = conv.astype(F32)
    pre = wt[0:1, :] * xp_ref[PAD:, :]
    for lag in range(1, KERNEL):
        pre = pre + wt[lag : lag + 1, :] * (xp_ref[PAD - lag : PAD - lag + rows, :] * mask_ref[lag - 1])
    return pre


def group_part(ref):
    half = ref.shape[1] // 2
    whole = ref[...].astype(F32)
    first = lax.axis_index("head") < lax.axis_size("head") // 2
    return jnp.where(first, whole[:, :half], whole[:, half:]).astype(BF16)


def whole_kernel(
    since_ref, low_ref, step_ref, bias_ref, rate_ref, b_ref, c_ref, wt_ref,
    k_hbm, v_hbm, q_hbm, do_hbm, conv_hbm, gate_hbm, mix_hbm,
    dq_ref, dk_ref, dv_ref, gconv_ref, ggate_ref, gstep_ref, gin_ref, gout_ref, total_ref,
    k_ref, v_ref, q_ref, do_ref, conv_ref, gate_ref, mix_ref,
    pack_ref, recv_ref, prev_ref, q_all, do_all, k_all, v_all, dk_all, dv_all,
    back_out, back_in, dq_out, dq_in, kv_out, kv_in,
    tail_buf, cols_ref, rowc_ref, spread_ref, mask_ref, xp_ref,
    ends_ref, a_ref, end_out, cot_out, g_out, e_in, c_in, ge_in, gc_in, chain_out, state_ref, t_out, t_all,
    mix_bias, pair_ref, dpair_ref, dpad_ref, z_ref, u_ref, db_ref, dc_ref,
    sums_ref, edge_ref, end_ref, spill_ref, coef_out, coef_all, red_out, red_a, red_mid, red_b,
    sends, receives, back_sends, back_receives, loads,
):
    group, place, groups = where_am_i()
    head, head_count = lax.axis_index("head"), lax.axis_size("head")
    rows, heads = step_ref.shape
    channels = conv_ref.shape[1]
    pairs = channels // LANES
    span = PLACES * rows
    peers = [lax.rem(place + d, PLACES) for d in range(1, PLACES)]
    post = Post(sends, receives)
    fetches = []
    for n, (source, target) in enumerate((
        (k_hbm, k_ref), (v_hbm, v_ref), (q_hbm, q_ref), (do_hbm, do_ref),
        (conv_hbm, conv_ref), (gate_hbm, gate_ref), (mix_hbm, mix_ref),
    )):
        fetches.append(pltpu.make_async_copy(source, target, loads.at[n]))
        fetches[-1].start()
    partners = [shard(group + far, place, groups) for far in range(1, groups)]
    partners += [shard(group, peer, groups) for peer in peers]
    last, first = place == PLACES - 1, place == 0
    follower = shard(jnp.where(last, group + 1, group), lax.rem(place + 1, PLACES), groups)
    former = shard(jnp.where(first, group - 1, group), lax.rem(place + PLACES - 1, PLACES), groups)
    head_peers = [{"head": lax.rem(head + d, head_count)} for d in range(1, head_count)]
    wait_partners = greet(partners + [follower, former] + head_peers)

    for n, ref in ((2, k_ref), (3, v_ref), (1, do_ref), (0, q_ref)):
        fetches[(2, 3, 0, 1)[n]].wait()
        for r in range(PLACES):
            pack_ref[r, :, n * HEAD_DIM : (n + 1) * HEAD_DIM] = ref[:, r * HEAD_DIM : (r + 1) * HEAD_DIM]
    fetches[4].wait()
    wait_partners()
    ahead = shard(group + 1, place, groups)
    behind = shard(group - 1, place, groups)
    tail_copy = post.send(conv_ref.at[rows - 2 * PAD :, :], tail_buf, follower)
    key_cols, other_cols = pl.ds(3 * LANES, 4 * LANES), pl.ds(0, 3 * LANES)
    near_keys = [
        post.send(pack_ref.at[peer, :, key_cols], recv_ref.at[place, :, key_cols], shard(group, peer, groups))
        for peer in peers
    ]
    far_keys = [post.send(pack_ref.at[place, :, key_cols], prev_ref.at[place], ahead)]
    near_others = [
        post.send(pack_ref.at[peer, :, other_cols], recv_ref.at[place, :, other_cols], shard(group, peer, groups))
        for peer in peers
    ]
    recv_ref[place] = pack_ref[place]

    since = since_ref[...]
    raw = step_ref[...] + bias_ref[...]
    step = jnp.maximum(raw, 0.0) + jnp.log1p(jnp.exp(-jnp.abs(raw)))
    rate = jnp.exp(rate_ref[...])
    log_decay = -step * rate
    i, j = causal(rows)
    tri = (i >= j).astype(F32)
    cum = dot(tri, log_decay, 1, 0, EXACT)
    row_cum = dot(log_decay, tri, 0, 1, EXACT)
    t = lax.broadcasted_iota(jnp.int32, (rows, 1), 0)
    enter = jnp.where(since > t.astype(F32), jnp.exp(cum), 0.0)
    final = cum[rows - 1 : rows]
    to_end = jnp.where((rows - 1 - t).astype(F32) <= since[rows - 1 : rows], jnp.exp(final - cum), 0.0)
    through = enter[rows - 1 : rows]
    t_out[...] = jnp.zeros_like(t_out)
    t_out[0:1, 0:heads] = through
    t_all[place] = t_out[...]
    t_copies = [post.send(t_out, t_all.at[place], shard(group, peer, groups)) for peer in peers]
    for n in range(pairs):
        two = slice(2 * n, 2 * n + 2)
        cols_ref[n] = jnp.concatenate([cum[:, two], step[:, two], enter[:, two], to_end[:, two]], axis=1)
        rowc_ref[n] = row_cum[two]
    spread_ref[...] = spreader(heads, channels)
    fill_masks(since_ref, mask_ref)
    lower = lax.broadcasted_iota(jnp.int32, (rows, LANES), 1) < LANES // 2
    b_part, c_part = group_part(b_ref), group_part(c_ref)
    fetches[5].wait()
    fetches[6].wait()
    tail_copy.wait()

    def ends(n, carry):
        lanes = pl.ds(pl.multiple_of(n * LANES, LANES), LANES)
        cols = cols_ref[n]
        pre = conv_pre(conv_ref[:, lanes], tail_buf[:, lanes], wt_ref[:, lanes], mask_ref, xp_ref)
        act = pre * jax.nn.sigmoid(pre)
        weighted = act * pair_columns(cols, 1, lower) * pair_columns(cols, 3, lower)
        end = dot(b_part, weighted.astype(BF16), 0, 0).astype(BF16)
        gate = gate_ref[:, lanes].astype(F32)
        dy = mix_ref[:, lanes].astype(F32) * (gate * jax.nn.sigmoid(gate))
        start = dot(c_part, (dy * pair_columns(cols, 2, lower)).astype(BF16), 0, 0).astype(BF16)
        for r in range(PLACES):
            part = slice(2 * PAD * r, 2 * PAD * (r + 1))
            ends_ref[r, 0, :, lanes] = end[part]
            ends_ref[r, 1, :, lanes] = start[part]
        return carry

    lax.fori_loop(0, pairs // 2, ends, 0)
    for d in range(1, PLACES):
        near_keys[d - 1].wait()
        source = lax.rem(place + PLACES - d, PLACES)
        far_keys.append(post.send(recv_ref.at[source, :, key_cols], prev_ref.at[source], ahead))
    lax.fori_loop(pairs // 2, pairs, ends, 0)

    a_copies = [post.send(ends_ref.at[peer], a_ref.at[place], shard(group, peer, groups)) for peer in peers]
    a_ref[place] = ends_ref[place]
    for copy in near_others:
        copy.wait()
    for r in range(PLACES):
        here, later = slice(r * rows, (r + 1) * rows), slice(span + r * rows, span + (r + 1) * rows)
        q_all[here, :] = recv_ref[r, :, 0:HEAD_DIM]
        do_all[here, :] = recv_ref[r, :, HEAD_DIM : 2 * HEAD_DIM]
        k_all[later, :] = recv_ref[r, :, 2 * HEAD_DIM : 3 * HEAD_DIM]
        v_all[later, :] = recv_ref[r, :, 3 * HEAD_DIM : 4 * HEAD_DIM]
    dk_all[...] = jnp.zeros_like(dk_all)
    dv_all[...] = jnp.zeros_like(dv_all)
    for copy in t_copies + a_copies:
        copy.wait()
    decays = dot(t_all[...].reshape(PLACES * PAD, LANES), spread_ref[...], 1, 0, EXACT)
    decay = [decays[PAD * n : PAD * n + 1] for n in range(PLACES)]
    end_of = lambda n: a_ref[n, 0].astype(F32)
    cot_of = lambda n: a_ref[n, 1].astype(F32)
    end, cot = end_of(0), cot_of(PLACES - 1)
    for n in range(1, PLACES):
        end = end_of(n) + decay[n] * end
        cot = cot_of(PLACES - 1 - n) + decay[PLACES - 1 - n] * cot
    end_out[...] = end.astype(BF16)
    cot_out[...] = cot.astype(BF16)
    g_out[...] = t_all[0] * t_all[1] * t_all[2] * t_all[3]
    b_copies = []
    for far in range(1, REACH + 1):
        later, earlier = shard(group + far, place, groups), shard(group - far, place, groups)
        b_copies.append(post.send(g_out, ge_in.at[far - 1], later))
        b_copies.append(post.send(g_out, gc_in.at[far - 1], earlier))
        b_copies.append(post.send(end_out, e_in.at[far - 1], later))
        b_copies.append(post.send(cot_out, c_in.at[far - 1], earlier))
    for copy in b_copies:
        copy.wait()
    before = dot(ge_in[...].reshape(REACH * PAD, LANES), spread_ref[...], 1, 0, EXACT)
    after = dot(gc_in[...].reshape(REACH * PAD, LANES), spread_ref[...], 1, 0, EXACT)
    state = e_in[REACH - 1].astype(F32)
    cot = c_in[REACH - 1].astype(F32) * (group + REACH < groups).astype(F32)
    for far in range(REACH - 2, -1, -1):
        state = e_in[far].astype(F32) + before[PAD * far : PAD * far + 1] * state
        cot = (c_in[far].astype(F32) + after[PAD * far : PAD * far + 1] * cot) * (
            group + far + 1 < groups
        ).astype(F32)
    for n in range(PLACES):
        chain_out[n, 0] = state.astype(BF16)
        state = end_of(n) + decay[n] * state
        m = PLACES - 1 - n
        chain_out[m, 1] = cot.astype(BF16)
        cot = cot_of(m) + decay[m] * cot
    state_copies = [
        post.send(chain_out.at[peer], state_ref.at[place], shard(group, peer, groups)) for peer in peers
    ]
    state_ref[place] = chain_out[place]

    for copy in far_keys:
        copy.wait()
    skip = 2 * HEAD_DIM - 3 * LANES
    for r in range(PLACES):
        here = slice(r * rows, (r + 1) * rows)
        k_all[here, :] = prev_ref[r, :, skip : skip + HEAD_DIM]
        v_all[here, :] = prev_ref[r, :, skip + HEAD_DIM : skip + 2 * HEAD_DIM]

    def back_copy(b):
        return pltpu.make_async_remote_copy(
            src_ref=back_out.at[b], dst_ref=back_in.at[b], send_sem=back_sends.at[b],
            recv_sem=back_receives.at[b], device_id=behind, device_id_type=pl.DeviceIdType.MESH,
        )

    def block(b, carry):
        mine = pl.ds(pl.multiple_of(b * rows, rows), rows)
        q = q_all[mine, :]
        grad = do_all[mine, :]
        low = low_ref[pl.ds(b, 1), :]
        at = [pl.ds(pl.multiple_of((b + PLACES - gap) * rows, rows), rows) for gap in range(PLACES + 1)]
        scores = []
        top = None
        for gap in range(PLACES + 1):
            allowed = i + (b + PLACES - gap) * rows >= low
            if gap == 0:
                allowed = allowed & (j >= i)
            s = jnp.where(allowed, dot(k_all[at[gap], :], q, 1, 1) * SCALE, NEG_FILL)
            scores.append(s)
            m = jnp.max(s, axis=0, keepdims=True)
            top = m if top is None else jnp.maximum(top, m)
        total = None
        expo = []
        for gap in range(PLACES + 1):
            e = jnp.exp(scores[gap] - top)
            expo.append(e)
            e_sum = jnp.sum(e, axis=0, keepdims=True)
            total = e_sum if total is None else total + e_sum
        inverse = 1.0 / jnp.maximum(total, 1.0)
        delta = None
        dprobs = []
        for gap in range(PLACES + 1):
            half = (expo[gap] * inverse).astype(BF16)
            dp = dot(v_all[at[gap], :], grad, 1, 1)
            d = jnp.sum(half.astype(F32) * dp, axis=0, keepdims=True)
            delta = d if delta is None else delta + d
            dv_all[at[gap], :] += dot(half, grad, 1, 0)
            dprobs.append(dp)
        dq = None
        for gap in range(PLACES + 1):
            ds = (expo[gap] * inverse * (dprobs[gap] - delta)).astype(BF16)
            dk_all[at[gap], :] += dot(ds, q, 1, 0)
            part = dot(ds, k_all[at[gap], :], 0, 0)
            dq = part if dq is None else dq + part
        dq_out[b, :, 0:HEAD_DIM] = (dq * SCALE).astype(BF16)
        back_out[b, :, 0:HEAD_DIM] = dk_all[mine, :].astype(BF16)
        back_out[b, :, HEAD_DIM : 2 * HEAD_DIM] = dv_all[mine, :].astype(BF16)
        back_copy(b).start()
        return carry

    lax.fori_loop(0, PLACES, block, 0)
    dq_copies = [post.send(dq_out.at[peer], dq_in.at[place], shard(group, peer, groups)) for peer in peers]
    dq_in[place] = dq_out[place]

    mix_bias[...] = jnp.where((i >= j) & ((i - j).astype(F32) <= since), 0.0, NEG_FILL)
    pair_ref[...] = dot(c_part, b_part, 1, 1)
    for ref in (dpair_ref, z_ref, u_ref, db_ref, dc_ref, dpad_ref):
        ref[...] = jnp.zeros_like(ref)
    lane = lax.broadcasted_iota(jnp.int32, (rows, heads), 1)
    for copy in state_copies:
        copy.wait()

    def mixer(n, carry):
        lanes = pl.ds(pl.multiple_of(n * LANES, LANES), LANES)
        cols = cols_ref[n]
        wt = wt_ref[:, lanes]
        size = pair_columns(cols, 1, lower)
        enter = pair_columns(cols, 2, lower)
        to_end = pair_columns(cols, 3, lower)
        pre = conv_pre(conv_ref[:, lanes], tail_buf[:, lanes], wt, mask_ref, xp_ref)
        sig_pre = jax.nn.sigmoid(pre)
        act = pre * sig_pre
        x_half = (act * size).astype(BF16)
        gate = gate_ref[:, lanes].astype(F32)
        sig_gate = jax.nn.sigmoid(gate)
        silu_gate = gate * sig_gate
        cot = mix_ref[:, lanes].astype(F32)
        dy = cot * silu_gate
        dy_half = dy.astype(BF16)
        state = jnp.concatenate([state_ref[r, 0, :, lanes] for r in range(PLACES)], axis=0)
        end_cot = jnp.concatenate([state_ref[r, 1, :, lanes] for r in range(PLACES)], axis=0)
        zero = jnp.zeros_like(dy_half)
        y_parts, dx_parts = [], []
        dpair = dpair_ref[...]
        rowc = rowc_ref[n]
        for k in range(2):
            weights = jnp.exp((cols[:, k : k + 1] - rowc[k : k + 1, :]) + mix_bias[...])
            mixing = (pair_ref[...] * weights).astype(BF16)
            y_parts.append(dot(mixing, x_half, 1, 0))
            dx_parts.append(dot(mixing, dy_half, 0, 0))
            dy_one = jnp.where(lower if k == 0 else ~lower, dy_half, zero)
            dpair = dpair + dot(dy_one, x_half, 1, 1) * weights
        dpair_ref[...] = dpair
        inner = jnp.where(lower, y_parts[0], y_parts[1]) + enter * dot(c_part, state, 1, 0)
        end_part = to_end * dot(b_part, end_cot, 1, 0)
        dx = jnp.where(lower, dx_parts[0], dx_parts[1]) + end_part
        skip = wt[KERNEL : KERNEL + 1, :]
        y = inner + skip * act
        ggate_ref[:, lanes] = (cot * y * (sig_gate + silu_gate * (1.0 - sig_gate))).astype(BF16)
        x_wide = x_half.astype(F32)
        zed = dy_half.astype(F32) * inner - x_wide * dx
        you = dx * act
        for k in range(2):
            side = lower if k == 0 else ~lower
            here = lane == 2 * n + k
            z_one = jnp.sum(jnp.where(side, zed, 0.0), axis=1, keepdims=True)
            u_one = jnp.sum(jnp.where(side, you, 0.0), axis=1, keepdims=True)
            z_ref[...] = jnp.where(here, z_one, z_ref[...])
            u_ref[...] = jnp.where(here, u_one, u_ref[...])
        dc_ref[...] += dot((enter * dy).astype(BF16), state, 1, 1)
        db_ref[...] += dot((to_end * x_wide).astype(BF16), end_cot, 1, 1)
        dact = dx * size + skip * dy
        dpre = dact * (sig_pre + act * (1.0 - sig_pre))
        sums_ref[0:1, lanes] = jnp.sum(dpre * xp_ref[PAD:, :], axis=0, keepdims=True)
        dpad_ref[0, PAD : PAD + rows, :] = dpre
        grown = wt[0:1, :] * dpad_ref[0, 0 : rows + PAD, :]
        for lag in range(1, KERNEL):
            masked = dpre * mask_ref[lag - 1]
            sums_ref[lag : lag + 1, lanes] = jnp.sum(
                masked * xp_ref[PAD - lag : PAD - lag + rows, :], axis=0, keepdims=True
            )
            dpad_ref[lag, PAD : PAD + rows, :] = masked
            grown = grown + wt[lag : lag + 1, :] * dpad_ref[lag, lag : lag + rows + PAD, :]
        gconv_ref[:, lanes] = grown[PAD:, :].astype(BF16)
        edge_ref[:, lanes] = grown[:PAD, :]
        end_ref[:, lanes] = grown[rows:, :]
        sums_ref[4:5, lanes] = jnp.sum(dy * act, axis=0, keepdims=True)
        sums_ref[5:6, lanes] = jnp.sum(state.astype(F32) * end_cot.astype(F32), axis=0, keepdims=True)
        sums_ref[6:7, lanes] = jnp.sum(x_wide * end_part, axis=0, keepdims=True)
        sums_ref[7:8, lanes] = jnp.zeros((1, LANES), F32)
        return carry

    lax.fori_loop(0, pairs // 2, mixer, 0)
    for b in range(PLACES):
        back_copy(b).wait()
        rear = slice(span + b * rows, span + (b + 1) * rows)
        key = dk_all[rear, :] + back_in[b, :, 0:HEAD_DIM].astype(F32)
        kv_out[b, :, 0:HEAD_DIM] = (key * SCALE).astype(BF16)
        value = dv_all[rear, :] + back_in[b, :, HEAD_DIM : 2 * HEAD_DIM].astype(F32)
        kv_out[b, :, HEAD_DIM : 2 * HEAD_DIM] = value.astype(BF16)
    kv_copies = [post.send(kv_out.at[peer], kv_in.at[place], shard(group, peer, groups)) for peer in peers]
    kv_in[place] = kv_out[place]
    lax.fori_loop(pairs // 2, pairs, mixer, 0)

    spill_copy = post.send(edge_ref, spill_ref, former)
    per_head = dot(sums_ref[...], spread_ref[...], 1, 1, EXACT)[:, 0:heads]
    last_row = per_head[6:7] + through * per_head[5:6]
    dcum = z_ref[...] + jnp.where(t == rows - 1, last_row, 0.0)
    dlog = dot(tri, dcum, 0, 0, EXACT)
    grad_step = (u_ref[...] - dlog * rate) * jax.nn.sigmoid(raw)
    gstep_ref[...] = grad_step
    red_out[...] = jnp.where(
        lax.broadcasted_iota(jnp.int32, red_out.shape, 0) < KERNEL, sums_ref[...], 0.0
    )
    red_out[4:5, 0:heads] = jnp.sum(grad_step, axis=0, keepdims=True)
    red_out[5:6, 0:heads] = jnp.sum(dlog * log_decay, axis=0, keepdims=True)
    red_out[6:7, 0:heads] = per_head[4:5]
    near = [post.send(red_out, red_a.at[place], shard(group, peer, groups)) for peer in peers]
    red_a[place] = red_out[...]
    dpair = dpair_ref[...]
    dc_ref[...] += dot(dpair, b_part.astype(F32), 1, 0, EXACT)
    db_ref[...] += dot(dpair, c_part.astype(F32), 0, 0, EXACT)
    coef_out[...] = jnp.concatenate([db_ref[...], dc_ref[...]], axis=1).astype(BF16)
    coefs = [post.send(coef_out, coef_all.at[head], peer) for peer in head_peers]
    coef_all[head] = coef_out[...]
    for copy in near:
        copy.wait()
    red_mid[...] = red_a[0] + red_a[1] + red_a[2] + red_a[3]
    wide = [
        post.send(red_mid, red_b.at[group], shard(group + far, place, groups)) for far in range(1, groups)
    ]
    red_b[group] = red_mid[...]
    spill_copy.wait()
    gconv_ref[rows - PAD :, :] = (end_ref[...] + spill_ref[...]).astype(BF16)
    for copy in coefs:
        copy.wait()
    halves = [coef_all[2 * n].astype(F32) + coef_all[2 * n + 1].astype(F32) for n in range(2)]
    half = coef_out.shape[1] // 2
    gin_ref[...] = jnp.concatenate([halves[0][:, :half], halves[1][:, :half]], axis=1)
    gout_ref[...] = jnp.concatenate([halves[0][:, half:], halves[1][:, half:]], axis=1)
    for copy in dq_copies + kv_copies:
        copy.wait()
    for r in range(PLACES):
        cols = slice(r * HEAD_DIM, (r + 1) * HEAD_DIM)
        dq_ref[:, cols] = dq_in[r, :, 0:HEAD_DIM]
        dk_ref[:, cols] = kv_in[r, :, 0:HEAD_DIM]
        dv_ref[:, cols] = kv_in[r, :, HEAD_DIM : 2 * HEAD_DIM]
    for copy in wide:
        copy.wait()
    total = red_b[0]
    for n in range(1, groups):
        total = total + red_b[n]
    total_ref[...] = total


def local(
    queries, keys, values, attn_grad, doc_ids, conv_input, conv_weight, step_raw, step_bias,
    rate_log, skip_gain, input_coeff, output_coeff, gate_input, mix_grad,
):
    rows, width = queries.shape
    heads, channels = step_raw.shape[1], conv_input.shape[1]
    pairs = channels // LANES
    index = lax.axis_index("seq")
    groups = lax.axis_size("seq") // PLACES
    base = (index // PLACES) * PLACES * rows
    counts = jnp.sum(doc_ids[None, :] < jnp.arange(DOCS)[:, None], axis=1)
    docs = lax.dynamic_slice_in_dim(doc_ids, base, PLACES * rows)
    start = jnp.sum(jnp.where(docs[None, :] == jnp.arange(DOCS)[:, None], counts[:, None], 0), axis=0)
    where = base + jnp.arange(PLACES * rows, dtype=jnp.int32)
    low = (jnp.maximum(start, where - (WINDOW - 1)) - base + WINDOW).reshape(PLACES, rows)
    since = lax.dynamic_slice_in_dim(where - start, index % PLACES * rows, rows).astype(F32)[:, None]
    wt = jnp.concatenate(
        [conv_weight, jnp.repeat(skip_gain, channels // heads)[None], jnp.zeros((7 - KERNEL, channels), F32)]
    )
    bias, rate = step_bias[None], rate_log[None]

    struct = jax.ShapeDtypeStruct
    vmem = pl.BlockSpec(memory_space=pltpu.VMEM)
    loose = pl.BlockSpec(memory_space=pl.ANY)
    dma = lambda n: pltpu.SemaphoreType.DMA((n,))
    params = lambda n: pltpu.CompilerParams(
        collective_id=n, has_side_effects=True, vmem_limit_bytes=56 * 1024 * 1024
    )
    packed, keys_wide = 4 * HEAD_DIM, 4 * LANES
    quarter = (2, 2 * PAD, channels)
    part = quarter[1:]
    span = PLACES * rows
    half = lambda *shape: pltpu.VMEM(shape, BF16)
    full = lambda *shape: pltpu.VMEM(shape, F32)
    flat = full(PAD, channels)
    outs = pl.pallas_call(
        whole_kernel,
        in_specs=[vmem] * 8 + [loose] * 7,
        out_specs=[vmem] * 9,
        out_shape=[
            struct((rows, width), BF16), struct((rows, width), BF16), struct((rows, width), BF16),
            struct((rows, channels), BF16), struct((rows, channels), BF16), struct((rows, heads), F32),
            struct((rows, LANES), F32), struct((rows, LANES), F32), struct((PAD, channels), F32),
        ],
        scratch_shapes=[
            half(rows, width), half(rows, width), half(rows, width), half(rows, width),
            half(rows, channels), half(rows, channels), half(rows, channels),
            half(PLACES, rows, packed), half(PLACES, rows, packed), half(PLACES, rows, keys_wide),
            half(span, HEAD_DIM), half(span, HEAD_DIM), half(2 * span, HEAD_DIM), half(2 * span, HEAD_DIM),
            full(2 * span, HEAD_DIM), full(2 * span, HEAD_DIM),
            half(PLACES, rows, keys_wide), half(PLACES, rows, keys_wide),
            half(PLACES, rows, 2 * LANES), half(PLACES, rows, 2 * LANES),
            half(PLACES, rows, keys_wide), half(PLACES, rows, keys_wide),
            half(2 * PAD, channels), full(pairs, rows, 8), full(pairs, 2, rows), full(LANES, channels),
            full(KERNEL - 1, rows, LANES), full(rows + PAD, LANES),
            half(PLACES, *quarter), half(PLACES, *quarter), half(*part), half(*part), full(PAD, LANES),
            half(REACH, *part), half(REACH, *part), full(REACH, PAD, LANES), full(REACH, PAD, LANES),
            half(PLACES, *quarter), half(PLACES, *quarter), full(PAD, LANES), full(PLACES, PAD, LANES),
            full(rows, rows), full(rows, rows), full(rows, rows), full(KERNEL, rows + 2 * PAD, LANES),
            full(rows, heads), full(rows, heads), full(rows, LANES // 2), full(rows, LANES // 2),
            flat, flat, flat, flat, half(rows, LANES), half(4, rows, LANES),
            flat, full(PLACES, PAD, channels), flat, full(groups, PAD, channels),
            dma(SENDS), dma(SENDS), dma(PLACES), dma(PLACES), dma(7),
        ],
        name="whole",
        compiler_params=params(0),
    )(
        since, low, step_raw, bias, rate, input_coeff, output_coeff, wt,
        keys, values, queries, attn_grad, conv_input, gate_input, mix_grad,
    )
    total = outs[-1]
    return (
        *outs[:-1], total[:KERNEL], total[4, :heads], total[5, :heads], total[6, :heads],
    )


def solution(mesh):
    sharded = P("seq", "head")
    return jax.shard_map(
        local,
        mesh=mesh,
        in_specs=(
            sharded, sharded, sharded, sharded, P(), sharded, P(None, "head"), sharded,
            P("head"), P("head"), P("head"), P("seq", None), P("seq", None), sharded, sharded,
        ),
        out_specs=(
            sharded, sharded, sharded, sharded, sharded, sharded,
            P("seq", None), P("seq", None), P(None, "head"), P("head"), P("head"), P("head"),
        ),
        check_vma=False,
    )
```

```python
import jax
import jax.numpy as jnp
from jax import lax
from jax.experimental import pallas as pl
from jax.experimental.pallas import tpu as pltpu
from jax.sharding import PartitionSpec as P

HEAD_DIM = 224
WINDOW = 1024
KERNEL = 4
PAD = 8
LANES = 128
PLACES = 4
DOCS = 8
REACH = 4

EXACT = lax.Precision.HIGHEST
F32 = jnp.float32
BF16 = jnp.bfloat16
NEG_FILL = -1e30
SENDS = 69
SCALE = HEAD_DIM ** (-0.5)


def dot(a, b, ca, cb, precision=None):
    return lax.dot_general(
        a, b, (((ca,), (cb,)), ((), ())), preferred_element_type=F32, precision=precision
    )


def where_am_i():
    index = lax.axis_index("seq")
    groups = lax.axis_size("seq") // PLACES
    return lax.div(index, PLACES), lax.rem(index, PLACES), groups


def shard(group, place, groups):
    return {"seq": lax.rem(group + 2 * groups, groups) * PLACES + place}


def greet(partners):
    barrier = pltpu.get_barrier_semaphore()
    for partner in partners:
        pl.semaphore_signal(barrier, inc=1, device_id=partner, device_id_type=pl.DeviceIdType.MESH)
    return lambda: pl.semaphore_wait(barrier, len(partners))


class Post:
    def __init__(self, sends, receives):
        self.sends, self.receives, self.used = sends, receives, 0

    def send(self, source, target, device):
        copy = pltpu.make_async_remote_copy(
            src_ref=source, dst_ref=target, send_sem=self.sends.at[self.used],
            recv_sem=self.receives.at[self.used], device_id=device,
            device_id_type=pl.DeviceIdType.MESH,
        )
        self.used += 1
        copy.start()
        return copy


def spreader(heads, channels):
    width = channels // heads
    row = lax.broadcasted_iota(jnp.int32, (LANES, channels), 0)
    col = lax.broadcasted_iota(jnp.int32, (LANES, channels), 1)
    return ((col >= row * width) & (col < row * width + width)).astype(F32)


def causal(rows):
    i = lax.broadcasted_iota(jnp.int32, (rows, rows), 0)
    j = lax.broadcasted_iota(jnp.int32, (rows, rows), 1)
    return i, j


def pair_columns(cols, index, lower):
    return jnp.where(lower, cols[:, 2 * index : 2 * index + 1], cols[:, 2 * index + 1 : 2 * index + 2])


def fill_masks(since_ref, mask_ref):
    for lag in range(1, KERNEL):
        mask_ref[lag - 1] = jnp.broadcast_to((since_ref[...] >= lag).astype(F32), mask_ref.shape[1:])


def conv_pre(conv, tail, wt, mask_ref, xp_ref):
    rows = conv.shape[0]
    xp_ref[:PAD, :] = tail.astype(F32)[PAD:]
    xp_ref[PAD:, :] = conv.astype(F32)
    pre = wt[0:1, :] * xp_ref[PAD:, :]
    for lag in range(1, KERNEL):
        pre = pre + wt[lag : lag + 1, :] * (xp_ref[PAD - lag : PAD - lag + rows, :] * mask_ref[lag - 1])
    return pre


def group_part(ref):
    half = ref.shape[1] // 2
    whole = ref[...].astype(F32)
    first = lax.axis_index("head") < lax.axis_size("head") // 2
    return jnp.where(first, whole[:, :half], whole[:, half:]).astype(BF16)


def whole_kernel(
    since_ref, low_ref, step_ref, bias_ref, rate_ref, skip_ref, b_ref, c_ref, weight_ref,
    k_hbm, v_hbm, q_hbm, do_hbm, conv_hbm, gate_hbm, mix_hbm,
    dq_in, dk_in, dv_in, gconv_ref, ggate_ref, gfix_ref, gstep_ref, gin_ref, gout_ref, total_ref,
    k_ref, v_ref, q_ref, do_ref, conv_ref, gate_ref, mix_ref,
    k_pack, v_pack, q_pack, do_pack, q_all, do_all, k_all, v_all, dk_all, dv_all,
    dk_out, dv_out, dk_back, dv_back, dq_own, dk_own, dv_own,
    tail_buf, wt_ref, cols_ref, rowc_ref, spread_ref, mask_ref, xp_ref,
    act_all, slope_all, dy_all, cg_all, inner_all, dx_all,
    ends_ref, a_ref, end_out, cot_out, g_out, e_in, c_in, ge_in, gc_in, chain_out, state_ref, t_out, t_all,
    mix_bias, pair_ref, dpair_ref, dpad_ref, z_ref, u_ref, db_ref, dc_ref,
    sums_ref, edge_ref, end_ref, spill_ref, coef_out, coef_all, red_out, red_a, red_mid, red_b,
    sends, receives, back_sends, back_receives, loads, keeps,
):
    group, place, groups = where_am_i()
    head, head_count = lax.axis_index("head"), lax.axis_size("head")
    rows, heads = step_ref.shape
    channels = conv_ref.shape[1]
    pairs = channels // LANES
    peers = [lax.rem(place + d, PLACES) for d in range(1, PLACES)]
    post = Post(sends, receives)
    fetches = []
    for n, (source, target) in enumerate((
        (k_hbm, k_ref), (v_hbm, v_ref), (conv_hbm, conv_ref), (q_hbm, q_ref), (do_hbm, do_ref),
        (gate_hbm, gate_ref), (mix_hbm, mix_ref),
    )):
        fetches.append(pltpu.make_async_copy(source, target, loads.at[n]))
        fetches[-1].start()
    partners = [shard(group + far, place, groups) for far in range(1, groups)]
    partners += [shard(group, peer, groups) for peer in peers]
    last, first = place == PLACES - 1, place == 0
    follower = shard(jnp.where(last, group + 1, group), lax.rem(place + 1, PLACES), groups)
    former = shard(jnp.where(first, group - 1, group), lax.rem(place + PLACES - 1, PLACES), groups)
    head_peers = [{"head": lax.rem(head + d, head_count)} for d in range(1, head_count)]
    wait_partners = greet(partners + [follower, former] + head_peers)
    ahead = shard(group + 1, place, groups)
    behind = shard(group - 1, place, groups)

    def pack(source, target):
        for r in range(PLACES):
            target[r, :, 0:HEAD_DIM] = source[:, r * HEAD_DIM : (r + 1) * HEAD_DIM]
            target[r, :, HEAD_DIM:] = jnp.zeros((rows, target.shape[2] - HEAD_DIM), BF16)

    def spread(source, target, offset):
        return [
            post.send(source.at[peer], target.at[offset + place], shard(group, peer, groups)) for peer in peers
        ]

    fetches[0].wait()
    pack(k_ref, k_pack)
    fetches[1].wait()
    pack(v_ref, v_pack)
    fetches[2].wait()
    wait_partners()
    tail_copy = post.send(conv_ref.at[rows - 2 * PAD :, :], tail_buf, follower)
    far = [post.send(k_pack.at[place], k_all.at[place], ahead)]
    near_k = spread(k_pack, k_all, PLACES)
    far.append(post.send(v_pack.at[place], v_all.at[place], ahead))
    near_v = spread(v_pack, v_all, PLACES)
    fetches[3].wait()
    pack(q_ref, q_pack)
    fetches[4].wait()
    pack(do_ref, do_pack)
    near = spread(q_pack, q_all, 0) + spread(do_pack, do_all, 0)

    since = since_ref[...]
    raw = step_ref[...] + bias_ref[...]
    step = jnp.maximum(raw, 0.0) + jnp.log1p(jnp.exp(-jnp.abs(raw)))
    rate = jnp.exp(rate_ref[...])
    log_decay = -step * rate
    i, j = causal(rows)
    tri = (i >= j).astype(F32)
    cum = dot(tri, log_decay, 1, 0, EXACT)
    row_cum = dot(log_decay, tri, 0, 1, EXACT)
    t = lax.broadcasted_iota(jnp.int32, (rows, 1), 0)
    enter = jnp.where(since > t.astype(F32), jnp.exp(cum), 0.0)
    final = cum[rows - 1 : rows]
    to_end = jnp.where((rows - 1 - t).astype(F32) <= since[rows - 1 : rows], jnp.exp(final - cum), 0.0)
    through = enter[rows - 1 : rows]
    t_out[...] = jnp.zeros_like(t_out)
    t_out[0:1, 0:heads] = through
    t_all[place] = t_out[...]
    t_copies = [post.send(t_out, t_all.at[place], shard(group, peer, groups)) for peer in peers]
    for n in range(pairs):
        two = slice(2 * n, 2 * n + 2)
        cols_ref[n] = jnp.concatenate([cum[:, two], step[:, two], enter[:, two], to_end[:, two]], axis=1)
        rowc_ref[n] = row_cum[two]
    spread_ref[...] = spreader(heads, channels)
    wt_ref[0:KERNEL, :] = weight_ref[...]
    wt_ref[KERNEL : KERNEL + 1, :] = dot(skip_ref[...], spread_ref[0:heads, :], 1, 0, EXACT)
    fill_masks(since_ref, mask_ref)
    lower = lax.broadcasted_iota(jnp.int32, (rows, LANES), 1) < LANES // 2
    b_part, c_part = group_part(b_ref), group_part(c_ref)
    fetches[5].wait()
    fetches[6].wait()
    tail_copy.wait()

    def ends(n, carry):
        lanes = pl.ds(pl.multiple_of(n * LANES, LANES), LANES)
        cols = cols_ref[n]
        pre = conv_pre(conv_ref[:, lanes], tail_buf[:, lanes], wt_ref[:, lanes], mask_ref, xp_ref)
        sig_pre = jax.nn.sigmoid(pre)
        act = pre * sig_pre
        act_all[:, lanes] = act
        slope_all[:, lanes] = sig_pre + act * (1.0 - sig_pre)
        weighted = act * pair_columns(cols, 1, lower) * pair_columns(cols, 3, lower)
        end = dot(b_part, weighted.astype(BF16), 0, 0).astype(BF16)
        gate = gate_ref[:, lanes].astype(F32)
        sig_gate = jax.nn.sigmoid(gate)
        silu_gate = gate * sig_gate
        cot = mix_ref[:, lanes].astype(F32)
        dy = cot * silu_gate
        dy_all[:, lanes] = dy
        cg_all[:, lanes] = cot * (sig_gate + silu_gate * (1.0 - sig_gate))
        start = dot(c_part, (dy * pair_columns(cols, 2, lower)).astype(BF16), 0, 0).astype(BF16)
        for r in range(PLACES):
            part = slice(2 * PAD * r, 2 * PAD * (r + 1))
            ends_ref[r, 0, :, lanes] = end[part]
            ends_ref[r, 1, :, lanes] = start[part]
        return carry

    def pass_on(copies, target):
        for d in range(1, PLACES):
            copies[d - 1].wait()
            source = lax.rem(place + PLACES - d, PLACES)
            far.append(post.send(target.at[PLACES + source], target.at[source], ahead))

    lax.fori_loop(0, pairs // 4, ends, 0)
    pass_on(near_k, k_all)
    lax.fori_loop(pairs // 4, 3 * pairs // 4, ends, 0)
    pass_on(near_v, v_all)
    lax.fori_loop(3 * pairs // 4, pairs, ends, 0)

    a_copies = [post.send(ends_ref.at[peer], a_ref.at[place], shard(group, peer, groups)) for peer in peers]
    a_ref[place] = ends_ref[place]
    for mine, everyone, offset in (
        (k_pack, k_all, PLACES), (v_pack, v_all, PLACES), (q_pack, q_all, 0), (do_pack, do_all, 0)
    ):
        everyone[offset + place] = mine[place]
    dk_all[...] = jnp.zeros_like(dk_all)
    dv_all[...] = jnp.zeros_like(dv_all)

    mix_bias[...] = jnp.where((i >= j) & ((i - j).astype(F32) <= since), 0.0, NEG_FILL)
    pair_ref[...] = dot(c_part, b_part, 1, 1)
    for ref in (dpair_ref, z_ref, u_ref, db_ref, dc_ref, dpad_ref, red_out):
        ref[...] = jnp.zeros_like(ref)

    def within(n, carry):
        lanes = pl.ds(pl.multiple_of(n * LANES, LANES), LANES)
        cols = cols_ref[n]
        x_half = (act_all[:, lanes] * pair_columns(cols, 1, lower)).astype(BF16)
        dy_half = dy_all[:, lanes].astype(BF16)
        zero = jnp.zeros_like(dy_half)
        y_parts, dx_parts = [], []
        dpair = dpair_ref[...]
        rowc = rowc_ref[n]
        for k in range(2):
            weights = jnp.exp((cols[:, k : k + 1] - rowc[k : k + 1, :]) + mix_bias[...])
            mixing = (pair_ref[...] * weights).astype(BF16)
            y_parts.append(dot(mixing, x_half, 1, 0))
            dx_parts.append(dot(mixing, dy_half, 0, 0))
            dy_one = jnp.where(lower if k == 0 else ~lower, dy_half, zero)
            dpair = dpair + dot(dy_one, x_half, 1, 1) * weights
        dpair_ref[...] = dpair
        inner_all[:, lanes] = jnp.where(lower, y_parts[0], y_parts[1])
        dx_all[:, lanes] = jnp.where(lower, dx_parts[0], dx_parts[1])
        return carry

    lax.fori_loop(0, pairs // 3, within, 0)
    for copy in t_copies + a_copies:
        copy.wait()
    decays = dot(t_all[...].reshape(PLACES * PAD, LANES), spread_ref[...], 1, 0, EXACT)
    decay = [decays[PAD * n : PAD * n + 1] for n in range(PLACES)]
    end_of = lambda n: a_ref[n, 0].astype(F32)
    cot_of = lambda n: a_ref[n, 1].astype(F32)
    end, cot = end_of(0), cot_of(PLACES - 1)
    for n in range(1, PLACES):
        end = end_of(n) + decay[n] * end
        cot = cot_of(PLACES - 1 - n) + decay[PLACES - 1 - n] * cot
    end_out[...] = end.astype(BF16)
    cot_out[...] = cot.astype(BF16)
    g_out[...] = t_all[0] * t_all[1] * t_all[2] * t_all[3]
    b_copies = []
    for away in range(1, REACH + 1):
        later, earlier = shard(group + away, place, groups), shard(group - away, place, groups)
        b_copies.append(post.send(g_out, ge_in.at[away - 1], later))
        b_copies.append(post.send(g_out, gc_in.at[away - 1], earlier))
        b_copies.append(post.send(end_out, e_in.at[away - 1], later))
        b_copies.append(post.send(cot_out, c_in.at[away - 1], earlier))
    lax.fori_loop(pairs // 3, pairs, within, 0)
    for copy in b_copies:
        copy.wait()
    before = dot(ge_in[...].reshape(REACH * PAD, LANES), spread_ref[...], 1, 0, EXACT)
    after = dot(gc_in[...].reshape(REACH * PAD, LANES), spread_ref[...], 1, 0, EXACT)
    state = e_in[REACH - 1].astype(F32)
    cot = c_in[REACH - 1].astype(F32) * (group + REACH < groups).astype(F32)
    for away in range(REACH - 2, -1, -1):
        state = e_in[away].astype(F32) + before[PAD * away : PAD * away + 1] * state
        cot = (c_in[away].astype(F32) + after[PAD * away : PAD * away + 1] * cot) * (
            group + away + 1 < groups
        ).astype(F32)
    for n in range(PLACES):
        chain_out[n, 0] = state.astype(BF16)
        state = end_of(n) + decay[n] * state
        m = PLACES - 1 - n
        chain_out[m, 1] = cot.astype(BF16)
        cot = cot_of(m) + decay[m] * cot
    state_copies = [
        post.send(chain_out.at[peer], state_ref.at[place], shard(group, peer, groups)) for peer in peers
    ]
    state_ref[place] = chain_out[place]

    for copy in near + far:
        copy.wait()

    def back_copy(source, target, b, n):
        return pltpu.make_async_remote_copy(
            src_ref=source.at[b], dst_ref=target.at[b], send_sem=back_sends.at[n],
            recv_sem=back_receives.at[n], device_id=behind, device_id_type=pl.DeviceIdType.MESH,
        )

    def block(b, carry):
        q = q_all[b]
        grad = do_all[b]
        low = low_ref[pl.ds(b, 1), :]
        at = [b + PLACES - gap for gap in range(PLACES + 1)]
        scores = []
        top = None
        for gap in range(PLACES + 1):
            allowed = i + at[gap] * rows >= low
            if gap == 0:
                allowed = allowed & (j >= i)
            s = jnp.where(allowed, dot(k_all[at[gap]], q, 1, 1) * SCALE, NEG_FILL)
            scores.append(s)
            m = jnp.max(s, axis=0, keepdims=True)
            top = m if top is None else jnp.maximum(top, m)
        total = None
        expo = []
        for gap in range(PLACES + 1):
            e = jnp.exp(scores[gap] - top)
            expo.append(e)
            e_sum = jnp.sum(e, axis=0, keepdims=True)
            total = e_sum if total is None else total + e_sum
        inverse = 1.0 / jnp.maximum(total, 1.0)
        delta = None
        dprobs = []
        for gap in range(PLACES + 1):
            half = (expo[gap] * inverse).astype(BF16)
            dp = dot(v_all[at[gap]], grad, 1, 1)
            d = jnp.sum(half.astype(F32) * dp, axis=0, keepdims=True)
            delta = d if delta is None else delta + d
            dv_all[at[gap]] += dot(half, grad, 1, 0)
            dprobs.append(dp)
        dq = None
        for gap in range(PLACES + 1):
            ds = (expo[gap] * inverse * (dprobs[gap] - delta)).astype(BF16)
            dk_all[at[gap]] += dot(ds, q, 1, 0)
            part = dot(ds, k_all[at[gap]], 0, 0)
            dq = part if dq is None else dq + part
        dq_own[b] = (dq * SCALE).astype(BF16)
        dk_out[b] = dk_all[b].astype(BF16)
        dv_out[b] = dv_all[b].astype(BF16)
        back_copy(dk_out, dk_back, b, b).start()
        return carry

    lax.fori_loop(0, PLACES, block, 0)
    for b in range(PLACES):
        back_copy(dv_out, dv_back, b, PLACES + b).start()
    kept = []

    def give_back(source, target):
        copies = spread(source, target, 0)
        copies.append(pltpu.make_async_copy(source.at[place], target.at[place], keeps.at[len(kept)]))
        copies[-1].start()
        kept.extend(copies)

    give_back(dq_own, dq_in)

    def across(n, carry):
        lanes = pl.ds(pl.multiple_of(n * LANES, LANES), LANES)
        cols = cols_ref[n]
        wt = wt_ref[:, lanes]
        size = pair_columns(cols, 1, lower)
        enter = pair_columns(cols, 2, lower)
        to_end = pair_columns(cols, 3, lower)
        xp_ref[:PAD, :] = tail_buf[:, lanes].astype(F32)[PAD:]
        xp_ref[PAD:, :] = conv_ref[:, lanes].astype(F32)
        act = act_all[:, lanes]
        dy = dy_all[:, lanes]
        x_wide = (act * size).astype(BF16).astype(F32)
        state = jnp.concatenate([state_ref[r, 0, :, lanes] for r in range(PLACES)], axis=0)
        end_cot = jnp.concatenate([state_ref[r, 1, :, lanes] for r in range(PLACES)], axis=0)
        inner = inner_all[:, lanes] + enter * dot(c_part, state, 1, 0)
        end_part = to_end * dot(b_part, end_cot, 1, 0)
        dx = dx_all[:, lanes] + end_part
        skip = wt[KERNEL : KERNEL + 1, :]
        ggate_ref[:, lanes] = (cg_all[:, lanes] * (inner + skip * act)).astype(BF16)
        zed = dy.astype(BF16).astype(F32) * inner - x_wide * dx
        you = dx * act
        for k in range(2):
            side = lower if k == 0 else ~lower
            here = lane == 2 * n + k
            z_one = jnp.sum(jnp.where(side, zed, 0.0), axis=1, keepdims=True)
            u_one = jnp.sum(jnp.where(side, you, 0.0), axis=1, keepdims=True)
            z_ref[...] = jnp.where(here, z_one, z_ref[...])
            u_ref[...] = jnp.where(here, u_one, u_ref[...])
        dc_ref[...] += dot((enter * dy).astype(BF16), state, 1, 1)
        db_ref[...] += dot((to_end * x_wide).astype(BF16), end_cot, 1, 1)
        dpre = (dx * size + skip * dy) * slope_all[:, lanes]
        red_out[pl.ds(n, 1), :] = jnp.sum(dpre * xp_ref[PAD:, :], axis=0, keepdims=True)
        dpad_ref[0, PAD : PAD + rows, :] = dpre
        grown = wt[0:1, :] * dpad_ref[0, 0 : rows + PAD, :]
        for lag in range(1, KERNEL):
            masked = dpre * mask_ref[lag - 1]
            red_out[pl.ds(lag * pairs + n, 1), :] = jnp.sum(
                masked * xp_ref[PAD - lag : PAD - lag + rows, :], axis=0, keepdims=True
            )
            dpad_ref[lag, PAD : PAD + rows, :] = masked
            grown = grown + wt[lag : lag + 1, :] * dpad_ref[lag, lag : lag + rows + PAD, :]
        gconv_ref[:, lanes] = grown[PAD:, :].astype(BF16)
        edge_ref[:, lanes] = grown[:PAD, :]
        end_ref[:, lanes] = grown[rows:, :]
        sums_ref[0:1, lanes] = jnp.sum(dy * act, axis=0, keepdims=True)
        sums_ref[1:2, lanes] = jnp.sum(state.astype(F32) * end_cot.astype(F32), axis=0, keepdims=True)
        sums_ref[2:3, lanes] = jnp.sum(x_wide * end_part, axis=0, keepdims=True)
        sums_ref[3:8, lanes] = jnp.zeros((5, LANES), F32)
        return carry

    def whole_sum(source, target, total, out, offset, factor):
        for b in range(PLACES):
            back_copy(source, target, b, offset + b).wait()
            out[b] = ((total[PLACES + b] + target[b].astype(F32)) * factor).astype(BF16)

    lane = lax.broadcasted_iota(jnp.int32, (rows, heads), 1)
    for copy in state_copies:
        copy.wait()
    lax.fori_loop(0, pairs // 2, across, 0)
    whole_sum(dk_out, dk_back, dk_all, dk_own, 0, SCALE)
    give_back(dk_own, dk_in)
    lax.fori_loop(pairs // 2, pairs, across, 0)

    spill_copy = post.send(edge_ref, spill_ref, former)
    per_head = dot(sums_ref[...], spread_ref[...], 1, 1, EXACT)[:, 0:heads]
    last_row = per_head[2:3] + through * per_head[1:2]
    dcum = z_ref[...] + jnp.where(t == rows - 1, last_row, 0.0)
    dlog = dot(tri, dcum, 0, 0, EXACT)
    grad_step = (u_ref[...] - dlog * rate) * jax.nn.sigmoid(raw)
    gstep_ref[...] = grad_step
    small = KERNEL * pairs
    red_out[small : small + 1, 0:heads] = jnp.sum(grad_step, axis=0, keepdims=True)
    red_out[small + 1 : small + 2, 0:heads] = jnp.sum(dlog * log_decay, axis=0, keepdims=True)
    red_out[small + 2 : small + 3, 0:heads] = per_head[0:1]
    reds = [post.send(red_out, red_a.at[place], shard(group, peer, groups)) for peer in peers]
    red_a[place] = red_out[...]
    dpair = dpair_ref[...]
    dc_ref[...] += dot(dpair, b_part.astype(F32), 1, 0, EXACT)
    db_ref[...] += dot(dpair, c_part.astype(F32), 0, 0, EXACT)
    coef_out[...] = jnp.concatenate([db_ref[...], dc_ref[...]], axis=1).astype(BF16)
    coefs = [post.send(coef_out, coef_all.at[head], peer) for peer in head_peers]
    coef_all[head] = coef_out[...]
    for copy in reds:
        copy.wait()
    red_mid[...] = red_a[0] + red_a[1] + red_a[2] + red_a[3]
    wide = [
        post.send(red_mid, red_b.at[group], shard(group + away, place, groups)) for away in range(1, groups)
    ]
    red_b[group] = red_mid[...]
    whole_sum(dv_out, dv_back, dv_all, dv_own, PLACES, 1.0)
    give_back(dv_own, dv_in)
    spill_copy.wait()
    gfix_ref[...] = end_ref[...] + spill_ref[...]
    for copy in coefs:
        copy.wait()
    halves = [coef_all[2 * n].astype(F32) + coef_all[2 * n + 1].astype(F32) for n in range(2)]
    half = coef_out.shape[1] // 2
    gin_ref[...] = jnp.concatenate([halves[0][:, :half], halves[1][:, :half]], axis=1)
    gout_ref[...] = jnp.concatenate([halves[0][:, half:], halves[1][:, half:]], axis=1)
    for copy in wide:
        copy.wait()
    total = red_b[0]
    for n in range(1, groups):
        total = total + red_b[n]
    total_ref[...] = total
    for copy in kept:
        copy.wait()


def finish_kernel(
    dq_in, dk_in, dv_in, gconv_in, ggate_in, gfix_ref, gstep_in, gin_in, gout_in, total_ref,
    dq_ref, dk_ref, dv_ref, gconv_ref, ggate_ref, gstep_ref, gin_ref, gout_ref, conv_ref, bias_ref, rate_ref, skip_ref,
):
    for source, target in ((dq_in, dq_ref), (dk_in, dk_ref), (dv_in, dv_ref)):
        for r in range(PLACES):
            target[:, r * HEAD_DIM : (r + 1) * HEAD_DIM] = source[r, :, 0:HEAD_DIM]
    for source, target in (
        (gconv_in, gconv_ref), (ggate_in, ggate_ref), (gstep_in, gstep_ref), (gin_in, gin_ref), (gout_in, gout_ref)
    ):
        target[...] = source[...]

    @pl.when(pl.program_id(0) == pl.num_programs(0) - 1)
    def _():
        rows = gconv_ref.shape[0]
        gconv_ref[rows - PAD :, :] = gfix_ref[...].astype(BF16)
        pairs = conv_ref.shape[1] // LANES
        heads = bias_ref.shape[1]
        for lag in range(KERNEL):
            for n in range(pairs):
                row = lag * pairs + n
                conv_ref[lag : lag + 1, n * LANES : (n + 1) * LANES] = total_ref[row : row + 1, :]
        for n, ref in enumerate((bias_ref, rate_ref, skip_ref)):
            row = KERNEL * pairs + n
            ref[...] = total_ref[row : row + 1, 0:heads]


def local(
    queries, keys, values, attn_grad, doc_ids, conv_input, conv_weight, step_raw, step_bias,
    rate_log, skip_gain, input_coeff, output_coeff, gate_input, mix_grad,
):
    rows, width = queries.shape
    heads, channels = step_raw.shape[1], conv_input.shape[1]
    pairs = channels // LANES
    index = lax.axis_index("seq")
    groups = lax.axis_size("seq") // PLACES
    base = (index // PLACES) * PLACES * rows
    counts = jnp.sum(doc_ids[None, :] < jnp.arange(DOCS)[:, None], axis=1)
    docs = lax.dynamic_slice_in_dim(doc_ids, base, PLACES * rows)
    start = jnp.sum(jnp.where(docs[None, :] == jnp.arange(DOCS)[:, None], counts[:, None], 0), axis=0)
    where = base + jnp.arange(PLACES * rows, dtype=jnp.int32)
    low = (jnp.maximum(start, where - (WINDOW - 1)) - base + WINDOW).reshape(PLACES, rows)
    since = lax.dynamic_slice_in_dim(where - start, index % PLACES * rows, rows).astype(F32)[:, None]

    struct = jax.ShapeDtypeStruct
    vmem = pl.BlockSpec(memory_space=pltpu.VMEM)
    loose = pl.BlockSpec(memory_space=pl.ANY)
    dma = lambda n: pltpu.SemaphoreType.DMA((n,))
    head_cols = 2 * LANES
    quarter = (2, 2 * PAD, channels)
    part = quarter[1:]
    half = lambda *shape: pltpu.VMEM(shape, BF16)
    full = lambda *shape: pltpu.VMEM(shape, F32)
    flat = full(PAD, channels)
    piece = lambda n: half(n, rows, head_cols)
    red_rows = 64
    wide_shape = (rows, channels)
    mid = pl.pallas_call(
        whole_kernel,
        in_specs=[vmem] * 9 + [loose] * 7,
        out_specs=[loose] * 3 + [vmem] * 7,
        out_shape=[struct((PLACES, rows, head_cols), BF16)] * 3
        + [
            struct(wide_shape, BF16), struct(wide_shape, BF16), struct((PAD, channels), F32),
            struct((rows, heads), F32), struct((rows, LANES), F32), struct((rows, LANES), F32),
            struct((red_rows, LANES), F32),
        ],
        scratch_shapes=[
            half(rows, width), half(rows, width), half(rows, width), half(rows, width),
            half(*wide_shape), half(*wide_shape), half(*wide_shape),
            piece(PLACES), piece(PLACES), piece(PLACES), piece(PLACES),
            piece(PLACES), piece(PLACES), piece(2 * PLACES), piece(2 * PLACES),
            full(2 * PLACES, rows, head_cols), full(2 * PLACES, rows, head_cols),
            piece(PLACES), piece(PLACES), piece(PLACES), piece(PLACES),
            piece(PLACES), piece(PLACES), piece(PLACES),
            half(2 * PAD, channels), flat, full(pairs, rows, 8), full(pairs, 2, rows), full(LANES, channels),
            full(KERNEL - 1, rows, LANES), full(rows + PAD, LANES),
            full(*wide_shape), full(*wide_shape), full(*wide_shape), full(*wide_shape), full(*wide_shape),
            full(*wide_shape),
            half(PLACES, *quarter), half(PLACES, *quarter), half(*part), half(*part), full(PAD, LANES),
            half(REACH, *part), half(REACH, *part), full(REACH, PAD, LANES), full(REACH, PAD, LANES),
            half(PLACES, *quarter), half(PLACES, *quarter), full(PAD, LANES), full(PLACES, PAD, LANES),
            full(rows, rows), full(rows, rows), full(rows, rows), full(KERNEL, rows + 2 * PAD, LANES),
            full(rows, heads), full(rows, heads), full(rows, LANES // 2), full(rows, LANES // 2),
            flat, flat, flat, flat, half(rows, LANES), half(4, rows, LANES),
            full(red_rows, LANES), full(PLACES, red_rows, LANES), full(red_rows, LANES),
            full(groups, red_rows, LANES),
            dma(SENDS), dma(SENDS), dma(2 * PLACES), dma(2 * PLACES), dma(7), dma(3 * PLACES),
        ],
        name="whole",
        compiler_params=pltpu.CompilerParams(
            collective_id=0, has_side_effects=True, vmem_limit_bytes=58 * 1024 * 1024
        ),
    )(
        since, low, step_raw, step_bias[None], rate_log[None], skip_gain[None], input_coeff, output_coeff,
        conv_weight, keys, values, queries, attn_grad, conv_input, gate_input, mix_grad,
    )
    steps = 4
    tall = lambda cols: pl.BlockSpec((rows // steps, cols), lambda n: (n, 0))
    piled = pl.BlockSpec((PLACES, rows // steps, head_cols), lambda n: (0, n, 0))
    whole = lambda *shape: pl.BlockSpec(shape, lambda n: (0, 0))
    *outs, conv, bias, rate, skip = pl.pallas_call(
        finish_kernel,
        grid=(steps,),
        in_specs=[piled] * 3
        + [
            tall(channels), tall(channels), whole(PAD, channels), tall(heads), tall(LANES), tall(LANES),
            whole(red_rows, LANES),
        ],
        out_specs=[tall(width)] * 3
        + [tall(channels), tall(channels), tall(heads), tall(LANES), tall(LANES), whole(KERNEL, channels)]
        + [whole(1, heads)] * 3,
        out_shape=[struct((rows, width), BF16)] * 3
        + [
            struct(wide_shape, BF16), struct(wide_shape, BF16), struct((rows, heads), F32),
            struct((rows, LANES), F32), struct((rows, LANES), F32), struct((KERNEL, channels), F32),
        ]
        + [struct((1, heads), F32)] * 3,
        name="finish",
        compiler_params=pltpu.CompilerParams(dimension_semantics=("arbitrary",)),
    )(*mid)
    return (*outs, conv, bias[0], rate[0], skip[0])


def solution(mesh):
    sharded = P("seq", "head")
    return jax.shard_map(
        local,
        mesh=mesh,
        in_specs=(
            sharded, sharded, sharded, sharded, P(), sharded, P(None, "head"), sharded,
            P("head"), P("head"), P("head"), P("seq", None), P("seq", None), sharded, sharded,
        ),
        out_specs=(
            sharded, sharded, sharded, sharded, sharded, sharded,
            P("seq", None), P("seq", None), P(None, "head"), P("head"), P("head"), P("head"),
        ),
        check_vma=False,
    )
```

```python
import jax
import jax.numpy as jnp
from jax import lax
from jax.experimental import pallas as pl
from jax.experimental.pallas import tpu as pltpu
from jax.sharding import PartitionSpec as P

HEAD_DIM = 224
WINDOW = 1024
KERNEL = 4
PAD = 8
LANES = 128
PLACES = 4
DOCS = 8
REACH = 4

EXACT = lax.Precision.HIGHEST
F32 = jnp.float32
BF16 = jnp.bfloat16
NEG_FILL = -1e30
SENDS = 69
SCALE = HEAD_DIM ** (-0.5)


def dot(a, b, ca, cb, precision=None):
    return lax.dot_general(
        a, b, (((ca,), (cb,)), ((), ())), preferred_element_type=F32, precision=precision
    )


def where_am_i():
    index = lax.axis_index("seq")
    groups = lax.axis_size("seq") // PLACES
    return lax.div(index, PLACES), lax.rem(index, PLACES), groups


def shard(group, place, groups):
    return {"seq": lax.rem(group + 2 * groups, groups) * PLACES + place}


def greet(partners):
    barrier = pltpu.get_barrier_semaphore()
    for partner in partners:
        pl.semaphore_signal(barrier, inc=1, device_id=partner, device_id_type=pl.DeviceIdType.MESH)
    return lambda: pl.semaphore_wait(barrier, len(partners))


class Post:
    def __init__(self, sends, receives):
        self.sends, self.receives, self.used = sends, receives, 0

    def send(self, source, target, device):
        copy = pltpu.make_async_remote_copy(
            src_ref=source, dst_ref=target, send_sem=self.sends.at[self.used],
            recv_sem=self.receives.at[self.used], device_id=device,
            device_id_type=pl.DeviceIdType.MESH,
        )
        self.used += 1
        copy.start()
        return copy


def spreader(heads, channels):
    width = channels // heads
    row = lax.broadcasted_iota(jnp.int32, (LANES, channels), 0)
    col = lax.broadcasted_iota(jnp.int32, (LANES, channels), 1)
    return ((col >= row * width) & (col < row * width + width)).astype(F32)


def causal(rows):
    i = lax.broadcasted_iota(jnp.int32, (rows, rows), 0)
    j = lax.broadcasted_iota(jnp.int32, (rows, rows), 1)
    return i, j


def pair_columns(cols, index, lower):
    return jnp.where(lower, cols[:, 2 * index : 2 * index + 1], cols[:, 2 * index + 1 : 2 * index + 2])


def fill_masks(since, mask_ref):
    for lag in range(1, KERNEL):
        mask_ref[lag - 1] = jnp.broadcast_to((since >= lag).astype(F32), mask_ref.shape[1:])


def conv_pre(conv, tail, wt, mask_ref, xp_ref):
    rows = conv.shape[0]
    xp_ref[:PAD, :] = tail.astype(F32)[PAD:]
    xp_ref[PAD:, :] = conv.astype(F32)
    pre = wt[0:1, :] * xp_ref[PAD:, :]
    for lag in range(1, KERNEL):
        pre = pre + wt[lag : lag + 1, :] * (xp_ref[PAD - lag : PAD - lag + rows, :] * mask_ref[lag - 1])
    return pre


def group_part(ref):
    half = ref.shape[1] // 2
    whole = ref[...].astype(F32)
    first = lax.axis_index("head") < lax.axis_size("head") // 2
    return jnp.where(first, whole[:, :half], whole[:, half:]).astype(BF16)


def whole_kernel(
    small_hbm,
    k_hbm, v_hbm, q_hbm, do_hbm, conv_hbm, gate_hbm, mix_hbm,
    dq_in, dk_in, dv_in, gconv_hbm, ggate_hbm, gfix_ref, gstep_ref, gin_ref, gout_ref, total_ref,
    small_refs, gconv_ref, ggate_ref, low_ref, since_ref, turn_ref, turn_back, k_ref, v_ref, q_ref, do_ref, conv_ref, gate_ref, mix_ref,
    k_pack, v_pack, q_pack, do_pack, q_all, do_all, k_all, v_all, dk_all, dv_all,
    dk_out, dv_out, dk_back, dv_back, dq_own, dk_own, dv_own,
    tail_buf, wt_ref, cols_ref, rowc_ref, spread_ref, mask_ref, xp_ref,
    act_all, slope_all, dy_all, cg_all, inner_all, dx_all,
    ends_ref, a_ref, end_out, cot_out, g_out, e_in, c_in, ge_in, gc_in, chain_out, state_ref, t_out, t_all,
    mix_bias, pair_ref, dpair_ref, dpad_ref, z_ref, u_ref, db_ref, dc_ref,
    sums_ref, edge_ref, end_ref, spill_ref, coef_out, coef_all, red_out, red_a, red_mid, red_b,
    sends, receives, back_sends, back_receives, loads, keeps, writes, small_loads,
):
    group, place, groups = where_am_i()
    head, head_count = lax.axis_index("head"), lax.axis_size("head")
    doc_ref, step_ref, bias_ref, rate_ref, skip_ref, b_ref, c_ref, weight_ref = small_refs
    heads, rows = step_ref.shape
    channels = conv_ref.shape[1]
    pairs = channels // LANES
    peers = [lax.rem(place + d, PLACES) for d in range(1, PLACES)]
    post = Post(sends, receives)
    fetches = []
    for n, (source, target) in enumerate((
        (k_hbm, k_ref), (v_hbm, v_ref), (conv_hbm, conv_ref), (q_hbm, q_ref), (do_hbm, do_ref),
        (gate_hbm, gate_ref), (mix_hbm, mix_ref),
    )):
        fetches.append(pltpu.make_async_copy(source, target, loads.at[n]))
        fetches[-1].start()
    small_fetches = [
        pltpu.make_async_copy(source, target, small_loads.at[n])
        for n, (source, target) in enumerate(zip(small_hbm, small_refs))
    ]
    for fetch in small_fetches:
        fetch.start()
    partners = [shard(group + far, place, groups) for far in range(1, groups)]
    partners += [shard(group, peer, groups) for peer in peers]
    last, first = place == PLACES - 1, place == 0
    follower = shard(jnp.where(last, group + 1, group), lax.rem(place + 1, PLACES), groups)
    former = shard(jnp.where(first, group - 1, group), lax.rem(place + PLACES - 1, PLACES), groups)
    head_peers = [{"head": lax.rem(head + d, head_count)} for d in range(1, head_count)]
    wait_partners = greet(partners + [follower, former] + head_peers)
    ahead = shard(group + 1, place, groups)
    behind = shard(group - 1, place, groups)

    def pack(source, target):
        for r in range(PLACES):
            target[r, :, 0:HEAD_DIM] = source[:, r * HEAD_DIM : (r + 1) * HEAD_DIM]
            target[r, :, HEAD_DIM:] = jnp.zeros((rows, target.shape[2] - HEAD_DIM), BF16)

    def spread(source, target, offset):
        return [
            post.send(source.at[peer], target.at[offset + place], shard(group, peer, groups)) for peer in peers
        ]

    fetches[0].wait()
    pack(k_ref, k_pack)
    fetches[1].wait()
    pack(v_ref, v_pack)
    fetches[2].wait()
    wait_partners()
    tail_copy = post.send(conv_ref.at[rows - 2 * PAD :, :], tail_buf, follower)
    far = [post.send(k_pack.at[place], k_all.at[place], ahead)]
    near_k = spread(k_pack, k_all, PLACES)
    far.append(post.send(v_pack.at[place], v_all.at[place], ahead))
    near_v = spread(v_pack, v_all, PLACES)
    fetches[3].wait()
    pack(q_ref, q_pack)
    fetches[4].wait()
    pack(do_ref, do_pack)

    for fetch in small_fetches:
        fetch.wait()
    per_row = rows // LANES
    docs = doc_ref[pl.ds(pl.multiple_of(group * PLACES * per_row, PLACES * per_row), PLACES * per_row), :]
    everyone_doc = doc_ref[...]
    begin = jnp.zeros(docs.shape, F32)
    for doc in range(1, DOCS):
        count = jnp.sum((everyone_doc < doc).astype(F32), axis=0, keepdims=True)
        count = jnp.sum(count, axis=1, keepdims=True)
        begin = jnp.where(docs == doc, count, begin)
    where = (
        lax.broadcasted_iota(jnp.int32, docs.shape, 0) * LANES
        + lax.broadcasted_iota(jnp.int32, docs.shape, 1)
        + group * (PLACES * rows)
    ).astype(F32)
    low = jnp.maximum(begin, where - (WINDOW - 1)) - (group * (PLACES * rows) - WINDOW).astype(F32)
    since_ref[...] = where - begin
    for n in range(PLACES * per_row):
        b, side = n // per_row, n % per_row
        low_ref[b : b + 1, side * LANES : (side + 1) * LANES] = low[n : n + 1]
    row = jnp.concatenate([since_ref[pl.ds(place * per_row + n, 1), :] for n in range(per_row)], axis=1)
    since = jnp.broadcast_to(row, (PAD, rows)).T[:, 0:1]

    turn_ref[...] = jnp.zeros_like(turn_ref)
    turn_ref[0:heads, :] = step_ref[...]
    raw = turn_ref[...].T[:, 0:heads] + bias_ref[...]
    step = jnp.maximum(raw, 0.0) + jnp.log1p(jnp.exp(-jnp.abs(raw)))
    rate = jnp.exp(rate_ref[...])
    log_decay = -step * rate
    i, j = causal(rows)
    tri = (i >= j).astype(F32)
    cum = dot(tri, log_decay, 1, 0, EXACT)
    row_cum = dot(log_decay, tri, 0, 1, EXACT)
    t = lax.broadcasted_iota(jnp.int32, (rows, 1), 0)
    enter = jnp.where(since > t.astype(F32), jnp.exp(cum), 0.0)
    final = cum[rows - 1 : rows]
    to_end = jnp.where((rows - 1 - t).astype(F32) <= since[rows - 1 : rows], jnp.exp(final - cum), 0.0)
    through = enter[rows - 1 : rows]
    t_out[...] = jnp.zeros_like(t_out)
    t_out[0:1, 0:heads] = through
    t_all[place] = t_out[...]
    t_copies = [post.send(t_out, t_all.at[place], shard(group, peer, groups)) for peer in peers]
    for n in range(pairs):
        two = slice(2 * n, 2 * n + 2)
        cols_ref[n] = jnp.concatenate([cum[:, two], step[:, two], enter[:, two], to_end[:, two]], axis=1)
        rowc_ref[n] = row_cum[two]
    spread_ref[...] = spreader(heads, channels)
    wt_ref[0:KERNEL, :] = weight_ref[...]
    wt_ref[KERNEL : KERNEL + 1, :] = dot(skip_ref[...], spread_ref[0:heads, :], 1, 0, EXACT)
    fill_masks(since, mask_ref)
    lower = lax.broadcasted_iota(jnp.int32, (rows, LANES), 1) < LANES // 2
    b_part, c_part = group_part(b_ref), group_part(c_ref)
    fetches[5].wait()
    fetches[6].wait()
    tail_copy.wait()

    def ends(n, carry):
        lanes = pl.ds(pl.multiple_of(n * LANES, LANES), LANES)
        cols = cols_ref[n]
        pre = conv_pre(conv_ref[:, lanes], tail_buf[:, lanes], wt_ref[:, lanes], mask_ref, xp_ref)
        sig_pre = jax.nn.sigmoid(pre)
        act = pre * sig_pre
        act_all[:, lanes] = act
        slope_all[:, lanes] = sig_pre + act * (1.0 - sig_pre)
        weighted = act * pair_columns(cols, 1, lower) * pair_columns(cols, 3, lower)
        end = dot(b_part, weighted.astype(BF16), 0, 0).astype(BF16)
        gate = gate_ref[:, lanes].astype(F32)
        sig_gate = jax.nn.sigmoid(gate)
        silu_gate = gate * sig_gate
        cot = mix_ref[:, lanes].astype(F32)
        dy = cot * silu_gate
        dy_all[:, lanes] = dy
        cg_all[:, lanes] = cot * (sig_gate + silu_gate * (1.0 - sig_gate))
        start = dot(c_part, (dy * pair_columns(cols, 2, lower)).astype(BF16), 0, 0).astype(BF16)
        for r in range(PLACES):
            part = slice(2 * PAD * r, 2 * PAD * (r + 1))
            ends_ref[r, 0, :, lanes] = end[part]
            ends_ref[r, 1, :, lanes] = start[part]
        return carry

    def pass_on(copies, target):
        for d in range(1, PLACES):
            copies[d - 1].wait()
            source = lax.rem(place + PLACES - d, PLACES)
            far.append(post.send(target.at[PLACES + source], target.at[source], ahead))

    lax.fori_loop(0, 2 * pairs // 3, ends, 0)
    pass_on(near_k, k_all)
    lax.fori_loop(2 * pairs // 3, pairs, ends, 0)

    a_copies = [post.send(ends_ref.at[peer], a_ref.at[place], shard(group, peer, groups)) for peer in peers]
    near = spread(q_pack, q_all, 0) + spread(do_pack, do_all, 0)
    a_ref[place] = ends_ref[place]
    pass_on(near_v, v_all)
    for mine, everyone, offset in (
        (k_pack, k_all, PLACES), (v_pack, v_all, PLACES), (q_pack, q_all, 0), (do_pack, do_all, 0)
    ):
        everyone[offset + place] = mine[place]
    dk_all[...] = jnp.zeros_like(dk_all)
    dv_all[...] = jnp.zeros_like(dv_all)

    mix_bias[...] = jnp.where((i >= j) & ((i - j).astype(F32) <= since), 0.0, NEG_FILL)
    pair_ref[...] = dot(c_part, b_part, 1, 1)
    for ref in (dpair_ref, z_ref, u_ref, db_ref, dc_ref, dpad_ref, red_out):
        ref[...] = jnp.zeros_like(ref)

    def within(n, carry):
        lanes = pl.ds(pl.multiple_of(n * LANES, LANES), LANES)
        cols = cols_ref[n]
        x_half = (act_all[:, lanes] * pair_columns(cols, 1, lower)).astype(BF16)
        dy_half = dy_all[:, lanes].astype(BF16)
        zero = jnp.zeros_like(dy_half)
        y_parts, dx_parts = [], []
        dpair = dpair_ref[...]
        rowc = rowc_ref[n]
        for k in range(2):
            weights = jnp.exp((cols[:, k : k + 1] - rowc[k : k + 1, :]) + mix_bias[...])
            mixing = (pair_ref[...] * weights).astype(BF16)
            y_parts.append(dot(mixing, x_half, 1, 0))
            dx_parts.append(dot(mixing, dy_half, 0, 0))
            dy_one = jnp.where(lower if k == 0 else ~lower, dy_half, zero)
            dpair = dpair + dot(dy_one, x_half, 1, 1) * weights
        dpair_ref[...] = dpair
        inner_all[:, lanes] = jnp.where(lower, y_parts[0], y_parts[1])
        dx_all[:, lanes] = jnp.where(lower, dx_parts[0], dx_parts[1])
        return carry

    lax.fori_loop(0, pairs // 3, within, 0)
    for copy in t_copies + a_copies:
        copy.wait()
    decays = dot(t_all[...].reshape(PLACES * PAD, LANES), spread_ref[...], 1, 0, EXACT)
    decay = [decays[PAD * n : PAD * n + 1] for n in range(PLACES)]
    end_of = lambda n: a_ref[n, 0].astype(F32)
    cot_of = lambda n: a_ref[n, 1].astype(F32)
    end, cot = end_of(0), cot_of(PLACES - 1)
    for n in range(1, PLACES):
        end = end_of(n) + decay[n] * end
        cot = cot_of(PLACES - 1 - n) + decay[PLACES - 1 - n] * cot
    end_out[...] = end.astype(BF16)
    cot_out[...] = cot.astype(BF16)
    g_out[...] = t_all[0] * t_all[1] * t_all[2] * t_all[3]
    b_copies = []
    for away in range(1, REACH + 1):
        later, earlier = shard(group + away, place, groups), shard(group - away, place, groups)
        b_copies.append(post.send(g_out, ge_in.at[away - 1], later))
        b_copies.append(post.send(g_out, gc_in.at[away - 1], earlier))
        b_copies.append(post.send(end_out, e_in.at[away - 1], later))
        b_copies.append(post.send(cot_out, c_in.at[away - 1], earlier))
    lax.fori_loop(pairs // 3, pairs, within, 0)
    dpair = dpair_ref[...]
    dc_ref[...] = dot(dpair, b_part.astype(F32), 1, 0, EXACT)
    db_ref[...] = dot(dpair, c_part.astype(F32), 0, 0, EXACT)
    for copy in near + far:
        copy.wait()

    def back_copy(source, target, b, n):
        return pltpu.make_async_remote_copy(
            src_ref=source.at[b], dst_ref=target.at[b], send_sem=back_sends.at[n],
            recv_sem=back_receives.at[n], device_id=behind, device_id_type=pl.DeviceIdType.MESH,
        )

    below = i.astype(F32)

    def block(b, carry):
        q = q_all[b]
        grad = do_all[b]
        low = low_ref[pl.ds(b, 1), :]
        at = [b + PLACES - gap for gap in range(PLACES + 1)]
        scores = []
        top = None
        for gap in range(PLACES + 1):
            allowed = below >= low - jnp.asarray(at[gap] * rows).astype(F32)
            if gap == 0:
                allowed = allowed & (j >= i)
            s = jnp.where(allowed, dot(k_all[at[gap]], q, 1, 1) * SCALE, NEG_FILL)
            scores.append(s)
            m = jnp.max(s, axis=0, keepdims=True)
            top = m if top is None else jnp.maximum(top, m)
        total = None
        expo = []
        for gap in range(PLACES + 1):
            e = jnp.exp(scores[gap] - top)
            expo.append(e)
            e_sum = jnp.sum(e, axis=0, keepdims=True)
            total = e_sum if total is None else total + e_sum
        inverse = 1.0 / jnp.maximum(total, 1.0)
        delta = None
        dprobs = []
        for gap in range(PLACES + 1):
            half = (expo[gap] * inverse).astype(BF16)
            dp = dot(v_all[at[gap]], grad, 1, 1)
            d = jnp.sum(half.astype(F32) * dp, axis=0, keepdims=True)
            delta = d if delta is None else delta + d
            dv_all[at[gap]] += dot(half, grad, 1, 0)
            dprobs.append(dp)
        dq = None
        for gap in range(PLACES + 1):
            ds = (expo[gap] * inverse * (dprobs[gap] - delta)).astype(BF16)
            dk_all[at[gap]] += dot(ds, q, 1, 0)
            part = dot(ds, k_all[at[gap]], 0, 0)
            dq = part if dq is None else dq + part
        dq_own[b] = (dq * SCALE).astype(BF16)
        dk_out[b] = dk_all[b].astype(BF16)
        dv_out[b] = dv_all[b].astype(BF16)
        back_copy(dk_out, dk_back, b, b).start()
        return carry

    lax.fori_loop(0, PLACES // 2, block, 0)
    for copy in b_copies:
        copy.wait()
    before = dot(ge_in[...].reshape(REACH * PAD, LANES), spread_ref[...], 1, 0, EXACT)
    after = dot(gc_in[...].reshape(REACH * PAD, LANES), spread_ref[...], 1, 0, EXACT)
    state = e_in[REACH - 1].astype(F32)
    cot = c_in[REACH - 1].astype(F32) * (group + REACH < groups).astype(F32)
    for away in range(REACH - 2, -1, -1):
        state = e_in[away].astype(F32) + before[PAD * away : PAD * away + 1] * state
        cot = (c_in[away].astype(F32) + after[PAD * away : PAD * away + 1] * cot) * (
            group + away + 1 < groups
        ).astype(F32)
    for n in range(PLACES):
        chain_out[n, 0] = state.astype(BF16)
        state = end_of(n) + decay[n] * state
        m = PLACES - 1 - n
        chain_out[m, 1] = cot.astype(BF16)
        cot = cot_of(m) + decay[m] * cot
    state_copies = [
        post.send(chain_out.at[peer], state_ref.at[place], shard(group, peer, groups)) for peer in peers
    ]
    state_ref[place] = chain_out[place]

    lax.fori_loop(PLACES // 2, PLACES, block, 0)
    for b in range(PLACES):
        back_copy(dv_out, dv_back, b, PLACES + b).start()
    kept = []

    def give_back(source, target):
        copies = spread(source, target, 0)
        copies.append(pltpu.make_async_copy(source.at[place], target.at[place], keeps.at[len(kept)]))
        copies[-1].start()
        kept.extend(copies)

    give_back(dq_own, dq_in)

    def across(n, carry):
        lanes = pl.ds(pl.multiple_of(n * LANES, LANES), LANES)
        cols = cols_ref[n]
        wt = wt_ref[:, lanes]
        size = pair_columns(cols, 1, lower)
        enter = pair_columns(cols, 2, lower)
        to_end = pair_columns(cols, 3, lower)
        xp_ref[:PAD, :] = tail_buf[:, lanes].astype(F32)[PAD:]
        xp_ref[PAD:, :] = conv_ref[:, lanes].astype(F32)
        act = act_all[:, lanes]
        dy = dy_all[:, lanes]
        x_wide = (act * size).astype(BF16).astype(F32)
        state = jnp.concatenate([state_ref[r, 0, :, lanes] for r in range(PLACES)], axis=0)
        end_cot = jnp.concatenate([state_ref[r, 1, :, lanes] for r in range(PLACES)], axis=0)
        inner = inner_all[:, lanes] + enter * dot(c_part, state, 1, 0)
        end_part = to_end * dot(b_part, end_cot, 1, 0)
        dx = dx_all[:, lanes] + end_part
        skip = wt[KERNEL : KERNEL + 1, :]
        ggate_ref[:, lanes] = (cg_all[:, lanes] * (inner + skip * act)).astype(BF16)
        zed = dy.astype(BF16).astype(F32) * inner - x_wide * dx
        you = dx * act
        for k in range(2):
            side = lower if k == 0 else ~lower
            here = lane == 2 * n + k
            z_one = jnp.sum(jnp.where(side, zed, 0.0), axis=1, keepdims=True)
            u_one = jnp.sum(jnp.where(side, you, 0.0), axis=1, keepdims=True)
            z_ref[...] = jnp.where(here, z_one, z_ref[...])
            u_ref[...] = jnp.where(here, u_one, u_ref[...])
        dc_ref[...] += dot((enter * dy).astype(BF16), state, 1, 1)
        db_ref[...] += dot((to_end * x_wide).astype(BF16), end_cot, 1, 1)
        dpre = (dx * size + skip * dy) * slope_all[:, lanes]
        red_out[pl.ds(n, 1), :] = jnp.sum(dpre * xp_ref[PAD:, :], axis=0, keepdims=True)
        dpad_ref[0, PAD : PAD + rows, :] = dpre
        grown = wt[0:1, :] * dpad_ref[0, 0 : rows + PAD, :]
        for lag in range(1, KERNEL):
            masked = dpre * mask_ref[lag - 1]
            red_out[pl.ds(lag * pairs + n, 1), :] = jnp.sum(
                masked * xp_ref[PAD - lag : PAD - lag + rows, :], axis=0, keepdims=True
            )
            dpad_ref[lag, PAD : PAD + rows, :] = masked
            grown = grown + wt[lag : lag + 1, :] * dpad_ref[lag, lag : lag + rows + PAD, :]
        gconv_ref[:, lanes] = grown[PAD:, :].astype(BF16)
        edge_ref[:, lanes] = grown[:PAD, :]
        end_ref[:, lanes] = grown[rows:, :]
        sums_ref[0:1, lanes] = jnp.sum(dy * act, axis=0, keepdims=True)
        sums_ref[1:2, lanes] = jnp.sum(state.astype(F32) * end_cot.astype(F32), axis=0, keepdims=True)
        sums_ref[2:3, lanes] = jnp.sum(x_wide * end_part, axis=0, keepdims=True)
        sums_ref[3:8, lanes] = jnp.zeros((5, LANES), F32)
        return carry

    def whole_sum(source, target, total, out, offset, factor):
        for b in range(PLACES):
            back_copy(source, target, b, offset + b).wait()
            out[b] = ((total[PLACES + b] + target[b].astype(F32)) * factor).astype(BF16)

    lane = lax.broadcasted_iota(jnp.int32, (rows, heads), 1)
    for copy in state_copies:
        copy.wait()
    lax.fori_loop(0, 2 * pairs // 3, across, 0)
    whole_sum(dk_out, dk_back, dk_all, dk_own, 0, SCALE)
    give_back(dk_own, dk_in)
    lax.fori_loop(2 * pairs // 3, pairs, across, 0)
    written = []
    for n, (source, target) in enumerate(((gconv_ref, gconv_hbm), (ggate_ref, ggate_hbm))):
        written.append(pltpu.make_async_copy(source, target, writes.at[n]))
        written[-1].start()

    spill_copy = post.send(edge_ref, spill_ref, former)
    per_head = dot(sums_ref[...], spread_ref[...], 1, 1, EXACT)[:, 0:heads]
    last_row = per_head[2:3] + through * per_head[1:2]
    dcum = z_ref[...] + jnp.where(t == rows - 1, last_row, 0.0)
    dlog = dot(tri, dcum, 0, 0, EXACT)
    grad_step = (u_ref[...] - dlog * rate) * jax.nn.sigmoid(raw)
    turn_back[...] = jnp.zeros_like(turn_back)
    turn_back[:, 0:heads] = grad_step
    gstep_ref[...] = turn_back[...].T[0:heads, :]
    small = KERNEL * pairs
    red_out[small : small + 1, 0:heads] = jnp.sum(grad_step, axis=0, keepdims=True)
    red_out[small + 1 : small + 2, 0:heads] = jnp.sum(dlog * log_decay, axis=0, keepdims=True)
    red_out[small + 2 : small + 3, 0:heads] = per_head[0:1]
    reds = [post.send(red_out, red_a.at[place], shard(group, peer, groups)) for peer in peers]
    red_a[place] = red_out[...]
    coef_out[...] = jnp.concatenate([db_ref[...], dc_ref[...]], axis=1).astype(BF16)
    coefs = [post.send(coef_out, coef_all.at[head], peer) for peer in head_peers]
    coef_all[head] = coef_out[...]
    whole_sum(dv_out, dv_back, dv_all, dv_own, PLACES, 1.0)
    give_back(dv_own, dv_in)
    for copy in reds:
        copy.wait()
    red_mid[...] = red_a[0] + red_a[1] + red_a[2] + red_a[3]
    wide = [
        post.send(red_mid, red_b.at[group], shard(group + away, place, groups)) for away in range(1, groups)
    ]
    red_b[group] = red_mid[...]
    spill_copy.wait()
    gfix_ref[...] = end_ref[...] + spill_ref[...]
    for copy in coefs:
        copy.wait()
    halves = [coef_all[2 * n].astype(F32) + coef_all[2 * n + 1].astype(F32) for n in range(2)]
    half = coef_out.shape[1] // 2
    gin_ref[...] = jnp.concatenate([halves[0][:, :half], halves[1][:, :half]], axis=1)
    gout_ref[...] = jnp.concatenate([halves[0][:, half:], halves[1][:, half:]], axis=1)
    for copy in wide:
        copy.wait()
    total = red_b[0]
    for n in range(1, groups):
        total = total + red_b[n]
    total_ref[...] = total
    for copy in kept + written:
        copy.wait()


def finish_kernel(
    dq_in, dk_in, dv_in, gconv_in, ggate_in, gfix_ref, gstep_in, gin_in, gout_in, total_ref,
    dq_ref, dk_ref, dv_ref, gconv_ref, ggate_ref, gstep_ref, gin_ref, gout_ref, conv_ref, bias_ref, rate_ref, skip_ref,
):
    for source, target in ((dq_in, dq_ref), (dk_in, dk_ref), (dv_in, dv_ref)):
        for r in range(PLACES):
            target[:, r * HEAD_DIM : (r + 1) * HEAD_DIM] = source[r, :, 0:HEAD_DIM]
    for source, target in (
        (gconv_in, gconv_ref), (ggate_in, ggate_ref), (gstep_in, gstep_ref), (gin_in, gin_ref), (gout_in, gout_ref)
    ):
        target[...] = source[...]

    @pl.when(pl.program_id(0) == pl.num_programs(0) - 1)
    def _():
        rows = gconv_ref.shape[0]
        gconv_ref[rows - PAD :, :] = gfix_ref[...].astype(BF16)
        pairs = conv_ref.shape[1] // LANES
        heads = bias_ref.shape[1]
        for lag in range(KERNEL):
            for n in range(pairs):
                row = lag * pairs + n
                conv_ref[lag : lag + 1, n * LANES : (n + 1) * LANES] = total_ref[row : row + 1, :]
        for n, ref in enumerate((bias_ref, rate_ref, skip_ref)):
            row = KERNEL * pairs + n
            ref[...] = total_ref[row : row + 1, 0:heads]


def local(
    queries, keys, values, attn_grad, doc_ids, conv_input, conv_weight, step_raw, step_bias,
    rate_log, skip_gain, input_coeff, output_coeff, gate_input, mix_grad,
):
    rows, width = queries.shape
    heads, channels = step_raw.shape[1], conv_input.shape[1]
    pairs = channels // LANES
    groups = lax.axis_size("seq") // PLACES
    struct = jax.ShapeDtypeStruct
    vmem = pl.BlockSpec(memory_space=pltpu.VMEM)
    loose = pl.BlockSpec(memory_space=pl.ANY)
    dma = lambda n: pltpu.SemaphoreType.DMA((n,))
    head_cols = 2 * LANES
    quarter = (2, 2 * PAD, channels)
    part = quarter[1:]
    half = lambda *shape: pltpu.VMEM(shape, BF16)
    full = lambda *shape: pltpu.VMEM(shape, F32)
    flat = full(PAD, channels)
    piece = lambda n: half(n, rows, head_cols)
    red_rows = 64
    wide_shape = (rows, channels)
    small = [
        doc_ids.reshape(-1, LANES), step_raw.T, step_bias[None], rate_log[None], skip_gain[None],
        input_coeff, output_coeff, conv_weight,
    ]
    mid = pl.pallas_call(
        whole_kernel,
        in_specs=[[loose] * 8] + [loose] * 7,
        out_specs=[loose] * 5 + [vmem] * 5,
        out_shape=[struct((PLACES, rows, head_cols), BF16)] * 3
        + [
            struct(wide_shape, BF16), struct(wide_shape, BF16), struct((PAD, channels), F32),
            struct((heads, rows), F32), struct((rows, LANES), F32), struct((rows, LANES), F32),
            struct((red_rows, LANES), F32),
        ],
        scratch_shapes=[
            [pltpu.VMEM(a.shape, a.dtype) for a in small], half(*wide_shape), half(*wide_shape),
            full(PAD, rows), full(PLACES * rows // LANES, LANES), full(LANES, rows), full(rows, LANES),
            half(rows, width), half(rows, width), half(rows, width), half(rows, width),
            half(*wide_shape), half(*wide_shape), half(*wide_shape),
            piece(PLACES), piece(PLACES), piece(PLACES), piece(PLACES),
            piece(PLACES), piece(PLACES), piece(2 * PLACES), piece(2 * PLACES),
            full(2 * PLACES, rows, head_cols), full(2 * PLACES, rows, head_cols),
            piece(PLACES), piece(PLACES), piece(PLACES), piece(PLACES),
            piece(PLACES), piece(PLACES), piece(PLACES),
            half(2 * PAD, channels), flat, full(pairs, rows, 8), full(pairs, 2, rows), full(LANES, channels),
            full(KERNEL - 1, rows, LANES), full(rows + PAD, LANES),
            full(*wide_shape), full(*wide_shape), full(*wide_shape), full(*wide_shape), full(*wide_shape),
            full(*wide_shape),
            half(PLACES, *quarter), half(PLACES, *quarter), half(*part), half(*part), full(PAD, LANES),
            half(REACH, *part), half(REACH, *part), full(REACH, PAD, LANES), full(REACH, PAD, LANES),
            half(PLACES, *quarter), half(PLACES, *quarter), full(PAD, LANES), full(PLACES, PAD, LANES),
            full(rows, rows), full(rows, rows), full(rows, rows), full(KERNEL, rows + 2 * PAD, LANES),
            full(rows, heads), full(rows, heads), full(rows, LANES // 2), full(rows, LANES // 2),
            flat, flat, flat, flat, half(rows, LANES), half(4, rows, LANES),
            full(red_rows, LANES), full(PLACES, red_rows, LANES), full(red_rows, LANES),
            full(groups, red_rows, LANES),
            dma(SENDS), dma(SENDS), dma(2 * PLACES), dma(2 * PLACES), dma(7), dma(3 * PLACES), dma(2), dma(8),
        ],
        name="whole",
        compiler_params=pltpu.CompilerParams(
            collective_id=0, has_side_effects=True, vmem_limit_bytes=58 * 1024 * 1024
        ),
    )(
        small, keys, values, queries, attn_grad, conv_input, gate_input, mix_grad,
    )
    steps = 4
    tall = lambda cols: pl.BlockSpec((rows // steps, cols), lambda n: (n, 0))
    piled = pl.BlockSpec((PLACES, rows // steps, head_cols), lambda n: (0, n, 0))
    whole = lambda *shape: pl.BlockSpec(shape, lambda n: (0, 0))
    *outs, conv, bias, rate, skip = pl.pallas_call(
        finish_kernel,
        grid=(steps,),
        in_specs=[piled] * 3
        + [
            tall(channels), tall(channels), whole(PAD, channels), whole(heads, rows), tall(LANES), tall(LANES),
            whole(red_rows, LANES),
        ],
        out_specs=[tall(width)] * 3
        + [tall(channels), tall(channels), whole(heads, rows), tall(LANES), tall(LANES), whole(KERNEL, channels)]
        + [whole(1, heads)] * 3,
        out_shape=[struct((rows, width), BF16)] * 3
        + [
            struct(wide_shape, BF16), struct(wide_shape, BF16), struct((heads, rows), F32),
            struct((rows, LANES), F32), struct((rows, LANES), F32), struct((KERNEL, channels), F32),
        ]
        + [struct((1, heads), F32)] * 3,
        name="finish",
        compiler_params=pltpu.CompilerParams(dimension_semantics=("arbitrary",)),
    )(*mid)
    outs[5] = outs[5].T
    return (*outs, conv, bias[0], rate[0], skip[0])


def solution(mesh):
    sharded = P("seq", "head")
    return jax.shard_map(
        local,
        mesh=mesh,
        in_specs=(
            sharded, sharded, sharded, sharded, P(), sharded, P(None, "head"), sharded,
            P("head"), P("head"), P("head"), P("seq", None), P("seq", None), sharded, sharded,
        ),
        out_specs=(
            sharded, sharded, sharded, sharded, sharded, sharded,
            P("seq", None), P("seq", None), P(None, "head"), P("head"), P("head"), P("head"),
        ),
        check_vma=False,
    )
```

```python
import jax
import jax.numpy as jnp
from jax import lax
from jax.experimental import pallas as pl
from jax.experimental.pallas import tpu as pltpu
from jax.sharding import PartitionSpec as P

HEAD_DIM = 224
WINDOW = 1024
KERNEL = 4
PAD = 8
LANES = 128
PLACES = 4
DOCS = 8
REACH = 4

EXACT = lax.Precision.HIGHEST
F32 = jnp.float32
BF16 = jnp.bfloat16
NEG_FILL = -1e30
SENDS = 79
SCALE = HEAD_DIM ** (-0.5)


def dot(a, b, ca, cb, precision=None):
    return lax.dot_general(
        a, b, (((ca,), (cb,)), ((), ())), preferred_element_type=F32, precision=precision
    )


def where_am_i():
    index = lax.axis_index("seq")
    groups = lax.axis_size("seq") // PLACES
    return lax.div(index, PLACES), lax.rem(index, PLACES), groups


def shard(group, place, groups):
    return {"seq": lax.rem(group + 2 * groups, groups) * PLACES + place}


def greet(partners):
    barrier = pltpu.get_barrier_semaphore()
    for partner in partners:
        pl.semaphore_signal(barrier, inc=1, device_id=partner, device_id_type=pl.DeviceIdType.MESH)
    return lambda: pl.semaphore_wait(barrier, len(partners))


class Post:
    def __init__(self, sends, receives):
        self.sends, self.receives, self.used = sends, receives, 0

    def send(self, source, target, device):
        copy = pltpu.make_async_remote_copy(
            src_ref=source, dst_ref=target, send_sem=self.sends.at[self.used],
            recv_sem=self.receives.at[self.used], device_id=device,
            device_id_type=pl.DeviceIdType.MESH,
        )
        self.used += 1
        copy.start()
        return copy


def spreader(heads, channels):
    width = channels // heads
    row = lax.broadcasted_iota(jnp.int32, (LANES, channels), 0)
    col = lax.broadcasted_iota(jnp.int32, (LANES, channels), 1)
    return ((col >= row * width) & (col < row * width + width)).astype(F32)


def causal(rows):
    i = lax.broadcasted_iota(jnp.int32, (rows, rows), 0)
    j = lax.broadcasted_iota(jnp.int32, (rows, rows), 1)
    return i, j


def pair_columns(cols, index, lower):
    return jnp.where(lower, cols[:, 2 * index : 2 * index + 1], cols[:, 2 * index + 1 : 2 * index + 2])


def fill_masks(since, mask_ref):
    for lag in range(1, KERNEL):
        mask_ref[lag - 1] = jnp.broadcast_to((since >= lag).astype(F32), mask_ref.shape[1:])


def conv_pre(conv, tail, wt, mask_ref, xp_ref):
    rows = conv.shape[0]
    xp_ref[:PAD, :] = tail.astype(F32)[PAD:]
    xp_ref[PAD:, :] = conv.astype(F32)
    pre = wt[0:1, :] * xp_ref[PAD:, :]
    for lag in range(1, KERNEL):
        pre = pre + wt[lag : lag + 1, :] * (xp_ref[PAD - lag : PAD - lag + rows, :] * mask_ref[lag - 1])
    return pre


def group_part(ref):
    half = ref.shape[1] // 2
    whole = ref[...].astype(F32)
    first = lax.axis_index("head") < lax.axis_size("head") // 2
    return jnp.where(first, whole[:, :half], whole[:, half:]).astype(BF16)


def fold(value, target, at=()):
    rows, (keep, quarter) = value.shape[0], (3 * value.shape[0] // 4, value.shape[0] // 4)
    target[(*at, slice(0, rows), slice(None))] = value[:, 0:LANES]
    rest, width = HEAD_DIM - LANES, LANES // 4
    target[(*at, slice(rows, rows + keep), slice(0, rest))] = value[0:keep, LANES:HEAD_DIM]
    for n in range(3):
        target[(*at, slice(rows + n * quarter, rows + (n + 1) * quarter), slice(rest, LANES))] = value[
            keep:, LANES + n * width : LANES + (n + 1) * width
        ]


def unfold(source, source_at, target, target_at, offset=0):
    rows = 4 * source.shape[-2] // 7
    keep, quarter, rest, width = 3 * rows // 4, rows // 4, HEAD_DIM - LANES, LANES // 4
    put = lambda a, b, c, d, value: target.__setitem__((*target_at, slice(a, b), slice(offset + c, offset + d)), value)
    get = lambda a, b, c, d: source[(*source_at, slice(a, b), slice(c, d))]
    put(0, rows, 0, LANES, get(0, rows, 0, LANES))
    put(0, keep, LANES, HEAD_DIM, get(rows, rows + keep, 0, rest))
    for n in range(3):
        put(
            keep, rows, LANES + n * width, LANES + (n + 1) * width,
            get(rows + n * quarter, rows + (n + 1) * quarter, rest, LANES),
        )


def whole_kernel(
    small_hbm,
    k_hbm, v_hbm, q_hbm, do_hbm, conv_hbm, gate_hbm, mix_hbm,
    dq_in, dk_in, dv_in, gconv_hbm, ggate_hbm, gfix_hbm, gstep_hbm, gin_hbm, gout_hbm, total_ref,
    small_refs, gfix_ref, gstep_ref, gin_ref, gout_ref, gconv_ref, ggate_ref, low_ref, since_ref, turn_ref, turn_back, k_ref, v_ref, q_ref, do_ref, conv_ref, gate_ref, mix_ref,
    k_pack, v_pack, q_pack, do_pack, q_in, do_in, k_in, v_in, own_fold, q_all, do_all, k_all, v_all, dk_all, dv_all,
    dk_out, dv_out, dk_back, dv_back, dq_own, dk_own, dv_own,
    tail_buf, wt_ref, cols_ref, rowc_ref, spread_ref, mask_ref, xp_ref,
    act_all, slope_all, dy_all, cg_all, inner_all, dx_all,
    ends_ref, a_ref, end_out, cot_out, g_out, e_in, c_in, ge_in, gc_in, chain_out, state_ref, t_out, t_all,
    mix_bias, pair_ref, dpair_ref, dpad_ref, z_ref, u_ref, db_ref, dc_ref,
    sums_ref, edge_ref, end_ref, spill_ref, coef_out, coef_all, red_out, red_a, red_mid, red_b,
    sends, receives, back_sends, back_receives, loads, keeps, writes, small_loads,
):
    group, place, groups = where_am_i()
    head, head_count = lax.axis_index("head"), lax.axis_size("head")
    doc_ref, step_ref, bias_ref, rate_ref, skip_ref, b_ref, c_ref, weight_ref = small_refs
    heads, rows = step_ref.shape
    channels = conv_ref.shape[1]
    pairs = channels // LANES
    peers = [lax.rem(place + d, PLACES) for d in range(1, PLACES)]
    post = Post(sends, receives)
    fetches = []
    for n, (source, target) in enumerate((
        (k_hbm, k_ref), (v_hbm, v_ref), (conv_hbm, conv_ref), (q_hbm, q_ref), (do_hbm, do_ref),
        (gate_hbm, gate_ref), (mix_hbm, mix_ref),
    )):
        fetches.append(pltpu.make_async_copy(source, target, loads.at[n]))
        fetches[-1].start()
    small_fetches = [
        pltpu.make_async_copy(source, target, small_loads.at[n])
        for n, (source, target) in enumerate(zip(small_hbm, small_refs))
    ]
    for fetch in small_fetches:
        fetch.start()
    partners = [shard(group + far, place, groups) for far in range(1, groups)]
    partners += [shard(group, peer, groups) for peer in peers]
    last, first = place == PLACES - 1, place == 0
    follower = shard(jnp.where(last, group + 1, group), lax.rem(place + 1, PLACES), groups)
    former = shard(jnp.where(first, group - 1, group), lax.rem(place + PLACES - 1, PLACES), groups)
    head_peers = [{"head": lax.rem(head + d, head_count)} for d in range(1, head_count)]
    wait_partners = greet(partners + [follower, former] + head_peers)
    ahead = shard(group + 1, place, groups)
    behind = shard(group - 1, place, groups)

    def pack(source, target):
        for r in range(PLACES):
            fold(source[:, r * HEAD_DIM : (r + 1) * HEAD_DIM], target, (r,))

    def spread(source, target, offset):
        return [
            post.send(source.at[peer], target.at[offset + place], shard(group, peer, groups)) for peer in peers
        ]

    fetches[0].wait()
    pack(k_ref, k_pack)
    fetches[2].wait()
    wait_partners()
    tail_copy = post.send(conv_ref.at[rows - 2 * PAD :, :], tail_buf, follower)
    far = [post.send(k_pack.at[place], k_in.at[place], ahead)]
    near_k = spread(k_pack, k_in, PLACES)
    fetches[1].wait()
    pack(v_ref, v_pack)
    far.append(post.send(v_pack.at[place], v_in.at[place], ahead))
    near_v = spread(v_pack, v_in, PLACES)
    fetches[3].wait()
    pack(q_ref, q_pack)
    fetches[4].wait()
    pack(do_ref, do_pack)

    for fetch in small_fetches:
        fetch.wait()
    per_row = rows // LANES
    docs = doc_ref[pl.ds(pl.multiple_of(group * PLACES * per_row, PLACES * per_row), PLACES * per_row), :]
    everyone_doc = doc_ref[...]
    begin = jnp.zeros(docs.shape, F32)
    for doc in range(1, DOCS):
        count = jnp.sum((everyone_doc < doc).astype(F32), axis=0, keepdims=True)
        count = jnp.sum(count, axis=1, keepdims=True)
        begin = jnp.where(docs == doc, count, begin)
    where = (
        lax.broadcasted_iota(jnp.int32, docs.shape, 0) * LANES
        + lax.broadcasted_iota(jnp.int32, docs.shape, 1)
        + group * (PLACES * rows)
    ).astype(F32)
    low = jnp.maximum(begin, where - (WINDOW - 1)) - (group * (PLACES * rows) - WINDOW).astype(F32)
    since_ref[...] = where - begin
    for n in range(PLACES * per_row):
        b, side = n // per_row, n % per_row
        low_ref[b : b + 1, side * LANES : (side + 1) * LANES] = low[n : n + 1]
    row = jnp.concatenate([since_ref[pl.ds(place * per_row + n, 1), :] for n in range(per_row)], axis=1)
    since = jnp.broadcast_to(row, (PAD, rows)).T[:, 0:1]

    turn_ref[...] = jnp.zeros_like(turn_ref)
    turn_ref[0:heads, :] = step_ref[...]
    raw = turn_ref[...].T[:, 0:heads] + bias_ref[...]
    step = jnp.maximum(raw, 0.0) + jnp.log1p(jnp.exp(-jnp.abs(raw)))
    rate = jnp.exp(rate_ref[...])
    log_decay = -step * rate
    i, j = causal(rows)
    tri = (i >= j).astype(F32)
    cum = dot(tri, log_decay, 1, 0, EXACT)
    row_cum = dot(log_decay, tri, 0, 1, EXACT)
    t = lax.broadcasted_iota(jnp.int32, (rows, 1), 0)
    enter = jnp.where(since > t.astype(F32), jnp.exp(cum), 0.0)
    final = cum[rows - 1 : rows]
    to_end = jnp.where((rows - 1 - t).astype(F32) <= since[rows - 1 : rows], jnp.exp(final - cum), 0.0)
    through = enter[rows - 1 : rows]
    t_out[...] = jnp.zeros_like(t_out)
    t_out[0:1, 0:heads] = through
    t_all[place] = t_out[...]
    t_copies = [post.send(t_out, t_all.at[place], shard(group, peer, groups)) for peer in peers]
    for n in range(pairs):
        two = slice(2 * n, 2 * n + 2)
        cols_ref[n] = jnp.concatenate([cum[:, two], step[:, two], enter[:, two], to_end[:, two]], axis=1)
        rowc_ref[n] = row_cum[two]
    spread_ref[...] = spreader(heads, channels)
    wt_ref[0:KERNEL, :] = weight_ref[...]
    wt_ref[KERNEL : KERNEL + 1, :] = dot(skip_ref[...], spread_ref[0:heads, :], 1, 0, EXACT)
    fill_masks(since, mask_ref)
    lower = lax.broadcasted_iota(jnp.int32, (rows, LANES), 1) < LANES // 2
    b_part, c_part = group_part(b_ref), group_part(c_ref)
    fetches[5].wait()
    fetches[6].wait()
    tail_copy.wait()

    def ends(n, carry):
        lanes = pl.ds(pl.multiple_of(n * LANES, LANES), LANES)
        cols = cols_ref[n]
        pre = conv_pre(conv_ref[:, lanes], tail_buf[:, lanes], wt_ref[:, lanes], mask_ref, xp_ref)
        sig_pre = jax.nn.sigmoid(pre)
        act = pre * sig_pre
        act_all[:, lanes] = act
        slope_all[:, lanes] = sig_pre + act * (1.0 - sig_pre)
        weighted = act * pair_columns(cols, 1, lower) * pair_columns(cols, 3, lower)
        end = dot(b_part, weighted.astype(BF16), 0, 0).astype(BF16)
        gate = gate_ref[:, lanes].astype(F32)
        sig_gate = jax.nn.sigmoid(gate)
        silu_gate = gate * sig_gate
        cot = mix_ref[:, lanes].astype(F32)
        dy = cot * silu_gate
        dy_all[:, lanes] = dy
        cg_all[:, lanes] = cot * (sig_gate + silu_gate * (1.0 - sig_gate))
        start = dot(c_part, (dy * pair_columns(cols, 2, lower)).astype(BF16), 0, 0).astype(BF16)
        for r in range(PLACES):
            part = slice(2 * PAD * r, 2 * PAD * (r + 1))
            ends_ref[r, 0, :, lanes] = end[part]
            ends_ref[r, 1, :, lanes] = start[part]
        return carry

    def pass_on(copies, target):
        for d in range(1, PLACES):
            copies[d - 1].wait()
            source = lax.rem(place + PLACES - d, PLACES)
            far.append(post.send(target.at[PLACES + source], target.at[source], ahead))

    lax.fori_loop(0, 2 * pairs // 3, ends, 0)
    pass_on(near_k, k_in)
    lax.fori_loop(2 * pairs // 3, pairs, ends, 0)

    a_copies = [post.send(ends_ref.at[peer], a_ref.at[place], shard(group, peer, groups)) for peer in peers]
    near = spread(q_pack, q_in, 0) + spread(do_pack, do_in, 0)
    a_ref[place] = ends_ref[place]
    pass_on(near_v, v_in)
    for mine, everyone, offset in (
        (k_pack, k_in, PLACES), (v_pack, v_in, PLACES), (q_pack, q_in, 0), (do_pack, do_in, 0)
    ):
        everyone[offset + place] = mine[place]

    def open_up(pairs_of, first, count):
        def one(n, carry):
            for source, target in pairs_of:
                unfold(source, (n,), target, (n,))
            return carry

        lax.fori_loop(first, first + count, one, 0)

    for ref in (k_all, v_all, q_all, do_all):
        ref[:, :, LANES:] = jnp.zeros((ref.shape[0], rows, LANES), BF16)
    open_up(((k_in, k_all), (v_in, v_all)), PLACES, PLACES)
    dk_all[...] = jnp.zeros_like(dk_all)
    dv_all[...] = jnp.zeros_like(dv_all)

    mix_bias[...] = jnp.where((i >= j) & ((i - j).astype(F32) <= since), 0.0, NEG_FILL)
    pair_ref[...] = dot(c_part, b_part, 1, 1)
    for ref in (dpair_ref, z_ref, u_ref, db_ref, dc_ref, dpad_ref, red_out):
        ref[...] = jnp.zeros_like(ref)

    def within(n, carry):
        lanes = pl.ds(pl.multiple_of(n * LANES, LANES), LANES)
        cols = cols_ref[n]
        x_half = (act_all[:, lanes] * pair_columns(cols, 1, lower)).astype(BF16)
        dy_half = dy_all[:, lanes].astype(BF16)
        zero = jnp.zeros_like(dy_half)
        y_parts, dx_parts = [], []
        dpair = dpair_ref[...]
        rowc = rowc_ref[n]
        for k in range(2):
            weights = jnp.exp((cols[:, k : k + 1] - rowc[k : k + 1, :]) + mix_bias[...])
            mixing = (pair_ref[...] * weights).astype(BF16)
            y_parts.append(dot(mixing, x_half, 1, 0))
            dx_parts.append(dot(mixing, dy_half, 0, 0))
            dy_one = jnp.where(lower if k == 0 else ~lower, dy_half, zero)
            dpair = dpair + dot(dy_one, x_half, 1, 1) * weights
        dpair_ref[...] = dpair
        inner_all[:, lanes] = jnp.where(lower, y_parts[0], y_parts[1])
        dx_all[:, lanes] = jnp.where(lower, dx_parts[0], dx_parts[1])
        return carry

    lax.fori_loop(0, pairs // 3, within, 0)
    for copy in t_copies + a_copies:
        copy.wait()
    decays = dot(t_all[...].reshape(PLACES * PAD, LANES), spread_ref[...], 1, 0, EXACT)
    decay = [decays[PAD * n : PAD * n + 1] for n in range(PLACES)]
    end_of = lambda n: a_ref[n, 0].astype(F32)
    cot_of = lambda n: a_ref[n, 1].astype(F32)
    end, cot = end_of(0), cot_of(PLACES - 1)
    for n in range(1, PLACES):
        end = end_of(n) + decay[n] * end
        cot = cot_of(PLACES - 1 - n) + decay[PLACES - 1 - n] * cot
    end_out[...] = end.astype(BF16)
    cot_out[...] = cot.astype(BF16)
    g_out[...] = t_all[0] * t_all[1] * t_all[2] * t_all[3]
    b_copies = []
    for away in range(1, REACH + 1):
        later, earlier = shard(group + away, place, groups), shard(group - away, place, groups)
        b_copies.append(post.send(g_out, ge_in.at[away - 1], later))
        b_copies.append(post.send(g_out, gc_in.at[away - 1], earlier))
        b_copies.append(post.send(end_out, e_in.at[away - 1], later))
        b_copies.append(post.send(cot_out, c_in.at[away - 1], earlier))
    lax.fori_loop(pairs // 3, pairs, within, 0)
    dpair = dpair_ref[...]
    dc_ref[...] = dot(dpair, b_part.astype(F32), 1, 0, EXACT)
    db_ref[...] = dot(dpair, c_part.astype(F32), 0, 0, EXACT)
    for copy in near:
        copy.wait()
    open_up(((q_in, q_all), (do_in, do_all)), 0, PLACES)
    for copy in far:
        copy.wait()
    open_up(((k_in, k_all), (v_in, v_all)), 0, PLACES)

    def back_copy(source, target, b, n):
        return pltpu.make_async_remote_copy(
            src_ref=source.at[b], dst_ref=target.at[b], send_sem=back_sends.at[n],
            recv_sem=back_receives.at[n], device_id=behind, device_id_type=pl.DeviceIdType.MESH,
        )

    below = i.astype(F32)

    def block(b, carry):
        q = q_all[b]
        grad = do_all[b]
        low = low_ref[pl.ds(b, 1), :]
        at = [b + PLACES - gap for gap in range(PLACES + 1)]
        scores = []
        top = None
        for gap in range(PLACES + 1):
            allowed = below >= low - jnp.asarray(at[gap] * rows).astype(F32)
            if gap == 0:
                allowed = allowed & (j >= i)
            s = jnp.where(allowed, dot(k_all[at[gap]], q, 1, 1) * SCALE, NEG_FILL)
            scores.append(s)
            m = jnp.max(s, axis=0, keepdims=True)
            top = m if top is None else jnp.maximum(top, m)
        total = None
        expo = []
        for gap in range(PLACES + 1):
            e = jnp.exp(scores[gap] - top)
            expo.append(e)
            e_sum = jnp.sum(e, axis=0, keepdims=True)
            total = e_sum if total is None else total + e_sum
        inverse = 1.0 / jnp.maximum(total, 1.0)
        delta = None
        dprobs = []
        for gap in range(PLACES + 1):
            half = (expo[gap] * inverse).astype(BF16)
            dp = dot(v_all[at[gap]], grad, 1, 1)
            d = jnp.sum(half.astype(F32) * dp, axis=0, keepdims=True)
            delta = d if delta is None else delta + d
            dv_all[at[gap]] += dot(half, grad, 1, 0)
            dprobs.append(dp)
        dq = None
        for gap in range(PLACES + 1):
            ds = (expo[gap] * inverse * (dprobs[gap] - delta)).astype(BF16)
            dk_all[at[gap]] += dot(ds, q, 1, 0)
            part = dot(ds, k_all[at[gap]], 0, 0)
            dq = part if dq is None else dq + part
        fold((dq * SCALE).astype(BF16), dq_own, (b,))
        fold(dk_all[b].astype(BF16), dk_out, (b,))
        back_copy(dk_out, dk_back, b, b).start()
        fold(dv_all[b].astype(BF16), dv_out, (b,))
        return carry

    lax.fori_loop(0, PLACES // 2, block, 0)
    for copy in b_copies:
        copy.wait()
    before = dot(ge_in[...].reshape(REACH * PAD, LANES), spread_ref[...], 1, 0, EXACT)
    after = dot(gc_in[...].reshape(REACH * PAD, LANES), spread_ref[...], 1, 0, EXACT)
    state = e_in[REACH - 1].astype(F32)
    cot = c_in[REACH - 1].astype(F32) * (group + REACH < groups).astype(F32)
    for away in range(REACH - 2, -1, -1):
        state = e_in[away].astype(F32) + before[PAD * away : PAD * away + 1] * state
        cot = (c_in[away].astype(F32) + after[PAD * away : PAD * away + 1] * cot) * (
            group + away + 1 < groups
        ).astype(F32)
    for n in range(PLACES):
        chain_out[n, 0] = state.astype(BF16)
        state = end_of(n) + decay[n] * state
        m = PLACES - 1 - n
        chain_out[m, 1] = cot.astype(BF16)
        cot = cot_of(m) + decay[m] * cot
    state_copies = [
        post.send(chain_out.at[peer], state_ref.at[place], shard(group, peer, groups)) for peer in peers
    ]
    state_ref[place] = chain_out[place]

    lax.fori_loop(PLACES // 2, PLACES, block, 0)
    for b in range(PLACES):
        back_copy(dv_out, dv_back, b, PLACES + b).start()
    kept = []

    def give_back(source, target):
        copies = spread(source, target, 0)
        copies.append(pltpu.make_async_copy(source.at[place], target.at[place], keeps.at[len(kept)]))
        copies[-1].start()
        kept.extend(copies)

    give_back(dq_own, dq_in)

    def across(n, carry):
        lanes = pl.ds(pl.multiple_of(n * LANES, LANES), LANES)
        cols = cols_ref[n]
        wt = wt_ref[:, lanes]
        size = pair_columns(cols, 1, lower)
        enter = pair_columns(cols, 2, lower)
        to_end = pair_columns(cols, 3, lower)
        xp_ref[:PAD, :] = tail_buf[:, lanes].astype(F32)[PAD:]
        xp_ref[PAD:, :] = conv_ref[:, lanes].astype(F32)
        act = act_all[:, lanes]
        dy = dy_all[:, lanes]
        x_wide = (act * size).astype(BF16).astype(F32)
        state = jnp.concatenate([state_ref[r, 0, :, lanes] for r in range(PLACES)], axis=0)
        end_cot = jnp.concatenate([state_ref[r, 1, :, lanes] for r in range(PLACES)], axis=0)
        inner = inner_all[:, lanes] + enter * dot(c_part, state, 1, 0)
        end_part = to_end * dot(b_part, end_cot, 1, 0)
        dx = dx_all[:, lanes] + end_part
        skip = wt[KERNEL : KERNEL + 1, :]
        ggate_ref[:, lanes] = (cg_all[:, lanes] * (inner + skip * act)).astype(BF16)
        zed = dy.astype(BF16).astype(F32) * inner - x_wide * dx
        you = dx * act
        for k in range(2):
            side = lower if k == 0 else ~lower
            here = lane == 2 * n + k
            z_one = jnp.sum(jnp.where(side, zed, 0.0), axis=1, keepdims=True)
            u_one = jnp.sum(jnp.where(side, you, 0.0), axis=1, keepdims=True)
            z_ref[...] = jnp.where(here, z_one, z_ref[...])
            u_ref[...] = jnp.where(here, u_one, u_ref[...])
        dc_ref[...] += dot((enter * dy).astype(BF16), state, 1, 1)
        db_ref[...] += dot((to_end * x_wide).astype(BF16), end_cot, 1, 1)
        dpre = (dx * size + skip * dy) * slope_all[:, lanes]
        red_out[pl.ds(KERNEL * n, 1), :] = jnp.sum(dpre * xp_ref[PAD:, :], axis=0, keepdims=True)
        dpad_ref[0, PAD : PAD + rows, :] = dpre
        grown = wt[0:1, :] * dpad_ref[0, 0 : rows + PAD, :]
        for lag in range(1, KERNEL):
            masked = dpre * mask_ref[lag - 1]
            red_out[pl.ds(KERNEL * n + lag, 1), :] = jnp.sum(
                masked * xp_ref[PAD - lag : PAD - lag + rows, :], axis=0, keepdims=True
            )
            dpad_ref[lag, PAD : PAD + rows, :] = masked
            grown = grown + wt[lag : lag + 1, :] * dpad_ref[lag, lag : lag + rows + PAD, :]
        gconv_ref[:, lanes] = grown[PAD:, :].astype(BF16)
        edge_ref[:, lanes] = grown[:PAD, :]
        end_ref[:, lanes] = grown[rows:, :]
        sums_ref[0:1, lanes] = jnp.sum(dy * act, axis=0, keepdims=True)
        sums_ref[1:2, lanes] = jnp.sum(state.astype(F32) * end_cot.astype(F32), axis=0, keepdims=True)
        sums_ref[2:3, lanes] = jnp.sum(x_wide * end_part, axis=0, keepdims=True)
        sums_ref[3:8, lanes] = jnp.zeros((5, LANES), F32)
        return carry

    def whole_sum(source, target, total, out, offset, factor):
        for b in range(PLACES):
            fold(total[PLACES + b], own_fold)
            back_copy(source, target, b, offset + b).wait()
            out[b] = ((own_fold[...] + target[b].astype(F32)) * factor).astype(BF16)

    lane = lax.broadcasted_iota(jnp.int32, (rows, heads), 1)
    for copy in state_copies:
        copy.wait()
    def exchange(part):
        return [
            post.send(red_out.at[part], red_a.at[place, part], shard(group, peer, groups)) for peer in peers
        ]

    def widen(part, copies):
        red_a[place, part] = red_out[part]
        for copy in copies:
            copy.wait()
        red_mid[part] = red_a[0, part] + red_a[1, part] + red_a[2, part] + red_a[3, part]
        red_b[group, part] = red_mid[part]
        return [
            post.send(red_mid.at[part], red_b.at[group, part], shard(group + away, place, groups))
            for away in range(1, groups)
        ]

    upper, under = pl.ds(0, 4 * PAD), pl.ds(4 * PAD, 4 * PAD)
    lax.fori_loop(0, 4 * PAD // KERNEL, across, 0)
    early = exchange(upper)
    whole_sum(dk_out, dk_back, dk_all, dk_own, 0, SCALE)
    give_back(dk_own, dk_in)
    lax.fori_loop(4 * PAD // KERNEL, pairs, across, 0)
    wide = widen(upper, early)
    written = []

    def write(source, target):
        written.append(pltpu.make_async_copy(source, target, writes.at[len(written)]))
        written[-1].start()

    write(gconv_ref, gconv_hbm)
    write(ggate_ref, ggate_hbm)

    spill_copy = post.send(edge_ref, spill_ref, former)
    per_head = dot(sums_ref[...], spread_ref[...], 1, 1, EXACT)[:, 0:heads]
    last_row = per_head[2:3] + through * per_head[1:2]
    dcum = z_ref[...] + jnp.where(t == rows - 1, last_row, 0.0)
    dlog = dot(tri, dcum, 0, 0, EXACT)
    grad_step = (u_ref[...] - dlog * rate) * jax.nn.sigmoid(raw)
    turn_back[...] = jnp.zeros_like(turn_back)
    turn_back[:, 0:heads] = grad_step
    gstep_ref[...] = turn_back[...].T[0:heads, :]
    write(gstep_ref, gstep_hbm)
    small = KERNEL * pairs
    red_out[small : small + 1, 0:heads] = jnp.sum(grad_step, axis=0, keepdims=True)
    red_out[small + 1 : small + 2, 0:heads] = jnp.sum(dlog * log_decay, axis=0, keepdims=True)
    red_out[small + 2 : small + 3, 0:heads] = per_head[0:1]
    reds = exchange(under)
    coef_out[...] = jnp.concatenate([db_ref[...], dc_ref[...]], axis=1).astype(BF16)
    coefs = [post.send(coef_out, coef_all.at[head], peer) for peer in head_peers]
    coef_all[head] = coef_out[...]
    wide += widen(under, reds)
    whole_sum(dv_out, dv_back, dv_all, dv_own, PLACES, 1.0)
    give_back(dv_own, dv_in)
    spill_copy.wait()
    gfix_ref[...] = end_ref[...] + spill_ref[...]
    write(gfix_ref, gfix_hbm)
    for copy in coefs:
        copy.wait()
    halves = [coef_all[2 * n].astype(F32) + coef_all[2 * n + 1].astype(F32) for n in range(2)]
    half = coef_out.shape[1] // 2
    gin_ref[...] = jnp.concatenate([halves[0][:, :half], halves[1][:, :half]], axis=1)
    gout_ref[...] = jnp.concatenate([halves[0][:, half:], halves[1][:, half:]], axis=1)
    write(gin_ref, gin_hbm)
    write(gout_ref, gout_hbm)
    for copy in wide:
        copy.wait()
    total = red_b[0]
    for n in range(1, groups):
        total = total + red_b[n]
    total_ref[...] = total
    for copy in kept + written:
        copy.wait()


def finish_kernel(ins, outs, in_bufs, out_bufs, load_sems, store_sems):
    loads = [pltpu.make_async_copy(a, b, load_sems.at[n]) for n, (a, b) in enumerate(zip(ins, in_bufs))]
    for load in loads:
        load.start()
    stores = []

    def store(source, target):
        stores.append(pltpu.make_async_copy(source, target, store_sems.at[len(stores)]))
        stores[-1].start()

    total, fix, gconv = in_bufs[0], in_bufs[1], in_bufs[2]
    for load in loads[:3]:
        load.wait()
    gconv[gconv.shape[0] - PAD :, :] = fix[...].astype(BF16)
    store(gconv, outs[3])
    conv, *small = out_bufs[3:]
    pairs, heads = conv.shape[1] // LANES, small[0].shape[1]
    for lag in range(KERNEL):
        for n in range(pairs):
            row = KERNEL * n + lag
            conv[lag : lag + 1, n * LANES : (n + 1) * LANES] = total[row : row + 1, :]
    for n, ref in enumerate(small):
        row = KERNEL * pairs + n
        ref[...] = total[row : row + 1, 0:heads]
    for n, ref in enumerate((conv, *small)):
        store(ref, outs[8 + n])
    for n in range(3, 7):
        loads[n].wait()
        store(in_bufs[n], outs[n + 1])
    for n in range(3):
        loads[7 + n].wait()
        for r in range(PLACES):
            unfold(in_bufs[7 + n], (r,), out_bufs[n], (), r * HEAD_DIM)
        store(out_bufs[n], outs[n])
    for copy in stores:
        copy.wait()


def local(
    queries, keys, values, attn_grad, doc_ids, conv_input, conv_weight, step_raw, step_bias,
    rate_log, skip_gain, input_coeff, output_coeff, gate_input, mix_grad,
):
    rows, width = queries.shape
    heads, channels = step_raw.shape[1], conv_input.shape[1]
    pairs = channels // LANES
    groups = lax.axis_size("seq") // PLACES
    struct = jax.ShapeDtypeStruct
    vmem = pl.BlockSpec(memory_space=pltpu.VMEM)
    loose = pl.BlockSpec(memory_space=pl.ANY)
    dma = lambda n: pltpu.SemaphoreType.DMA((n,))
    head_cols = 2 * LANES
    quarter = (2, 2 * PAD, channels)
    part = quarter[1:]
    half = lambda *shape: pltpu.VMEM(shape, BF16)
    full = lambda *shape: pltpu.VMEM(shape, F32)
    flat = full(PAD, channels)
    piece = lambda n: half(n, rows, head_cols)
    slim_rows = rows * HEAD_DIM // LANES
    slim = lambda n: half(n, slim_rows, LANES)
    red_rows = 64
    wide_shape = (rows, channels)
    small = [
        doc_ids.reshape(-1, LANES), step_raw.T, step_bias[None], rate_log[None], skip_gain[None],
        input_coeff, output_coeff, conv_weight,
    ]
    mid = pl.pallas_call(
        whole_kernel,
        in_specs=[[loose] * 8] + [loose] * 7,
        out_specs=[loose] * 9 + [vmem],
        out_shape=[struct((PLACES, slim_rows, LANES), BF16)] * 3
        + [
            struct(wide_shape, BF16), struct(wide_shape, BF16), struct((PAD, channels), F32),
            struct((heads, rows), F32), struct((rows, LANES), F32), struct((rows, LANES), F32),
            struct((red_rows, LANES), F32),
        ],
        scratch_shapes=[
            [pltpu.VMEM(a.shape, a.dtype) for a in small],
            flat, full(heads, rows), full(rows, LANES), full(rows, LANES), half(*wide_shape), half(*wide_shape),
            full(PAD, rows), full(PLACES * rows // LANES, LANES), full(LANES, rows), full(rows, LANES),
            half(rows, width), half(rows, width), half(rows, width), half(rows, width),
            half(*wide_shape), half(*wide_shape), half(*wide_shape),
            slim(PLACES), slim(PLACES), slim(PLACES), slim(PLACES),
            slim(PLACES), slim(PLACES), slim(2 * PLACES), slim(2 * PLACES), full(slim_rows, LANES),
            piece(PLACES), piece(PLACES), piece(2 * PLACES), piece(2 * PLACES),
            full(2 * PLACES, rows, head_cols), full(2 * PLACES, rows, head_cols),
            slim(PLACES), slim(PLACES), slim(PLACES), slim(PLACES),
            slim(PLACES), slim(PLACES), slim(PLACES),
            half(2 * PAD, channels), flat, full(pairs, rows, 8), full(pairs, 2, rows), full(LANES, channels),
            full(KERNEL - 1, rows, LANES), full(rows + PAD, LANES),
            full(*wide_shape), full(*wide_shape), full(*wide_shape), full(*wide_shape), full(*wide_shape),
            full(*wide_shape),
            half(PLACES, *quarter), half(PLACES, *quarter), half(*part), half(*part), full(PAD, LANES),
            half(REACH, *part), half(REACH, *part), full(REACH, PAD, LANES), full(REACH, PAD, LANES),
            half(PLACES, *quarter), half(PLACES, *quarter), full(PAD, LANES), full(PLACES, PAD, LANES),
            full(rows, rows), full(rows, rows), full(rows, rows), full(KERNEL, rows + 2 * PAD, LANES),
            full(rows, heads), full(rows, heads), full(rows, LANES // 2), full(rows, LANES // 2),
            flat, flat, flat, flat, half(rows, LANES), half(4, rows, LANES),
            full(red_rows, LANES), full(PLACES, red_rows, LANES), full(red_rows, LANES),
            full(groups, red_rows, LANES),
            dma(SENDS), dma(SENDS), dma(2 * PLACES), dma(2 * PLACES), dma(7), dma(3 * PLACES), dma(6), dma(8),
        ],
        name="whole",
        compiler_params=pltpu.CompilerParams(
            collective_id=0, has_side_effects=True, vmem_limit_bytes=58 * 1024 * 1024
        ),
    )(
        small, keys, values, queries, attn_grad, conv_input, gate_input, mix_grad,
    )
    dq, dk, dv, gconv, ggate, gfix, gstep, gin, gout, total = mid
    ins = [total, gfix, gconv, ggate, gstep, gin, gout, dq, dk, dv]
    shapes = [struct((rows, width), BF16)] * 3 + [
        struct(wide_shape, BF16), struct(wide_shape, BF16), struct((heads, rows), F32),
        struct((rows, LANES), F32), struct((rows, LANES), F32), struct((KERNEL, channels), F32),
    ] + [struct((1, heads), F32)] * 3
    *outs, conv, bias, rate, skip = pl.pallas_call(
        finish_kernel,
        in_specs=[[loose] * len(ins)],
        out_specs=[[loose] * len(shapes)],
        out_shape=[shapes],
        scratch_shapes=[
            [pltpu.VMEM(a.shape, a.dtype) for a in ins],
            [pltpu.VMEM(shapes[n].shape, shapes[n].dtype) for n in (0, 1, 2, 8, 9, 10, 11)],
            dma(len(ins)), dma(len(shapes)),
        ],
        name="finish",
    )(ins)[0]
    outs[5] = outs[5].T
    return (*outs, conv, bias[0], rate[0], skip[0])


def solution(mesh):
    sharded = P("seq", "head")
    return jax.shard_map(
        local,
        mesh=mesh,
        in_specs=(
            sharded, sharded, sharded, sharded, P(), sharded, P(None, "head"), sharded,
            P("head"), P("head"), P("head"), P("seq", None), P("seq", None), sharded, sharded,
        ),
        out_specs=(
            sharded, sharded, sharded, sharded, sharded, sharded,
            P("seq", None), P("seq", None), P(None, "head"), P("head"), P("head"), P("head"),
        ),
        check_vma=False,
    )
```

```python
import jax
import jax.numpy as jnp
from jax import lax
from jax.experimental import pallas as pl
from jax.experimental.pallas import tpu as pltpu
from jax.sharding import PartitionSpec as P

HEAD_DIM = 224
WINDOW = 1024
KERNEL = 4
PAD = 8
LANES = 128
PLACES = 4
DOCS = 8
REACH = 4

EXACT = lax.Precision.HIGHEST
F32 = jnp.float32
BF16 = jnp.bfloat16
NEG_FILL = -1e30
SENDS = 79
SCALE = HEAD_DIM ** (-0.5)


def dot(a, b, ca, cb, precision=None):
    return lax.dot_general(
        a, b, (((ca,), (cb,)), ((), ())), preferred_element_type=F32, precision=precision
    )


def where_am_i():
    index = lax.axis_index("seq")
    groups = lax.axis_size("seq") // PLACES
    return lax.div(index, PLACES), lax.rem(index, PLACES), groups


def shard(group, place, groups):
    return {"seq": lax.rem(group + 2 * groups, groups) * PLACES + place}


def greet(partners):
    barrier = pltpu.get_barrier_semaphore()
    for partner in partners:
        pl.semaphore_signal(barrier, inc=1, device_id=partner, device_id_type=pl.DeviceIdType.MESH)
    return lambda: pl.semaphore_wait(barrier, len(partners))


class Post:
    def __init__(self, sends, receives):
        self.sends, self.receives, self.used = sends, receives, 0

    def send(self, source, target, device):
        copy = pltpu.make_async_remote_copy(
            src_ref=source, dst_ref=target, send_sem=self.sends.at[self.used],
            recv_sem=self.receives.at[self.used], device_id=device,
            device_id_type=pl.DeviceIdType.MESH,
        )
        self.used += 1
        copy.start()
        return copy


def spreader(heads, channels):
    width = channels // heads
    row = lax.broadcasted_iota(jnp.int32, (LANES, channels), 0)
    col = lax.broadcasted_iota(jnp.int32, (LANES, channels), 1)
    return ((col >= row * width) & (col < row * width + width)).astype(F32)


def causal(rows):
    i = lax.broadcasted_iota(jnp.int32, (rows, rows), 0)
    j = lax.broadcasted_iota(jnp.int32, (rows, rows), 1)
    return i, j


def pair_columns(cols, index, lower):
    return jnp.where(lower, cols[:, 2 * index : 2 * index + 1], cols[:, 2 * index + 1 : 2 * index + 2])


def fill_masks(since, mask_ref):
    for lag in range(1, KERNEL):
        mask_ref[lag - 1] = jnp.broadcast_to((since >= lag).astype(F32), mask_ref.shape[1:])


def conv_pre(conv, tail, wt, mask_ref, xp_ref, lanes):
    rows = conv.shape[0]
    xp_ref[:PAD, lanes] = tail.astype(F32)[PAD:]
    xp_ref[PAD:, lanes] = conv.astype(F32)
    pre = wt[0:1, :] * conv.astype(F32)
    for lag in range(1, KERNEL):
        pre = pre + wt[lag : lag + 1, :] * (xp_ref[PAD - lag : PAD - lag + rows, lanes] * mask_ref[lag - 1])
    return pre


def group_part(ref):
    half = ref.shape[1] // 2
    whole = ref[...].astype(F32)
    first = lax.axis_index("head") < lax.axis_size("head") // 2
    return jnp.where(first, whole[:, :half], whole[:, half:]).astype(BF16)


def fold(value, target, at=()):
    rows, (keep, quarter) = value.shape[0], (3 * value.shape[0] // 4, value.shape[0] // 4)
    target[(*at, slice(0, rows), slice(None))] = value[:, 0:LANES]
    rest, width = HEAD_DIM - LANES, LANES // 4
    target[(*at, slice(rows, rows + keep), slice(0, rest))] = value[0:keep, LANES:HEAD_DIM]
    for n in range(3):
        target[(*at, slice(rows + n * quarter, rows + (n + 1) * quarter), slice(rest, LANES))] = value[
            keep:, LANES + n * width : LANES + (n + 1) * width
        ]


def unfold(source, source_at, target, target_at, offset=0):
    rows = 4 * source.shape[-2] // 7
    keep, quarter, rest, width = 3 * rows // 4, rows // 4, HEAD_DIM - LANES, LANES // 4
    put = lambda a, b, c, d, value: target.__setitem__((*target_at, slice(a, b), slice(offset + c, offset + d)), value)
    get = lambda a, b, c, d: source[(*source_at, slice(a, b), slice(c, d))]
    put(0, rows, 0, LANES, get(0, rows, 0, LANES))
    put(0, keep, LANES, HEAD_DIM, get(rows, rows + keep, 0, rest))
    for n in range(3):
        put(
            keep, rows, LANES + n * width, LANES + (n + 1) * width,
            get(rows + n * quarter, rows + (n + 1) * quarter, rest, LANES),
        )


def whole_kernel(
    small_hbm,
    k_hbm, v_hbm, q_hbm, do_hbm, conv_hbm, gate_hbm, mix_hbm,
    dq_in, dk_in, dv_in, gconv_hbm, ggate_hbm, gfix_hbm, gstep_hbm, gin_hbm, gout_hbm, total_ref,
    small_refs, gfix_ref, gstep_ref, gin_ref, gout_ref, gconv_ref, ggate_ref, low_ref, since_ref, turn_ref, turn_back, k_ref, v_ref, q_ref, do_ref, conv_ref, gate_ref, mix_ref,
    k_pack, v_pack, q_pack, do_pack, q_in, do_in, k_in, v_in, own_fold, q_all, do_all, k_all, v_all, dk_all, dv_all,
    dk_out, dv_out, dk_back, dv_back, dq_own, dk_own, dv_own,
    tail_buf, wt_ref, cols_ref, rowc_ref, spread_ref, mask_ref, xp_ref,
    act_all, slope_all, dy_all, cg_all, inner_all, dx_all,
    ends_ref, a_ref, end_out, cot_out, g_out, e_in, c_in, ge_in, gc_in, chain_out, state_ref, t_out, t_all,
    mix_bias, pair_ref, dpair_ref, dpad_ref, zu_ref, db_ref, dc_ref,
    sums_ref, edge_ref, end_ref, spill_ref, coef_out, coef_all, red_out, red_a, red_mid, red_b,
    sends, receives, back_sends, back_receives, loads, keeps, writes, small_loads,
):
    group, place, groups = where_am_i()
    head, head_count = lax.axis_index("head"), lax.axis_size("head")
    doc_ref, step_ref, bias_ref, rate_ref, skip_ref, b_ref, c_ref, weight_ref = small_refs
    heads, rows = step_ref.shape
    channels = conv_ref.shape[1]
    pairs = channels // LANES
    peers = [lax.rem(place + d, PLACES) for d in range(1, PLACES)]
    post = Post(sends, receives)
    fetches = []
    for n, (source, target) in enumerate((
        (k_hbm, k_ref), (v_hbm, v_ref), (conv_hbm, conv_ref), (q_hbm, q_ref), (do_hbm, do_ref),
        (gate_hbm, gate_ref), (mix_hbm, mix_ref),
    )):
        fetches.append(pltpu.make_async_copy(source, target, loads.at[n]))
        fetches[-1].start()
    small_fetches = [
        pltpu.make_async_copy(source, target, small_loads.at[n])
        for n, (source, target) in enumerate(zip(small_hbm, small_refs))
    ]
    for fetch in small_fetches:
        fetch.start()
    partners = [shard(group + far, place, groups) for far in range(1, groups)]
    partners += [shard(group, peer, groups) for peer in peers]
    last, first = place == PLACES - 1, place == 0
    follower = shard(jnp.where(last, group + 1, group), lax.rem(place + 1, PLACES), groups)
    former = shard(jnp.where(first, group - 1, group), lax.rem(place + PLACES - 1, PLACES), groups)
    head_peers = [{"head": lax.rem(head + d, head_count)} for d in range(1, head_count)]
    wait_partners = greet(partners + [follower, former] + head_peers)
    ahead = shard(group + 1, place, groups)
    behind = shard(group - 1, place, groups)

    def pack(source, target):
        for r in range(PLACES):
            fold(source[:, r * HEAD_DIM : (r + 1) * HEAD_DIM], target, (r,))

    def spread(source, target, offset):
        return [
            post.send(source.at[peer], target.at[offset + place], shard(group, peer, groups)) for peer in peers
        ]

    fetches[0].wait()
    pack(k_ref, k_pack)
    fetches[2].wait()
    wait_partners()
    tail_copy = post.send(conv_ref.at[rows - 2 * PAD :, :], tail_buf, follower)
    far = [post.send(k_pack.at[place], k_in.at[place], ahead)]
    near_k = spread(k_pack, k_in, PLACES)
    fetches[1].wait()
    pack(v_ref, v_pack)
    far.append(post.send(v_pack.at[place], v_in.at[place], ahead))
    near_v = spread(v_pack, v_in, PLACES)
    fetches[3].wait()
    pack(q_ref, q_pack)
    fetches[4].wait()
    pack(do_ref, do_pack)

    for fetch in small_fetches:
        fetch.wait()
    per_row = rows // LANES
    docs = doc_ref[pl.ds(pl.multiple_of(group * PLACES * per_row, PLACES * per_row), PLACES * per_row), :]
    everyone_doc = doc_ref[...]
    begin = jnp.zeros(docs.shape, F32)
    for doc in range(1, DOCS):
        count = jnp.sum((everyone_doc < doc).astype(F32), axis=0, keepdims=True)
        count = jnp.sum(count, axis=1, keepdims=True)
        begin = jnp.where(docs == doc, count, begin)
    where = (
        lax.broadcasted_iota(jnp.int32, docs.shape, 0) * LANES
        + lax.broadcasted_iota(jnp.int32, docs.shape, 1)
        + group * (PLACES * rows)
    ).astype(F32)
    low = jnp.maximum(begin, where - (WINDOW - 1)) - (group * (PLACES * rows) - WINDOW).astype(F32)
    since_ref[...] = where - begin
    for n in range(PLACES * per_row):
        b, side = n // per_row, n % per_row
        low_ref[b : b + 1, side * LANES : (side + 1) * LANES] = low[n : n + 1]
    row = jnp.concatenate([since_ref[pl.ds(place * per_row + n, 1), :] for n in range(per_row)], axis=1)
    since = jnp.broadcast_to(row, (PAD, rows)).T[:, 0:1]

    turn_ref[...] = jnp.zeros_like(turn_ref)
    turn_ref[0:heads, :] = step_ref[...]
    raw = turn_ref[...].T[:, 0:heads] + bias_ref[...]
    step = jnp.maximum(raw, 0.0) + jnp.log1p(jnp.exp(-jnp.abs(raw)))
    rate = jnp.exp(rate_ref[...])
    log_decay = -step * rate
    i, j = causal(rows)
    tri = (i >= j).astype(F32)
    cum = dot(tri, log_decay, 1, 0, EXACT)
    row_cum = dot(log_decay, tri, 0, 1, EXACT)
    t = lax.broadcasted_iota(jnp.int32, (rows, 1), 0)
    enter = jnp.where(since > t.astype(F32), jnp.exp(cum), 0.0)
    final = cum[rows - 1 : rows]
    to_end = jnp.where((rows - 1 - t).astype(F32) <= since[rows - 1 : rows], jnp.exp(final - cum), 0.0)
    through = enter[rows - 1 : rows]
    t_out[...] = jnp.zeros_like(t_out)
    t_out[0:1, 0:heads] = through
    t_all[place] = t_out[...]
    t_copies = [post.send(t_out, t_all.at[place], shard(group, peer, groups)) for peer in peers]
    for n in range(pairs):
        two = slice(2 * n, 2 * n + 2)
        cols_ref[n] = jnp.concatenate([cum[:, two], step[:, two], enter[:, two], to_end[:, two]], axis=1)
        rowc_ref[n] = row_cum[two]
    spread_ref[...] = spreader(heads, channels)
    wt_ref[0:KERNEL, :] = weight_ref[...]
    wt_ref[KERNEL : KERNEL + 1, :] = dot(skip_ref[...], spread_ref[0:heads, :], 1, 0, EXACT)
    fill_masks(since, mask_ref)
    lower = lax.broadcasted_iota(jnp.int32, (rows, LANES), 1) < LANES // 2
    b_part, c_part = group_part(b_ref), group_part(c_ref)
    fetches[5].wait()
    fetches[6].wait()
    tail_copy.wait()

    def ends(n, carry):
        lanes = pl.ds(pl.multiple_of(n * LANES, LANES), LANES)
        cols = cols_ref[n]
        pre = conv_pre(conv_ref[:, lanes], tail_buf[:, lanes], wt_ref[:, lanes], mask_ref, xp_ref, lanes)
        sig_pre = jax.nn.sigmoid(pre)
        act = pre * sig_pre
        act_all[:, lanes] = act
        slope_all[:, lanes] = sig_pre + act * (1.0 - sig_pre)
        weighted = act * pair_columns(cols, 1, lower) * pair_columns(cols, 3, lower)
        end = dot(b_part, weighted.astype(BF16), 0, 0).astype(BF16)
        gate = gate_ref[:, lanes].astype(F32)
        sig_gate = jax.nn.sigmoid(gate)
        silu_gate = gate * sig_gate
        cot = mix_ref[:, lanes].astype(F32)
        dy = cot * silu_gate
        dy_all[:, lanes] = dy
        cg_all[:, lanes] = cot * (sig_gate + silu_gate * (1.0 - sig_gate))
        start = dot(c_part, (dy * pair_columns(cols, 2, lower)).astype(BF16), 0, 0).astype(BF16)
        for r in range(PLACES):
            part = slice(2 * PAD * r, 2 * PAD * (r + 1))
            ends_ref[r, 0, :, lanes] = end[part]
            ends_ref[r, 1, :, lanes] = start[part]
        return carry

    def pass_on(copies, target):
        for d in range(1, PLACES):
            copies[d - 1].wait()
            source = lax.rem(place + PLACES - d, PLACES)
            far.append(post.send(target.at[PLACES + source], target.at[source], ahead))

    lax.fori_loop(0, 2 * pairs // 3, ends, 0)
    pass_on(near_k, k_in)
    lax.fori_loop(2 * pairs // 3, pairs, ends, 0)

    a_copies = [post.send(ends_ref.at[peer], a_ref.at[place], shard(group, peer, groups)) for peer in peers]
    near = spread(q_pack, q_in, 0) + spread(do_pack, do_in, 0)
    a_ref[place] = ends_ref[place]
    pass_on(near_v, v_in)
    for mine, everyone, offset in (
        (k_pack, k_in, PLACES), (v_pack, v_in, PLACES), (q_pack, q_in, 0), (do_pack, do_in, 0)
    ):
        everyone[offset + place] = mine[place]

    def open_up(pairs_of, first, count):
        def one(n, carry):
            for source, target in pairs_of:
                unfold(source, (n,), target, (n,))
            return carry

        lax.fori_loop(first, first + count, one, 0)

    for ref in (k_all, v_all, q_all, do_all):
        ref[:, :, LANES:] = jnp.zeros((ref.shape[0], rows, LANES), BF16)
    open_up(((k_in, k_all), (v_in, v_all)), PLACES, PLACES)
    dk_all[...] = jnp.zeros_like(dk_all)
    dv_all[...] = jnp.zeros_like(dv_all)

    mix_bias[...] = jnp.where((i >= j) & ((i - j).astype(F32) <= since), 0.0, NEG_FILL)
    pair_ref[...] = dot(c_part, b_part, 1, 1)
    for ref in (dpair_ref, zu_ref, db_ref, dc_ref, dpad_ref, red_out):
        ref[...] = jnp.zeros_like(ref)

    def within(n, carry):
        lanes = pl.ds(pl.multiple_of(n * LANES, LANES), LANES)
        cols = cols_ref[n]
        x_half = (act_all[:, lanes] * pair_columns(cols, 1, lower)).astype(BF16)
        dy_half = dy_all[:, lanes].astype(BF16)
        zero = jnp.zeros_like(dy_half)
        y_parts, dx_parts = [], []
        dpair = dpair_ref[...]
        rowc = rowc_ref[n]
        for k in range(2):
            weights = jnp.exp((cols[:, k : k + 1] - rowc[k : k + 1, :]) + mix_bias[...])
            mixing = (pair_ref[...] * weights).astype(BF16)
            y_parts.append(dot(mixing, x_half, 1, 0))
            dx_parts.append(dot(mixing, dy_half, 0, 0))
            dy_one = jnp.where(lower if k == 0 else ~lower, dy_half, zero)
            dpair = dpair + dot(dy_one, x_half, 1, 1) * weights
        dpair_ref[...] = dpair
        inner_all[:, lanes] = jnp.where(lower, y_parts[0], y_parts[1])
        dx_all[:, lanes] = jnp.where(lower, dx_parts[0], dx_parts[1])
        return carry

    lax.fori_loop(0, pairs // 3, within, 0)
    for copy in t_copies + a_copies:
        copy.wait()
    decays = dot(t_all[...].reshape(PLACES * PAD, LANES), spread_ref[...], 1, 0, EXACT)
    decay = [decays[PAD * n : PAD * n + 1] for n in range(PLACES)]
    end_of = lambda n: a_ref[n, 0].astype(F32)
    cot_of = lambda n: a_ref[n, 1].astype(F32)
    end, cot = end_of(0), cot_of(PLACES - 1)
    for n in range(1, PLACES):
        end = end_of(n) + decay[n] * end
        cot = cot_of(PLACES - 1 - n) + decay[PLACES - 1 - n] * cot
    end_out[...] = end.astype(BF16)
    cot_out[...] = cot.astype(BF16)
    g_out[...] = t_all[0] * t_all[1] * t_all[2] * t_all[3]
    b_copies = []
    for away in range(1, REACH + 1):
        later, earlier = shard(group + away, place, groups), shard(group - away, place, groups)
        b_copies.append(post.send(g_out, ge_in.at[away - 1], later))
        b_copies.append(post.send(g_out, gc_in.at[away - 1], earlier))
        b_copies.append(post.send(end_out, e_in.at[away - 1], later))
        b_copies.append(post.send(cot_out, c_in.at[away - 1], earlier))
    lax.fori_loop(pairs // 3, pairs, within, 0)
    dpair = dpair_ref[...]
    dc_ref[...] = dot(dpair, b_part.astype(F32), 1, 0, EXACT)
    db_ref[...] = dot(dpair, c_part.astype(F32), 0, 0, EXACT)
    for copy in near:
        copy.wait()
    open_up(((q_in, q_all), (do_in, do_all)), 0, PLACES)
    for copy in far:
        copy.wait()
    open_up(((k_in, k_all), (v_in, v_all)), 0, PLACES)

    def back_copy(source, target, b, n):
        return pltpu.make_async_remote_copy(
            src_ref=source.at[b], dst_ref=target.at[b], send_sem=back_sends.at[n],
            recv_sem=back_receives.at[n], device_id=behind, device_id_type=pl.DeviceIdType.MESH,
        )

    below = i.astype(F32)

    def block(b, carry):
        q = q_all[b]
        grad = do_all[b]
        low = low_ref[pl.ds(b, 1), :]
        at = [b + PLACES - gap for gap in range(PLACES + 1)]
        scores = []
        top = None
        for gap in range(PLACES + 1):
            allowed = below >= low - jnp.asarray(at[gap] * rows).astype(F32)
            if gap == 0:
                allowed = allowed & (j >= i)
            s = jnp.where(allowed, dot(k_all[at[gap]], q, 1, 1) * SCALE, NEG_FILL)
            scores.append(s)
            m = jnp.max(s, axis=0, keepdims=True)
            top = m if top is None else jnp.maximum(top, m)
        total = None
        expo = []
        for gap in range(PLACES + 1):
            e = jnp.exp(scores[gap] - top)
            expo.append(e)
            e_sum = jnp.sum(e, axis=0, keepdims=True)
            total = e_sum if total is None else total + e_sum
        inverse = 1.0 / jnp.maximum(total, 1.0)
        delta = None
        dprobs = []
        for gap in range(PLACES + 1):
            half = (expo[gap] * inverse).astype(BF16)
            dp = dot(v_all[at[gap]], grad, 1, 1)
            d = jnp.sum(half.astype(F32) * dp, axis=0, keepdims=True)
            delta = d if delta is None else delta + d
            dv_all[at[gap]] += dot(half, grad, 1, 0)
            dprobs.append(dp)
        dq = None
        for gap in range(PLACES + 1):
            ds = (expo[gap] * inverse * (dprobs[gap] - delta)).astype(BF16)
            dk_all[at[gap]] += dot(ds, q, 1, 0)
            part = dot(ds, k_all[at[gap]], 0, 0)
            dq = part if dq is None else dq + part
        fold((dq * SCALE).astype(BF16), dq_own, (b,))
        fold(dk_all[b].astype(BF16), dk_out, (b,))
        back_copy(dk_out, dk_back, b, b).start()
        fold(dv_all[b].astype(BF16), dv_out, (b,))
        return carry

    lax.fori_loop(0, 1, block, 0)
    for copy in b_copies:
        copy.wait()
    before = dot(ge_in[...].reshape(REACH * PAD, LANES), spread_ref[...], 1, 0, EXACT)
    after = dot(gc_in[...].reshape(REACH * PAD, LANES), spread_ref[...], 1, 0, EXACT)
    state = e_in[REACH - 1].astype(F32)
    cot = c_in[REACH - 1].astype(F32) * (group + REACH < groups).astype(F32)
    for away in range(REACH - 2, -1, -1):
        state = e_in[away].astype(F32) + before[PAD * away : PAD * away + 1] * state
        cot = (c_in[away].astype(F32) + after[PAD * away : PAD * away + 1] * cot) * (
            group + away + 1 < groups
        ).astype(F32)
    for n in range(PLACES):
        chain_out[n, 0] = state.astype(BF16)
        state = end_of(n) + decay[n] * state
        m = PLACES - 1 - n
        chain_out[m, 1] = cot.astype(BF16)
        cot = cot_of(m) + decay[m] * cot
    state_copies = [
        post.send(chain_out.at[peer], state_ref.at[place], shard(group, peer, groups)) for peer in peers
    ]
    state_ref[place] = chain_out[place]

    lax.fori_loop(1, PLACES, block, 0)
    for b in range(PLACES):
        back_copy(dv_out, dv_back, b, PLACES + b).start()
    kept = []

    def give_back(source, target):
        copies = spread(source, target, 0)
        copies.append(pltpu.make_async_copy(source.at[place], target.at[place], keeps.at[len(kept)]))
        copies[-1].start()
        kept.extend(copies)

    give_back(dq_own, dq_in)

    def across(n, carry):
        lanes = pl.ds(pl.multiple_of(n * LANES, LANES), LANES)
        cols = cols_ref[n]
        wt = wt_ref[:, lanes]
        size = pair_columns(cols, 1, lower)
        enter = pair_columns(cols, 2, lower)
        to_end = pair_columns(cols, 3, lower)
        act = act_all[:, lanes]
        dy = dy_all[:, lanes]
        x_wide = (act * size).astype(BF16).astype(F32)
        state = jnp.concatenate([state_ref[r, 0, :, lanes] for r in range(PLACES)], axis=0)
        end_cot = jnp.concatenate([state_ref[r, 1, :, lanes] for r in range(PLACES)], axis=0)
        inner = inner_all[:, lanes] + enter * dot(c_part, state, 1, 0)
        end_part = to_end * dot(b_part, end_cot, 1, 0)
        dx = dx_all[:, lanes] + end_part
        skip = wt[KERNEL : KERNEL + 1, :]
        ggate_ref[:, lanes] = (cg_all[:, lanes] * (inner + skip * act)).astype(BF16)
        zed = dy.astype(BF16).astype(F32) * inner - x_wide * dx
        you = dx * act
        zu = zu_ref[...]
        for k in range(2):
            side = lower if k == 0 else ~lower
            z_one = jnp.sum(jnp.where(side, zed, 0.0), axis=1, keepdims=True)
            u_one = jnp.sum(jnp.where(side, you, 0.0), axis=1, keepdims=True)
            zu = jnp.where(lane == 2 * n + k, z_one, jnp.where(lane == LANES // 2 + 2 * n + k, u_one, zu))
        zu_ref[...] = zu
        dc_ref[...] += dot((enter * dy).astype(BF16), state, 1, 1)
        db_ref[...] += dot((to_end * x_wide).astype(BF16), end_cot, 1, 1)
        dpre = (dx * size + skip * dy) * slope_all[:, lanes]
        red_out[pl.ds(KERNEL * n, 1), :] = jnp.sum(dpre * xp_ref[PAD:, lanes], axis=0, keepdims=True)
        dpad_ref[0, PAD : PAD + rows, :] = dpre
        grown = wt[0:1, :] * dpad_ref[0, 0 : rows + PAD, :]
        for lag in range(1, KERNEL):
            masked = dpre * mask_ref[lag - 1]
            red_out[pl.ds(KERNEL * n + lag, 1), :] = jnp.sum(
                masked * xp_ref[PAD - lag : PAD - lag + rows, lanes], axis=0, keepdims=True
            )
            dpad_ref[lag, PAD : PAD + rows, :] = masked
            grown = grown + wt[lag : lag + 1, :] * dpad_ref[lag, lag : lag + rows + PAD, :]
        gconv_ref[:, lanes] = grown[PAD:, :].astype(BF16)
        edge_ref[:, lanes] = grown[:PAD, :]
        end_ref[:, lanes] = grown[rows:, :]
        sums_ref[0:1, lanes] = jnp.sum(dy * act, axis=0, keepdims=True)
        sums_ref[1:2, lanes] = jnp.sum(state.astype(F32) * end_cot.astype(F32), axis=0, keepdims=True)
        sums_ref[2:3, lanes] = jnp.sum(x_wide * end_part, axis=0, keepdims=True)
        sums_ref[3:8, lanes] = jnp.zeros((5, LANES), F32)
        return carry

    def whole_sum(source, target, total, out, offset, factor):
        for b in range(PLACES):
            fold(total[PLACES + b], own_fold)
            back_copy(source, target, b, offset + b).wait()
            out[b] = ((own_fold[...] + target[b].astype(F32)) * factor).astype(BF16)

    lane = lax.broadcasted_iota(jnp.int32, (rows, LANES), 1)
    for copy in state_copies:
        copy.wait()
    def exchange(part):
        return [
            post.send(red_out.at[part], red_a.at[place, part], shard(group, peer, groups)) for peer in peers
        ]

    def widen(part, copies):
        red_a[place, part] = red_out[part]
        for copy in copies:
            copy.wait()
        red_mid[part] = red_a[0, part] + red_a[1, part] + red_a[2, part] + red_a[3, part]
        red_b[group, part] = red_mid[part]
        return [
            post.send(red_mid.at[part], red_b.at[group, part], shard(group + away, place, groups))
            for away in range(1, groups)
        ]

    upper, under = pl.ds(0, 4 * PAD), pl.ds(4 * PAD, 4 * PAD)
    lax.fori_loop(0, 4 * PAD // KERNEL, across, 0)
    early = exchange(upper)
    whole_sum(dk_out, dk_back, dk_all, dk_own, 0, SCALE)
    give_back(dk_own, dk_in)
    lax.fori_loop(4 * PAD // KERNEL, pairs, across, 0)
    wide = widen(upper, early)
    written = []

    def write(source, target):
        written.append(pltpu.make_async_copy(source, target, writes.at[len(written)]))
        written[-1].start()

    write(gconv_ref, gconv_hbm)
    write(ggate_ref, ggate_hbm)

    spill_copy = post.send(edge_ref, spill_ref, former)
    per_head = dot(sums_ref[...], spread_ref[...], 1, 1, EXACT)[:, 0:heads]
    last_row = per_head[2:3] + through * per_head[1:2]
    dcum = zu_ref[:, 0:heads] + jnp.where(t == rows - 1, last_row, 0.0)
    dlog = dot(tri, dcum, 0, 0, EXACT)
    grad_step = (zu_ref[:, LANES // 2 : LANES // 2 + heads] - dlog * rate) * jax.nn.sigmoid(raw)
    turn_back[...] = jnp.zeros_like(turn_back)
    turn_back[:, 0:heads] = grad_step
    gstep_ref[...] = turn_back[...].T[0:heads, :]
    write(gstep_ref, gstep_hbm)
    small = KERNEL * pairs
    red_out[small : small + 1, 0:heads] = jnp.sum(grad_step, axis=0, keepdims=True)
    red_out[small + 1 : small + 2, 0:heads] = jnp.sum(dlog * log_decay, axis=0, keepdims=True)
    red_out[small + 2 : small + 3, 0:heads] = per_head[0:1]
    reds = exchange(under)
    coef_out[...] = jnp.concatenate([db_ref[...], dc_ref[...]], axis=1).astype(BF16)
    coefs = [post.send(coef_out, coef_all.at[head], peer) for peer in head_peers]
    coef_all[head] = coef_out[...]
    wide += widen(under, reds)
    whole_sum(dv_out, dv_back, dv_all, dv_own, PLACES, 1.0)
    give_back(dv_own, dv_in)
    spill_copy.wait()
    gfix_ref[...] = end_ref[...] + spill_ref[...]
    write(gfix_ref, gfix_hbm)
    for copy in coefs:
        copy.wait()
    halves = [coef_all[2 * n].astype(F32) + coef_all[2 * n + 1].astype(F32) for n in range(2)]
    half = coef_out.shape[1] // 2
    gin_ref[...] = jnp.concatenate([halves[0][:, :half], halves[1][:, :half]], axis=1)
    gout_ref[...] = jnp.concatenate([halves[0][:, half:], halves[1][:, half:]], axis=1)
    write(gin_ref, gin_hbm)
    write(gout_ref, gout_hbm)
    for copy in wide:
        copy.wait()
    total = red_b[0]
    for n in range(1, groups):
        total = total + red_b[n]
    total_ref[...] = total
    for copy in kept + written:
        copy.wait()


def finish_kernel(ins, outs, in_bufs, out_bufs, load_sems, store_sems):
    loads = [pltpu.make_async_copy(a, b, load_sems.at[n]) for n, (a, b) in enumerate(zip(ins, in_bufs))]
    for load in loads:
        load.start()
    stores = []

    def store(source, target):
        stores.append(pltpu.make_async_copy(source, target, store_sems.at[len(stores)]))
        stores[-1].start()

    total, fix, gconv = in_bufs[0], in_bufs[1], in_bufs[2]
    for load in loads[:3]:
        load.wait()
    gconv[gconv.shape[0] - PAD :, :] = fix[...].astype(BF16)
    store(gconv, outs[3])
    conv, *small = out_bufs[3:]
    pairs, heads = conv.shape[1] // LANES, small[0].shape[1]
    for lag in range(KERNEL):
        for n in range(pairs):
            row = KERNEL * n + lag
            conv[lag : lag + 1, n * LANES : (n + 1) * LANES] = total[row : row + 1, :]
    for n, ref in enumerate(small):
        row = KERNEL * pairs + n
        ref[...] = total[row : row + 1, 0:heads]
    for n, ref in enumerate((conv, *small)):
        store(ref, outs[8 + n])
    for n in range(3, 7):
        loads[n].wait()
        store(in_bufs[n], outs[n + 1])
    for n in range(3):
        loads[7 + n].wait()
        for r in range(PLACES):
            unfold(in_bufs[7 + n], (r,), out_bufs[n], (), r * HEAD_DIM)
        store(out_bufs[n], outs[n])
    for copy in stores:
        copy.wait()


def local(
    queries, keys, values, attn_grad, doc_ids, conv_input, conv_weight, step_raw, step_bias,
    rate_log, skip_gain, input_coeff, output_coeff, gate_input, mix_grad,
):
    rows, width = queries.shape
    heads, channels = step_raw.shape[1], conv_input.shape[1]
    pairs = channels // LANES
    groups = lax.axis_size("seq") // PLACES
    struct = jax.ShapeDtypeStruct
    vmem = pl.BlockSpec(memory_space=pltpu.VMEM)
    loose = pl.BlockSpec(memory_space=pl.ANY)
    dma = lambda n: pltpu.SemaphoreType.DMA((n,))
    head_cols = 2 * LANES
    quarter = (2, 2 * PAD, channels)
    part = quarter[1:]
    half = lambda *shape: pltpu.VMEM(shape, BF16)
    full = lambda *shape: pltpu.VMEM(shape, F32)
    flat = full(PAD, channels)
    piece = lambda n: half(n, rows, head_cols)
    slim_rows = rows * HEAD_DIM // LANES
    slim = lambda n: half(n, slim_rows, LANES)
    red_rows = 64
    wide_shape = (rows, channels)
    small = [
        doc_ids.reshape(-1, LANES), step_raw.T, step_bias[None], rate_log[None], skip_gain[None],
        input_coeff, output_coeff, conv_weight,
    ]
    mid = pl.pallas_call(
        whole_kernel,
        in_specs=[[loose] * 8] + [loose] * 7,
        out_specs=[loose] * 9 + [vmem],
        out_shape=[struct((PLACES, slim_rows, LANES), BF16)] * 3
        + [
            struct(wide_shape, BF16), struct(wide_shape, BF16), struct((PAD, channels), F32),
            struct((heads, rows), F32), struct((rows, LANES), F32), struct((rows, LANES), F32),
            struct((red_rows, LANES), F32),
        ],
        scratch_shapes=[
            [pltpu.VMEM(a.shape, a.dtype) for a in small],
            flat, full(heads, rows), full(rows, LANES), full(rows, LANES), half(*wide_shape), half(*wide_shape),
            full(PAD, rows), full(PLACES * rows // LANES, LANES), full(LANES, rows), full(rows, LANES),
            half(rows, width), half(rows, width), half(rows, width), half(rows, width),
            half(*wide_shape), half(*wide_shape), half(*wide_shape),
            slim(PLACES), slim(PLACES), slim(PLACES), slim(PLACES),
            slim(PLACES), slim(PLACES), slim(2 * PLACES), slim(2 * PLACES), full(slim_rows, LANES),
            piece(PLACES), piece(PLACES), piece(2 * PLACES), piece(2 * PLACES),
            full(2 * PLACES, rows, head_cols), full(2 * PLACES, rows, head_cols),
            slim(PLACES), slim(PLACES), slim(PLACES), slim(PLACES),
            slim(PLACES), slim(PLACES), slim(PLACES),
            half(2 * PAD, channels), flat, full(pairs, rows, 8), full(pairs, 2, rows), full(LANES, channels),
            full(KERNEL - 1, rows, LANES), full(rows + PAD, channels),
            full(*wide_shape), full(*wide_shape), full(*wide_shape), full(*wide_shape), full(*wide_shape),
            full(*wide_shape),
            half(PLACES, *quarter), half(PLACES, *quarter), half(*part), half(*part), full(PAD, LANES),
            half(REACH, *part), half(REACH, *part), full(REACH, PAD, LANES), full(REACH, PAD, LANES),
            half(PLACES, *quarter), half(PLACES, *quarter), full(PAD, LANES), full(PLACES, PAD, LANES),
            full(rows, rows), full(rows, rows), full(rows, rows), full(KERNEL, rows + 2 * PAD, LANES),
            full(rows, LANES), full(rows, LANES // 2), full(rows, LANES // 2),
            flat, flat, flat, flat, half(rows, LANES), half(4, rows, LANES),
            full(red_rows, LANES), full(PLACES, red_rows, LANES), full(red_rows, LANES),
            full(groups, red_rows, LANES),
            dma(SENDS), dma(SENDS), dma(2 * PLACES), dma(2 * PLACES), dma(7), dma(3 * PLACES), dma(6), dma(8),
        ],
        name="whole",
        compiler_params=pltpu.CompilerParams(
            collective_id=0, has_side_effects=True, vmem_limit_bytes=58 * 1024 * 1024
        ),
    )(
        small, keys, values, queries, attn_grad, conv_input, gate_input, mix_grad,
    )
    dq, dk, dv, gconv, ggate, gfix, gstep, gin, gout, total = mid
    ins = [total, gfix, gconv, ggate, gstep, gin, gout, dq, dk, dv]
    shapes = [struct((rows, width), BF16)] * 3 + [
        struct(wide_shape, BF16), struct(wide_shape, BF16), struct((heads, rows), F32),
        struct((rows, LANES), F32), struct((rows, LANES), F32), struct((KERNEL, channels), F32),
    ] + [struct((1, heads), F32)] * 3
    *outs, conv, bias, rate, skip = pl.pallas_call(
        finish_kernel,
        in_specs=[[loose] * len(ins)],
        out_specs=[[loose] * len(shapes)],
        out_shape=[shapes],
        scratch_shapes=[
            [pltpu.VMEM(a.shape, a.dtype) for a in ins],
            [pltpu.VMEM(shapes[n].shape, shapes[n].dtype) for n in (0, 1, 2, 8, 9, 10, 11)],
            dma(len(ins)), dma(len(shapes)),
        ],
        name="finish",
    )(ins)[0]
    outs[5] = outs[5].T
    return (*outs, conv, bias[0], rate[0], skip[0])


def solution(mesh):
    sharded = P("seq", "head")
    return jax.shard_map(
        local,
        mesh=mesh,
        in_specs=(
            sharded, sharded, sharded, sharded, P(), sharded, P(None, "head"), sharded,
            P("head"), P("head"), P("head"), P("seq", None), P("seq", None), sharded, sharded,
        ),
        out_specs=(
            sharded, sharded, sharded, sharded, sharded, sharded,
            P("seq", None), P("seq", None), P(None, "head"), P("head"), P("head"), P("head"),
        ),
        check_vma=False,
    )
```

```python
import jax
import jax.numpy as jnp
from jax import lax
from jax.experimental import pallas as pl
from jax.experimental.pallas import tpu as pltpu
from jax.sharding import PartitionSpec as P

HEAD_DIM = 224
WINDOW = 1024
KERNEL = 4
PAD = 8
LANES = 128
PLACES = 4
DOCS = 8
REACH = 4

EXACT = lax.Precision.HIGHEST
F32 = jnp.float32
BF16 = jnp.bfloat16
NEG_FILL = -1e30
SENDS = 79
SCALE = HEAD_DIM ** (-0.5)


def dot(a, b, ca, cb, precision=None):
    return lax.dot_general(
        a, b, (((ca,), (cb,)), ((), ())), preferred_element_type=F32, precision=precision
    )


def where_am_i():
    index = lax.axis_index("seq")
    groups = lax.axis_size("seq") // PLACES
    return lax.div(index, PLACES), lax.rem(index, PLACES), groups


def shard(group, place, groups):
    return {"seq": lax.rem(group + 2 * groups, groups) * PLACES + place}


def greet(partners):
    barrier = pltpu.get_barrier_semaphore()
    for partner in partners:
        pl.semaphore_signal(barrier, inc=1, device_id=partner, device_id_type=pl.DeviceIdType.MESH)
    return lambda: pl.semaphore_wait(barrier, len(partners))


class Post:
    def __init__(self, sends, receives):
        self.sends, self.receives, self.used = sends, receives, 0

    def send(self, source, target, device):
        copy = pltpu.make_async_remote_copy(
            src_ref=source, dst_ref=target, send_sem=self.sends.at[self.used],
            recv_sem=self.receives.at[self.used], device_id=device,
            device_id_type=pl.DeviceIdType.MESH,
        )
        self.used += 1
        copy.start()
        return copy


def spreader(heads, channels):
    width = channels // heads
    row = lax.broadcasted_iota(jnp.int32, (LANES, channels), 0)
    col = lax.broadcasted_iota(jnp.int32, (LANES, channels), 1)
    return ((col >= row * width) & (col < row * width + width)).astype(F32)


def causal(rows):
    i = lax.broadcasted_iota(jnp.int32, (rows, rows), 0)
    j = lax.broadcasted_iota(jnp.int32, (rows, rows), 1)
    return i, j


def pair_columns(cols, index, lower):
    return jnp.where(lower, cols[:, 2 * index : 2 * index + 1], cols[:, 2 * index + 1 : 2 * index + 2])


def fill_masks(since, mask_ref):
    for lag in range(1, KERNEL):
        mask_ref[lag - 1] = jnp.broadcast_to((since >= lag).astype(F32), mask_ref.shape[1:])


def conv_pre(conv, tail, wt, mask_ref, xp_ref, lanes):
    rows = conv.shape[0]
    xp_ref[:PAD, lanes] = tail.astype(F32)[PAD:]
    xp_ref[PAD:, lanes] = conv.astype(F32)
    pre = wt[0:1, :] * conv.astype(F32)
    for lag in range(1, KERNEL):
        pre = pre + wt[lag : lag + 1, :] * (xp_ref[PAD - lag : PAD - lag + rows, lanes] * mask_ref[lag - 1])
    return pre


def group_part(ref):
    half = ref.shape[1] // 2
    whole = ref[...].astype(F32)
    first = lax.axis_index("head") < lax.axis_size("head") // 2
    return jnp.where(first, whole[:, :half], whole[:, half:]).astype(BF16)


def fold(value, target, at=()):
    rows, (keep, quarter) = value.shape[0], (3 * value.shape[0] // 4, value.shape[0] // 4)
    target[(*at, slice(0, rows), slice(None))] = value[:, 0:LANES]
    rest, width = HEAD_DIM - LANES, LANES // 4
    target[(*at, slice(rows, rows + keep), slice(0, rest))] = value[0:keep, LANES:HEAD_DIM]
    for n in range(3):
        target[(*at, slice(rows + n * quarter, rows + (n + 1) * quarter), slice(rest, LANES))] = value[
            keep:, LANES + n * width : LANES + (n + 1) * width
        ]


def unfold(source, source_at, target, target_at, offset=0):
    rows = 4 * source.shape[-2] // 7
    keep, quarter, rest, width = 3 * rows // 4, rows // 4, HEAD_DIM - LANES, LANES // 4
    put = lambda a, b, c, d, value: target.__setitem__((*target_at, slice(a, b), slice(offset + c, offset + d)), value)
    get = lambda a, b, c, d: source[(*source_at, slice(a, b), slice(c, d))]
    put(0, rows, 0, LANES, get(0, rows, 0, LANES))
    put(0, keep, LANES, HEAD_DIM, get(rows, rows + keep, 0, rest))
    for n in range(3):
        put(
            keep, rows, LANES + n * width, LANES + (n + 1) * width,
            get(rows + n * quarter, rows + (n + 1) * quarter, rest, LANES),
        )


def whole_kernel(
    small_hbm,
    k_hbm, v_hbm, q_hbm, do_hbm, conv_hbm, gate_hbm, mix_hbm,
    dq_in, dk_in, dv_in, gconv_hbm, ggate_hbm, gfix_hbm, gstep_hbm, gin_hbm, gout_hbm, total_ref,
    small_refs, gfix_ref, gstep_ref, gin_ref, gout_ref, gconv_ref, ggate_ref, low_ref, since_ref, turn_ref, turn_back, k_ref, v_ref, q_ref, do_ref, conv_ref, gate_ref, mix_ref,
    k_pack, v_pack, q_pack, do_pack, q_in, do_in, k_in, v_in, own_fold, q_all, do_all, k_all, v_all, dk_all, dv_all,
    dk_out, dv_out, dk_back, dv_back, dq_own, dk_own, dv_own,
    tail_buf, wt_ref, cols_ref, rowc_ref, spread_ref, mask_ref, xp_ref,
    act_all, slope_all, dy_all, cg_all, inner_all, dx_all,
    ends_ref, a_ref, end_out, cot_out, g_out, e_in, c_in, ge_in, gc_in, chain_out, state_ref, t_out, t_all,
    mix_bias, pair_ref, dpair_ref, dpad_ref, zu_ref, db_ref, dc_ref,
    sums_ref, edge_ref, end_ref, spill_ref, coef_out, coef_all, red_out, red_a, red_mid, red_b,
    sends, receives, back_sends, back_receives, loads, keeps, writes, small_loads,
):
    group, place, groups = where_am_i()
    head, head_count = lax.axis_index("head"), lax.axis_size("head")
    doc_ref, step_ref, bias_ref, rate_ref, skip_ref, b_ref, c_ref, weight_ref = small_refs
    heads, rows = step_ref.shape
    channels = conv_ref.shape[1]
    pairs = channels // LANES
    peers = [lax.rem(place + d, PLACES) for d in range(1, PLACES)]
    post = Post(sends, receives)
    fetches = []
    for n, (source, target) in enumerate((
        (k_hbm, k_ref), (v_hbm, v_ref), (conv_hbm, conv_ref), (q_hbm, q_ref), (do_hbm, do_ref),
        (gate_hbm, gate_ref), (mix_hbm, mix_ref),
    )):
        fetches.append(pltpu.make_async_copy(source, target, loads.at[n]))
        fetches[-1].start()
    small_fetches = [
        pltpu.make_async_copy(source, target, small_loads.at[n])
        for n, (source, target) in enumerate(zip(small_hbm, small_refs))
    ]
    for fetch in small_fetches:
        fetch.start()
    partners = [shard(group + far, place, groups) for far in range(1, groups)]
    partners += [shard(group, peer, groups) for peer in peers]
    last, first = place == PLACES - 1, place == 0
    follower = shard(jnp.where(last, group + 1, group), lax.rem(place + 1, PLACES), groups)
    former = shard(jnp.where(first, group - 1, group), lax.rem(place + PLACES - 1, PLACES), groups)
    head_peers = [{"head": lax.rem(head + d, head_count)} for d in range(1, head_count)]
    wait_partners = greet(partners + [follower, former] + head_peers)
    ahead = shard(group + 1, place, groups)
    behind = shard(group - 1, place, groups)

    def pack(source, target):
        for r in range(PLACES):
            fold(source[:, r * HEAD_DIM : (r + 1) * HEAD_DIM], target, (r,))

    def spread(source, target, offset):
        return [
            post.send(source.at[peer], target.at[offset + place], shard(group, peer, groups)) for peer in peers
        ]

    fetches[0].wait()
    pack(k_ref, k_pack)
    fetches[2].wait()
    wait_partners()
    tail_copy = post.send(conv_ref.at[rows - 2 * PAD :, :], tail_buf, follower)
    far = [post.send(k_pack.at[place], k_in.at[place], ahead)]
    near_k = spread(k_pack, k_in, PLACES)
    fetches[1].wait()
    pack(v_ref, v_pack)
    far.append(post.send(v_pack.at[place], v_in.at[place], ahead))
    near_v = spread(v_pack, v_in, PLACES)
    fetches[3].wait()
    pack(q_ref, q_pack)
    fetches[4].wait()
    pack(do_ref, do_pack)

    for fetch in small_fetches:
        fetch.wait()
    per_row = rows // LANES
    docs = doc_ref[pl.ds(pl.multiple_of(group * PLACES * per_row, PLACES * per_row), PLACES * per_row), :]
    everyone_doc = doc_ref[...]
    begin = jnp.zeros(docs.shape, F32)
    for doc in range(1, DOCS):
        count = jnp.sum((everyone_doc < doc).astype(F32), axis=0, keepdims=True)
        count = jnp.sum(count, axis=1, keepdims=True)
        begin = jnp.where(docs == doc, count, begin)
    where = (
        lax.broadcasted_iota(jnp.int32, docs.shape, 0) * LANES
        + lax.broadcasted_iota(jnp.int32, docs.shape, 1)
        + group * (PLACES * rows)
    ).astype(F32)
    low = jnp.maximum(begin, where - (WINDOW - 1)) - (group * (PLACES * rows) - WINDOW).astype(F32)
    since_ref[...] = where - begin
    for n in range(PLACES * per_row):
        b, side = n // per_row, n % per_row
        low_ref[b : b + 1, side * LANES : (side + 1) * LANES] = low[n : n + 1]
    row = jnp.concatenate([since_ref[pl.ds(place * per_row + n, 1), :] for n in range(per_row)], axis=1)
    since = jnp.broadcast_to(row, (PAD, rows)).T[:, 0:1]

    turn_ref[...] = jnp.zeros_like(turn_ref)
    turn_ref[0:heads, :] = step_ref[...]
    raw = turn_ref[...].T[:, 0:heads] + bias_ref[...]
    step = jnp.maximum(raw, 0.0) + jnp.log1p(jnp.exp(-jnp.abs(raw)))
    rate = jnp.exp(rate_ref[...])
    log_decay = -step * rate
    i, j = causal(rows)
    tri = (i >= j).astype(F32)
    cum = dot(tri, log_decay, 1, 0, EXACT)
    row_cum = dot(log_decay, tri, 0, 1, EXACT)
    t = lax.broadcasted_iota(jnp.int32, (rows, 1), 0)
    enter = jnp.where(since > t.astype(F32), jnp.exp(cum), 0.0)
    final = cum[rows - 1 : rows]
    to_end = jnp.where((rows - 1 - t).astype(F32) <= since[rows - 1 : rows], jnp.exp(final - cum), 0.0)
    through = enter[rows - 1 : rows]
    t_out[...] = jnp.zeros_like(t_out)
    t_out[0:1, 0:heads] = through
    t_all[place] = t_out[...]
    t_copies = [post.send(t_out, t_all.at[place], shard(group, peer, groups)) for peer in peers]
    for n in range(pairs):
        two = slice(2 * n, 2 * n + 2)
        cols_ref[n] = jnp.concatenate([cum[:, two], step[:, two], enter[:, two], to_end[:, two]], axis=1)
        rowc_ref[n] = row_cum[two]
    spread_ref[...] = spreader(heads, channels)
    wt_ref[0:KERNEL, :] = weight_ref[...]
    wt_ref[KERNEL : KERNEL + 1, :] = dot(skip_ref[...], spread_ref[0:heads, :], 1, 0, EXACT)
    fill_masks(since, mask_ref)
    lower = lax.broadcasted_iota(jnp.int32, (rows, LANES), 1) < LANES // 2
    b_part, c_part = group_part(b_ref), group_part(c_ref)
    fetches[5].wait()
    fetches[6].wait()
    tail_copy.wait()

    def ends(n, carry):
        lanes = pl.ds(pl.multiple_of(n * LANES, LANES), LANES)
        cols = cols_ref[n]
        pre = conv_pre(conv_ref[:, lanes], tail_buf[:, lanes], wt_ref[:, lanes], mask_ref, xp_ref, lanes)
        sig_pre = jax.nn.sigmoid(pre)
        act = pre * sig_pre
        act_all[:, lanes] = act
        slope_all[:, lanes] = sig_pre + act * (1.0 - sig_pre)
        weighted = act * pair_columns(cols, 1, lower) * pair_columns(cols, 3, lower)
        end = dot(b_part, weighted.astype(BF16), 0, 0).astype(BF16)
        gate = gate_ref[:, lanes].astype(F32)
        sig_gate = jax.nn.sigmoid(gate)
        silu_gate = gate * sig_gate
        cot = mix_ref[:, lanes].astype(F32)
        dy = cot * silu_gate
        dy_all[:, lanes] = dy
        cg_all[:, lanes] = cot * (sig_gate + silu_gate * (1.0 - sig_gate))
        start = dot(c_part, (dy * pair_columns(cols, 2, lower)).astype(BF16), 0, 0).astype(BF16)
        for r in range(PLACES):
            part = slice(2 * PAD * r, 2 * PAD * (r + 1))
            ends_ref[r, 0, :, lanes] = end[part]
            ends_ref[r, 1, :, lanes] = start[part]
        return carry

    def pass_on(copies, target):
        for d in range(1, PLACES):
            copies[d - 1].wait()
            source = lax.rem(place + PLACES - d, PLACES)
            far.append(post.send(target.at[PLACES + source], target.at[source], ahead))

    lax.fori_loop(0, 2 * pairs // 3, ends, 0)
    pass_on(near_k, k_in)
    lax.fori_loop(2 * pairs // 3, pairs, ends, 0)

    a_copies = [post.send(ends_ref.at[peer], a_ref.at[place], shard(group, peer, groups)) for peer in peers]
    near = spread(q_pack, q_in, 0) + spread(do_pack, do_in, 0)
    a_ref[place] = ends_ref[place]
    pass_on(near_v, v_in)
    for mine, everyone, offset in (
        (k_pack, k_in, PLACES), (v_pack, v_in, PLACES), (q_pack, q_in, 0), (do_pack, do_in, 0)
    ):
        everyone[offset + place] = mine[place]

    def open_up(pairs_of, first, count):
        def one(n, carry):
            for source, target in pairs_of:
                unfold(source, (n,), target, (n,))
            return carry

        lax.fori_loop(first, first + count, one, 0)

    for ref in (k_all, v_all, q_all, do_all):
        ref[:, :, LANES:] = jnp.zeros((ref.shape[0], rows, LANES), BF16)
    open_up(((k_in, k_all), (v_in, v_all)), PLACES, PLACES)
    dk_all[...] = jnp.zeros_like(dk_all)
    dv_all[...] = jnp.zeros_like(dv_all)

    mix_bias[...] = jnp.where((i >= j) & ((i - j).astype(F32) <= since), 0.0, NEG_FILL)
    pair_ref[...] = dot(c_part, b_part, 1, 1)
    for ref in (dpair_ref, zu_ref, db_ref, dc_ref, dpad_ref, red_out):
        ref[...] = jnp.zeros_like(ref)

    def within(n, carry):
        lanes = pl.ds(pl.multiple_of(n * LANES, LANES), LANES)
        cols = cols_ref[n]
        x_half = (act_all[:, lanes] * pair_columns(cols, 1, lower)).astype(BF16)
        dy_half = dy_all[:, lanes].astype(BF16)
        zero = jnp.zeros_like(dy_half)
        y_parts, dx_parts = [], []
        dpair = dpair_ref[...]
        rowc = rowc_ref[n]
        for k in range(2):
            weights = jnp.exp((cols[:, k : k + 1] - rowc[k : k + 1, :]) + mix_bias[...])
            mixing = (pair_ref[...] * weights).astype(BF16)
            y_parts.append(dot(mixing, x_half, 1, 0))
            dx_parts.append(dot(mixing, dy_half, 0, 0))
            dy_one = jnp.where(lower if k == 0 else ~lower, dy_half, zero)
            dpair = dpair + dot(dy_one, x_half, 1, 1) * weights
        dpair_ref[...] = dpair
        inner_all[:, lanes] = jnp.where(lower, y_parts[0], y_parts[1])
        dx_all[:, lanes] = jnp.where(lower, dx_parts[0], dx_parts[1])
        return carry

    lax.fori_loop(0, pairs // 3, within, 0)
    for copy in t_copies + a_copies:
        copy.wait()
    decays = dot(t_all[...].reshape(PLACES * PAD, LANES), spread_ref[...], 1, 0, EXACT)
    decay = [decays[PAD * n : PAD * n + 1] for n in range(PLACES)]
    end_of = lambda n: a_ref[n, 0].astype(F32)
    cot_of = lambda n: a_ref[n, 1].astype(F32)
    end, cot = end_of(0), cot_of(PLACES - 1)
    for n in range(1, PLACES):
        end = end_of(n) + decay[n] * end
        cot = cot_of(PLACES - 1 - n) + decay[PLACES - 1 - n] * cot
    end_out[...] = end.astype(BF16)
    cot_out[...] = cot.astype(BF16)
    g_out[...] = t_all[0] * t_all[1] * t_all[2] * t_all[3]
    b_copies = []
    for away in range(1, REACH + 1):
        later, earlier = shard(group + away, place, groups), shard(group - away, place, groups)
        b_copies.append(post.send(g_out, ge_in.at[away - 1], later))
        b_copies.append(post.send(g_out, gc_in.at[away - 1], earlier))
        b_copies.append(post.send(end_out, e_in.at[away - 1], later))
        b_copies.append(post.send(cot_out, c_in.at[away - 1], earlier))
    lax.fori_loop(pairs // 3, pairs, within, 0)
    dpair = dpair_ref[...]
    dc_ref[...] = dot(dpair, b_part.astype(F32), 1, 0, EXACT)
    db_ref[...] = dot(dpair, c_part.astype(F32), 0, 0, EXACT)
    for copy in near:
        copy.wait()
    open_up(((q_in, q_all), (do_in, do_all)), 0, PLACES)
    for copy in far:
        copy.wait()
    open_up(((k_in, k_all), (v_in, v_all)), 0, PLACES)

    def back_copy(source, target, b, n):
        return pltpu.make_async_remote_copy(
            src_ref=source.at[b], dst_ref=target.at[b], send_sem=back_sends.at[n],
            recv_sem=back_receives.at[n], device_id=behind, device_id_type=pl.DeviceIdType.MESH,
        )

    below = i.astype(F32)

    def block(b, carry):
        q = q_all[b]
        grad = do_all[b]
        low = low_ref[pl.ds(b, 1), :]
        at = [b + PLACES - gap for gap in range(PLACES + 1)]
        scores = []
        top = None
        for gap in range(PLACES + 1):
            allowed = below >= low - jnp.asarray(at[gap] * rows).astype(F32)
            if gap == 0:
                allowed = allowed & (j >= i)
            s = jnp.where(allowed, dot(k_all[at[gap]], q, 1, 1) * SCALE, NEG_FILL)
            scores.append(s)
            m = jnp.max(s, axis=0, keepdims=True)
            top = m if top is None else jnp.maximum(top, m)
        total = None
        expo = []
        for gap in range(PLACES + 1):
            e = jnp.exp(scores[gap] - top)
            expo.append(e)
            e_sum = jnp.sum(e, axis=0, keepdims=True)
            total = e_sum if total is None else total + e_sum
        inverse = 1.0 / jnp.maximum(total, 1.0)
        delta = None
        dprobs = []
        for gap in range(PLACES + 1):
            half = (expo[gap] * inverse).astype(BF16)
            dp = dot(v_all[at[gap]], grad, 1, 1)
            d = jnp.sum(half.astype(F32) * dp, axis=0, keepdims=True)
            delta = d if delta is None else delta + d
            dv_all[at[gap]] += dot(half, grad, 1, 0)
            dprobs.append(dp)
        dq = None
        for gap in range(PLACES + 1):
            ds = (expo[gap] * inverse * (dprobs[gap] - delta)).astype(BF16)
            dk_all[at[gap]] += dot(ds, q, 1, 0)
            part = dot(ds, k_all[at[gap]], 0, 0)
            dq = part if dq is None else dq + part
        fold((dq * SCALE).astype(BF16), dq_own, (b,))
        fold(dk_all[b].astype(BF16), dk_out, (b,))
        back_copy(dk_out, dk_back, b, b).start()
        fold(dv_all[b].astype(BF16), dv_out, (b,))
        return carry

    lax.fori_loop(0, 1, block, 0)
    for copy in b_copies:
        copy.wait()
    before = dot(ge_in[...].reshape(REACH * PAD, LANES), spread_ref[...], 1, 0, EXACT)
    after = dot(gc_in[...].reshape(REACH * PAD, LANES), spread_ref[...], 1, 0, EXACT)
    state = e_in[REACH - 1].astype(F32)
    cot = c_in[REACH - 1].astype(F32) * (group + REACH < groups).astype(F32)
    for away in range(REACH - 2, -1, -1):
        state = e_in[away].astype(F32) + before[PAD * away : PAD * away + 1] * state
        cot = (c_in[away].astype(F32) + after[PAD * away : PAD * away + 1] * cot) * (
            group + away + 1 < groups
        ).astype(F32)
    for n in range(PLACES):
        chain_out[n, 0] = state.astype(BF16)
        state = end_of(n) + decay[n] * state
        m = PLACES - 1 - n
        chain_out[m, 1] = cot.astype(BF16)
        cot = cot_of(m) + decay[m] * cot
    state_copies = [
        post.send(chain_out.at[peer], state_ref.at[place], shard(group, peer, groups)) for peer in peers
    ]
    state_ref[place] = chain_out[place]

    lax.fori_loop(1, PLACES, block, 0)
    for b in range(PLACES):
        back_copy(dv_out, dv_back, b, PLACES + b).start()
    kept = []

    def give_back(source, target):
        copies = spread(source, target, 0)
        copies.append(pltpu.make_async_copy(source.at[place], target.at[place], keeps.at[len(kept)]))
        copies[-1].start()
        kept.extend(copies)

    give_back(dq_own, dq_in)

    def across(n, carry):
        lanes = pl.ds(pl.multiple_of(n * LANES, LANES), LANES)
        cols = cols_ref[n]
        wt = wt_ref[:, lanes]
        size = pair_columns(cols, 1, lower)
        enter = pair_columns(cols, 2, lower)
        to_end = pair_columns(cols, 3, lower)
        act = act_all[:, lanes]
        dy = dy_all[:, lanes]
        x_wide = (act * size).astype(BF16).astype(F32)
        state = jnp.concatenate([state_ref[r, 0, :, lanes] for r in range(PLACES)], axis=0)
        end_cot = jnp.concatenate([state_ref[r, 1, :, lanes] for r in range(PLACES)], axis=0)
        inner = inner_all[:, lanes] + enter * dot(c_part, state, 1, 0)
        end_part = to_end * dot(b_part, end_cot, 1, 0)
        dx = dx_all[:, lanes] + end_part
        skip = wt[KERNEL : KERNEL + 1, :]
        ggate_ref[:, lanes] = (cg_all[:, lanes] * (inner + skip * act)).astype(BF16)
        zed = dy.astype(BF16).astype(F32) * inner - x_wide * dx
        you = dx * act
        zu = zu_ref[...]
        for k in range(2):
            side = lower if k == 0 else ~lower
            z_one = jnp.sum(jnp.where(side, zed, 0.0), axis=1, keepdims=True)
            u_one = jnp.sum(jnp.where(side, you, 0.0), axis=1, keepdims=True)
            zu = jnp.where(lane == 2 * n + k, z_one, jnp.where(lane == LANES // 2 + 2 * n + k, u_one, zu))
        zu_ref[...] = zu
        dc_ref[...] += dot((enter * dy).astype(BF16), state, 1, 1)
        db_ref[...] += dot((to_end * x_wide).astype(BF16), end_cot, 1, 1)
        dpre = (dx * size + skip * dy) * slope_all[:, lanes]
        red_out[pl.ds(KERNEL * n, 1), :] = jnp.sum(dpre * xp_ref[PAD:, lanes], axis=0, keepdims=True)
        dpad_ref[0, PAD : PAD + rows, :] = dpre
        grown = wt[0:1, :] * dpad_ref[0, 0 : rows + PAD, :]
        for lag in range(1, KERNEL):
            masked = dpre * mask_ref[lag - 1]
            red_out[pl.ds(KERNEL * n + lag, 1), :] = jnp.sum(
                masked * xp_ref[PAD - lag : PAD - lag + rows, lanes], axis=0, keepdims=True
            )
            dpad_ref[lag, PAD : PAD + rows, :] = masked
            grown = grown + wt[lag : lag + 1, :] * dpad_ref[lag, lag : lag + rows + PAD, :]
        gconv_ref[:, lanes] = grown[PAD:, :].astype(BF16)
        edge_ref[:, lanes] = grown[:PAD, :]
        end_ref[:, lanes] = grown[rows:, :]
        sums_ref[0:1, lanes] = jnp.sum(dy * act, axis=0, keepdims=True)
        sums_ref[1:2, lanes] = jnp.sum(state.astype(F32) * end_cot.astype(F32), axis=0, keepdims=True)
        sums_ref[2:3, lanes] = jnp.sum(x_wide * end_part, axis=0, keepdims=True)
        sums_ref[3:8, lanes] = jnp.zeros((5, LANES), F32)
        return carry

    def whole_sum(source, target, total, out, offset, factor):
        for b in range(PLACES):
            fold(total[PLACES + b], own_fold)
            back_copy(source, target, b, offset + b).wait()
            out[b] = ((own_fold[...] + target[b].astype(F32)) * factor).astype(BF16)

    lane = lax.broadcasted_iota(jnp.int32, (rows, LANES), 1)
    for copy in state_copies:
        copy.wait()
    def exchange(part):
        return [
            post.send(red_out.at[part], red_a.at[place, part], shard(group, peer, groups)) for peer in peers
        ]

    def widen(part, copies):
        red_a[place, part] = red_out[part]
        for copy in copies:
            copy.wait()
        red_mid[part] = red_a[0, part] + red_a[1, part] + red_a[2, part] + red_a[3, part]
        red_b[group, part] = red_mid[part]
        return [
            post.send(red_mid.at[part], red_b.at[group, part], shard(group + away, place, groups))
            for away in range(1, groups)
        ]

    upper, under = pl.ds(0, 4 * PAD), pl.ds(4 * PAD, 4 * PAD)
    lax.fori_loop(0, 4 * PAD // KERNEL, across, 0)
    early = exchange(upper)
    whole_sum(dk_out, dk_back, dk_all, dk_own, 0, SCALE)
    give_back(dk_own, dk_in)
    lax.fori_loop(4 * PAD // KERNEL, pairs, across, 0)
    coef_out[...] = jnp.concatenate([db_ref[...], dc_ref[...]], axis=1).astype(BF16)
    coefs = [post.send(coef_out, coef_all.at[head], peer) for peer in head_peers]
    coef_all[head] = coef_out[...]
    wide = widen(upper, early)
    written = []

    def write(source, target):
        written.append(pltpu.make_async_copy(source, target, writes.at[len(written)]))
        written[-1].start()

    write(gconv_ref, gconv_hbm)
    write(ggate_ref, ggate_hbm)

    spill_copy = post.send(edge_ref, spill_ref, former)
    per_head = dot(sums_ref[...], spread_ref[...], 1, 1, EXACT)[:, 0:heads]
    last_row = per_head[2:3] + through * per_head[1:2]
    dcum = zu_ref[:, 0:heads] + jnp.where(t == rows - 1, last_row, 0.0)
    dlog = dot(tri, dcum, 0, 0, EXACT)
    grad_step = (zu_ref[:, LANES // 2 : LANES // 2 + heads] - dlog * rate) * jax.nn.sigmoid(raw)
    turn_back[...] = jnp.zeros_like(turn_back)
    turn_back[:, 0:heads] = grad_step
    gstep_ref[...] = turn_back[...].T[0:heads, :]
    write(gstep_ref, gstep_hbm)
    small = KERNEL * pairs
    red_out[small : small + 1, 0:heads] = jnp.sum(grad_step, axis=0, keepdims=True)
    red_out[small + 1 : small + 2, 0:heads] = jnp.sum(dlog * log_decay, axis=0, keepdims=True)
    red_out[small + 2 : small + 3, 0:heads] = per_head[0:1]
    reds = exchange(under)
    wide += widen(under, reds)
    whole_sum(dv_out, dv_back, dv_all, dv_own, PLACES, 1.0)
    give_back(dv_own, dv_in)
    spill_copy.wait()
    gfix_ref[...] = end_ref[...] + spill_ref[...]
    write(gfix_ref, gfix_hbm)
    for copy in coefs:
        copy.wait()
    halves = [coef_all[2 * n].astype(F32) + coef_all[2 * n + 1].astype(F32) for n in range(2)]
    half = coef_out.shape[1] // 2
    gin_ref[...] = jnp.concatenate([halves[0][:, :half], halves[1][:, :half]], axis=1)
    gout_ref[...] = jnp.concatenate([halves[0][:, half:], halves[1][:, half:]], axis=1)
    write(gin_ref, gin_hbm)
    write(gout_ref, gout_hbm)
    for copy in wide:
        copy.wait()
    total = red_b[0]
    for n in range(1, groups):
        total = total + red_b[n]
    total_ref[...] = total
    for copy in kept + written:
        copy.wait()


def finish_kernel(ins, outs, in_bufs, out_bufs, load_sems, store_sems):
    loads = [pltpu.make_async_copy(a, b, load_sems.at[n]) for n, (a, b) in enumerate(zip(ins, in_bufs))]
    for load in loads:
        load.start()
    stores = []

    def store(source, target):
        stores.append(pltpu.make_async_copy(source, target, store_sems.at[len(stores)]))
        stores[-1].start()

    total, fix, gconv = in_bufs[0], in_bufs[1], in_bufs[2]
    for load in loads[:3]:
        load.wait()
    gconv[gconv.shape[0] - PAD :, :] = fix[...].astype(BF16)
    store(gconv, outs[3])
    conv, *small = out_bufs[3:]
    pairs, heads = conv.shape[1] // LANES, small[0].shape[1]
    for lag in range(KERNEL):
        for n in range(pairs):
            row = KERNEL * n + lag
            conv[lag : lag + 1, n * LANES : (n + 1) * LANES] = total[row : row + 1, :]
    for n, ref in enumerate(small):
        row = KERNEL * pairs + n
        ref[...] = total[row : row + 1, 0:heads]
    for n, ref in enumerate((conv, *small)):
        store(ref, outs[8 + n])
    for n in range(3, 7):
        loads[n].wait()
        store(in_bufs[n], outs[n + 1])
    for n in range(3):
        loads[7 + n].wait()
        for r in range(PLACES):
            unfold(in_bufs[7 + n], (r,), out_bufs[n], (), r * HEAD_DIM)
        store(out_bufs[n], outs[n])
    for copy in stores:
        copy.wait()


def local(
    queries, keys, values, attn_grad, doc_ids, conv_input, conv_weight, step_raw, step_bias,
    rate_log, skip_gain, input_coeff, output_coeff, gate_input, mix_grad,
):
    rows, width = queries.shape
    heads, channels = step_raw.shape[1], conv_input.shape[1]
    pairs = channels // LANES
    groups = lax.axis_size("seq") // PLACES
    struct = jax.ShapeDtypeStruct
    vmem = pl.BlockSpec(memory_space=pltpu.VMEM)
    loose = pl.BlockSpec(memory_space=pl.ANY)
    dma = lambda n: pltpu.SemaphoreType.DMA((n,))
    head_cols = 2 * LANES
    quarter = (2, 2 * PAD, channels)
    part = quarter[1:]
    half = lambda *shape: pltpu.VMEM(shape, BF16)
    full = lambda *shape: pltpu.VMEM(shape, F32)
    flat = full(PAD, channels)
    piece = lambda n: half(n, rows, head_cols)
    slim_rows = rows * HEAD_DIM // LANES
    slim = lambda n: half(n, slim_rows, LANES)
    red_rows = 64
    wide_shape = (rows, channels)
    small = [
        doc_ids.reshape(-1, LANES), step_raw.T, step_bias[None], rate_log[None], skip_gain[None],
        input_coeff, output_coeff, conv_weight,
    ]
    mid = pl.pallas_call(
        whole_kernel,
        in_specs=[[loose] * 8] + [loose] * 7,
        out_specs=[loose] * 9 + [vmem],
        out_shape=[struct((PLACES, slim_rows, LANES), BF16)] * 3
        + [
            struct(wide_shape, BF16), struct(wide_shape, BF16), struct((PAD, channels), F32),
            struct((heads, rows), F32), struct((rows, LANES), F32), struct((rows, LANES), F32),
            struct((red_rows, LANES), F32),
        ],
        scratch_shapes=[
            [pltpu.VMEM(a.shape, a.dtype) for a in small],
            flat, full(heads, rows), full(rows, LANES), full(rows, LANES), half(*wide_shape), half(*wide_shape),
            full(PAD, rows), full(PLACES * rows // LANES, LANES), full(LANES, rows), full(rows, LANES),
            half(rows, width), half(rows, width), half(rows, width), half(rows, width),
            half(*wide_shape), half(*wide_shape), half(*wide_shape),
            slim(PLACES), slim(PLACES), slim(PLACES), slim(PLACES),
            slim(PLACES), slim(PLACES), slim(2 * PLACES), slim(2 * PLACES), full(slim_rows, LANES),
            piece(PLACES), piece(PLACES), piece(2 * PLACES), piece(2 * PLACES),
            full(2 * PLACES, rows, head_cols), full(2 * PLACES, rows, head_cols),
            slim(PLACES), slim(PLACES), slim(PLACES), slim(PLACES),
            slim(PLACES), slim(PLACES), slim(PLACES),
            half(2 * PAD, channels), flat, full(pairs, rows, 8), full(pairs, 2, rows), full(LANES, channels),
            full(KERNEL - 1, rows, LANES), full(rows + PAD, channels),
            full(*wide_shape), full(*wide_shape), full(*wide_shape), full(*wide_shape), full(*wide_shape),
            full(*wide_shape),
            half(PLACES, *quarter), half(PLACES, *quarter), half(*part), half(*part), full(PAD, LANES),
            half(REACH, *part), half(REACH, *part), full(REACH, PAD, LANES), full(REACH, PAD, LANES),
            half(PLACES, *quarter), half(PLACES, *quarter), full(PAD, LANES), full(PLACES, PAD, LANES),
            full(rows, rows), full(rows, rows), full(rows, rows), full(KERNEL, rows + 2 * PAD, LANES),
            full(rows, LANES), full(rows, LANES // 2), full(rows, LANES // 2),
            flat, flat, flat, flat, half(rows, LANES), half(4, rows, LANES),
            full(red_rows, LANES), full(PLACES, red_rows, LANES), full(red_rows, LANES),
            full(groups, red_rows, LANES),
            dma(SENDS), dma(SENDS), dma(2 * PLACES), dma(2 * PLACES), dma(7), dma(3 * PLACES), dma(6), dma(8),
        ],
        name="whole",
        compiler_params=pltpu.CompilerParams(
            collective_id=0, has_side_effects=True, vmem_limit_bytes=58 * 1024 * 1024
        ),
    )(
        small, keys, values, queries, attn_grad, conv_input, gate_input, mix_grad,
    )
    dq, dk, dv, gconv, ggate, gfix, gstep, gin, gout, total = mid
    ins = [total, gfix, gconv, ggate, gstep, gin, gout, dq, dk, dv]
    shapes = [struct((rows, width), BF16)] * 3 + [
        struct(wide_shape, BF16), struct(wide_shape, BF16), struct((heads, rows), F32),
        struct((rows, LANES), F32), struct((rows, LANES), F32), struct((KERNEL, channels), F32),
    ] + [struct((1, heads), F32)] * 3
    *outs, conv, bias, rate, skip = pl.pallas_call(
        finish_kernel,
        in_specs=[[loose] * len(ins)],
        out_specs=[[loose] * len(shapes)],
        out_shape=[shapes],
        scratch_shapes=[
            [pltpu.VMEM(a.shape, a.dtype) for a in ins],
            [pltpu.VMEM(shapes[n].shape, shapes[n].dtype) for n in (0, 1, 2, 8, 9, 10, 11)],
            dma(len(ins)), dma(len(shapes)),
        ],
        name="finish",
    )(ins)[0]
    outs[5] = outs[5].T
    return (*outs, conv, bias[0], rate[0], skip[0])


def solution(mesh):
    sharded = P("seq", "head")
    return jax.shard_map(
        local,
        mesh=mesh,
        in_specs=(
            sharded, sharded, sharded, sharded, P(), sharded, P(None, "head"), sharded,
            P("head"), P("head"), P("head"), P("seq", None), P("seq", None), sharded, sharded,
        ),
        out_specs=(
            sharded, sharded, sharded, sharded, sharded, sharded,
            P("seq", None), P("seq", None), P(None, "head"), P("head"), P("head"), P("head"),
        ),
        check_vma=False,
    )
```
